32 devices in a mesh: req: 4 (over x, y), dap: 8 (over z, core).
Axes of the slice: x: 2, y: 2, z: 4, core: 2. Of those that a mesh axis runs over, the one named last changes fastest.
Arguments:
- msa_act: bfloat16 [1024, 128, 256], P(('req', 'dap')), parts along dimension 0
- pair_act: bfloat16 [512, 128, 128], P(('req', 'dap')), parts along dimension 0
- msa_mask: int32 [1024, 128], P(('req', 'dap')), parts along dimension 0
- pair_mask: int32 [512, 128], P(('req', 'dap')), parts along dimension 0
- row_qkvg: bfloat16 [2, 256, 1024], replicated
- row_bias: bfloat16 [2, 128, 8], replicated
- row_out: bfloat16 [2, 256, 256], replicated
- col_qkvg: bfloat16 [2, 256, 1024], replicated
- col_out: bfloat16 [2, 256, 256], replicated
- mtr_in: bfloat16 [2, 256, 1024], replicated
- mtr_out: bfloat16 [2, 1024, 256], replicated
- opm_proj: bfloat16 [2, 256, 64], replicated
- opm_out: bfloat16 [2, 1024, 128], replicated
- tmo_proj: bfloat16 [2, 128, 640], replicated
- tmo_out: bfloat16 [2, 128, 128], replicated
- tmi_proj: bfloat16 [2, 128, 640], replicated
- tmi_out: bfloat16 [2, 128, 128], replicated
- tas_qkvg: bfloat16 [2, 128, 512], replicated
- tas_bias: bfloat16 [2, 128, 4], replicated
- tas_out: bfloat16 [2, 128, 128], replicated
- tae_qkvg: bfloat16 [2, 128, 512], replicated
- tae_bias: bfloat16 [2, 128, 4], replicated
- tae_out: bfloat16 [2, 128, 128], replicated
- ptr_in: bfloat16 [2, 128, 512], replicated
- ptr_out: bfloat16 [2, 512, 128], replicated
Outputs:
- output 1: bfloat16 [1024, 128, 256], P(('req', 'dap')), parts along dimension 0
- output 2: bfloat16 [512, 128, 128], P(('req', 'dap')), parts along dimension 0
There are 4 independent parts. The reference program is written for one: setup_inputs(seed, part) draws one part's arguments, and reference() takes and returns one part's arrays. A program takes and returns all parts, laid end to end along the dimension named above; an argument that names none is the same for every part.
All inputs are finite; a program needn't handle non-finite values.
Results may differ from the reference program's by a relative error of at most 0.02.
Values are sent between devices in bfloat16 or wider.
A program may use at most 1 GiB of HBM per device.

```python
import jax
import jax.numpy as jnp
from jax import lax

SEQ = 256
RES = 128
MSA_DIM = 256
PAIR_DIM = 128
MSA_HEADS = 8
MSA_HEAD_DIM = 32
PAIR_HEADS = 4
PAIR_HEAD_DIM = 32
OPM_DIM = 32
TRI_DIM = 128
LAYERS = 2

WEIGHT_NAMES = ('row_qkvg', 'row_bias', 'row_out', 'col_qkvg', 'col_out', 'mtr_in', 'mtr_out', 'opm_proj', 'opm_out', 'tmo_proj', 'tmo_out', 'tmi_proj', 'tmi_out', 'tas_qkvg', 'tas_bias', 'tas_out', 'tae_qkvg', 'tae_bias', 'tae_out', 'ptr_in', 'ptr_out')


def weight_fans():
    msa_width = MSA_HEADS * MSA_HEAD_DIM
    pair_width = PAIR_HEADS * PAIR_HEAD_DIM
    return ((MSA_DIM, 4 * msa_width), (PAIR_DIM, MSA_HEADS), (msa_width, MSA_DIM),
            (MSA_DIM, 4 * msa_width), (msa_width, MSA_DIM),
            (MSA_DIM, 4 * MSA_DIM), (4 * MSA_DIM, MSA_DIM),
            (MSA_DIM, 2 * OPM_DIM), (OPM_DIM * OPM_DIM, PAIR_DIM),
            (PAIR_DIM, 4 * TRI_DIM + PAIR_DIM), (TRI_DIM, PAIR_DIM),
            (PAIR_DIM, 4 * TRI_DIM + PAIR_DIM), (TRI_DIM, PAIR_DIM),
            (PAIR_DIM, 4 * pair_width), (PAIR_DIM, PAIR_HEADS), (pair_width, PAIR_DIM),
            (PAIR_DIM, 4 * pair_width), (PAIR_DIM, PAIR_HEADS), (pair_width, PAIR_DIM),
            (PAIR_DIM, 4 * PAIR_DIM), (4 * PAIR_DIM, PAIR_DIM))


def draw_masks(mask_key):
    key_list = jax.random.split(mask_key, 4)
    pad_len = jax.random.randint(key_list[0], (), 1, RES // 16 + 1)
    res_ids = jnp.arange(RES)
    seq_ids = jnp.arange(SEQ)[:, None]
    is_valid = res_ids < RES - pad_len
    shallow = jax.random.randint(key_list[1], (RES,), 0, 4) == 0
    depths = jnp.where(shallow, jax.random.randint(key_list[2], (RES,), 1, SEQ // 4 + 1), SEQ)
    kept_mask = (jax.random.randint(key_list[3], (SEQ, RES), 0, 8) != 0) | (seq_ids == 0)
    msa_mask = ((seq_ids < depths[None, :]) & kept_mask & is_valid[None, :]).astype(jnp.int32)
    pair_mask = (is_valid[:, None] & is_valid[None, :]).astype(jnp.int32)
    return msa_mask, pair_mask


def setup_inputs(seed: int = 0, part: int = 0) -> dict:
    part_key = jax.random.fold_in(jax.random.key(seed), part)
    key_list = jax.random.split(part_key, 3)
    shared = jax.random.normal(key_list[0], (1, RES, MSA_DIM), jnp.float32)
    spread = jax.random.normal(key_list[1], (SEQ, RES, MSA_DIM), jnp.float32)
    msa_act = (shared + spread).astype(jnp.bfloat16)
    pair_act = jax.random.normal(key_list[2], (RES, RES, PAIR_DIM), jnp.float32).astype(jnp.bfloat16)
    msa_mask, pair_mask = draw_masks(jax.random.fold_in(part_key, 5))
    inputs = {'msa_act': msa_act, 'pair_act': pair_act, 'msa_mask': msa_mask, 'pair_mask': pair_mask}
    weight_key = jax.random.key(seed + 1)
    for w_index, fan_pair in enumerate(weight_fans()):
        sample = jax.random.normal(jax.random.fold_in(weight_key, w_index), (LAYERS,) + fan_pair, jnp.float32)
        inputs[WEIGHT_NAMES[w_index]] = (sample * fan_pair[0] ** -0.5).astype(jnp.bfloat16)
    return inputs


def layer_norm(x):
    values = x.astype(jnp.float32)
    centered = values - jnp.mean(values, axis=-1, keepdims=True)
    variance = jnp.mean(centered * centered, axis=-1, keepdims=True)
    return (centered * lax.rsqrt(variance + 1e-5)).astype(jnp.bfloat16)


def linear(x, weight):
    flat_x = x.reshape(-1, x.shape[-1])
    result = jnp.dot(flat_x, weight, preferred_element_type=jnp.float32)
    return result.reshape(x.shape[:-1] + (weight.shape[-1],))


def residual(x, update):
    return (x.astype(jnp.float32) + update).astype(jnp.bfloat16)


def attend_row(x_row, bias_hij, mask_row, w_qkvg, w_out, num_heads):
    length = x_row.shape[0]
    head_width = w_out.shape[0]
    head_dim = head_width // num_heads
    projected = jnp.dot(x_row, w_qkvg, preferred_element_type=jnp.float32).astype(jnp.bfloat16).astype(jnp.float32)
    queries = projected[:, :head_width].reshape(length, num_heads, head_dim)
    keyset = projected[:, head_width:2 * head_width].reshape(length, num_heads, head_dim)
    valset = projected[:, 2 * head_width:3 * head_width].reshape(length, num_heads, head_dim)
    gate_act = jax.nn.sigmoid(projected[:, 3 * head_width:])
    logits = jnp.einsum('ihd,jhd->hij', queries, keyset) * head_dim ** -0.5 + bias_hij.astype(jnp.float32)
    logits = jnp.where(mask_row[None, None, :] > 0, logits, -1e9)
    attn_prob = jax.nn.softmax(logits, axis=-1).astype(jnp.bfloat16).astype(jnp.float32)
    attended = jnp.einsum('hij,jhd->ihd', attn_prob, valset).reshape(length, head_width)
    gated = (attended * gate_act).astype(jnp.bfloat16)
    return jnp.dot(gated, w_out, preferred_element_type=jnp.float32)


def row_attention(msa_act, pair_act, msa_mask, w_qkvg, w_bias, w_out):
    pair_bias = jnp.transpose(linear(layer_norm(pair_act), w_bias).astype(jnp.bfloat16), (2, 0, 1))
    msa_norm = layer_norm(msa_act)
    return lax.map(lambda item: attend_row(item[0], pair_bias, item[1], w_qkvg, w_out, w_bias.shape[1]), (msa_norm, msa_mask))


def column_attention(msa_act, msa_mask, w_qkvg, w_out, num_heads):
    msa_norm = jnp.swapaxes(layer_norm(msa_act), 0, 1)
    zero_bias = jnp.zeros((1, 1, 1), jnp.float32)
    update = lax.map(lambda item: attend_row(item[0], zero_bias, item[1], w_qkvg, w_out, num_heads), (msa_norm, msa_mask.T))
    return jnp.swapaxes(update, 0, 1)


def transition(x, w_in, w_out):
    hidden = jnp.maximum(linear(layer_norm(x), w_in), 0.0).astype(jnp.bfloat16)
    return linear(hidden, w_out)


def outer_product_mean(msa_act, msa_mask, w_proj, w_out):
    opm_dim = w_proj.shape[1] // 2
    projected = linear(layer_norm(msa_act), w_proj).astype(jnp.bfloat16)
    mask_bf = msa_mask.astype(jnp.bfloat16)[:, :, None]
    left_act = (projected[..., :opm_dim] * mask_bf).astype(jnp.float32)
    right_act = (projected[..., opm_dim:] * mask_bf).astype(jnp.float32)
    mask_f = msa_mask.astype(jnp.float32)
    overlap = jnp.dot(mask_f.T, mask_f)

    def outer_row(left_row):
        outer_prod = jnp.einsum('sc,sje->jce', left_row, right_act).astype(jnp.bfloat16)
        return linear(outer_prod.reshape(outer_prod.shape[0], opm_dim * opm_dim), w_out)

    update = lax.map(outer_row, jnp.swapaxes(left_act, 0, 1))
    return update / (1e-3 + overlap)[:, :, None]


def tri_mul(pair_act, pair_mask, w_proj, w_out, form):
    tri_dim = (w_proj.shape[1] - pair_act.shape[-1]) // 4
    projected = linear(layer_norm(pair_act), w_proj)
    mask_f = pair_mask.astype(jnp.float32)[:, :, None]
    left_act = (mask_f * jax.nn.sigmoid(projected[..., 2 * tri_dim:3 * tri_dim]) * projected[..., :tri_dim]).astype(jnp.bfloat16)
    right_act = (mask_f * jax.nn.sigmoid(projected[..., 3 * tri_dim:4 * tri_dim]) * projected[..., tri_dim:2 * tri_dim]).astype(jnp.bfloat16)
    gate_act = jax.nn.sigmoid(projected[..., 4 * tri_dim:])
    product = jnp.einsum(form, left_act.astype(jnp.float32), right_act.astype(jnp.float32))
    return gate_act * linear(layer_norm(product), w_out)


def tri_attention(pair_act, pair_mask, w_qkvg, w_bias, w_out):
    pair_norm = layer_norm(pair_act)
    pair_bias = jnp.transpose(linear(pair_norm, w_bias).astype(jnp.bfloat16), (2, 0, 1))
    return lax.map(lambda item: attend_row(item[0], pair_bias, item[1], w_qkvg, w_out, w_bias.shape[1]), (pair_norm, pair_mask))


def evoformer_block(msa_act, pair_act, msa_mask, pair_mask, layer_w):
    (row_qkvg, row_bias, row_out, col_qkvg, col_out, mtr_in, mtr_out, opm_proj, opm_out,
     tmo_proj, tmo_out, tmi_proj, tmi_out, tas_qkvg, tas_bias, tas_out,
     tae_qkvg, tae_bias, tae_out, ptr_in, ptr_out) = layer_w
    msa_act = residual(msa_act, row_attention(msa_act, pair_act, msa_mask, row_qkvg, row_bias, row_out))
    msa_act = residual(msa_act, column_attention(msa_act, msa_mask, col_qkvg, col_out, row_bias.shape[1]))
    msa_act = residual(msa_act, transition(msa_act, mtr_in, mtr_out))
    pair_act = residual(pair_act, outer_product_mean(msa_act, msa_mask, opm_proj, opm_out))
    pair_act = residual(pair_act, tri_mul(pair_act, pair_mask, tmo_proj, tmo_out, 'ikc,jkc->ijc'))
    pair_act = residual(pair_act, tri_mul(pair_act, pair_mask, tmi_proj, tmi_out, 'kic,kjc->ijc'))
    pair_act = residual(pair_act, tri_attention(pair_act, pair_mask, tas_qkvg, tas_bias, tas_out))
    pair_swap = jnp.swapaxes(pair_act, 0, 1)
    pair_act = residual(pair_act, jnp.swapaxes(tri_attention(pair_swap, pair_mask.T, tae_qkvg, tae_bias, tae_out), 0, 1))
    pair_act = residual(pair_act, transition(pair_act, ptr_in, ptr_out))
    return msa_act, pair_act


def reference(msa_act, pair_act, msa_mask, pair_mask, row_qkvg, row_bias, row_out, col_qkvg, col_out, mtr_in, mtr_out, opm_proj, opm_out, tmo_proj, tmo_out, tmi_proj, tmi_out, tas_qkvg, tas_bias, tas_out, tae_qkvg, tae_bias, tae_out, ptr_in, ptr_out):
    stacked = (row_qkvg, row_bias, row_out, col_qkvg, col_out, mtr_in, mtr_out, opm_proj, opm_out,
               tmo_proj, tmo_out, tmi_proj, tmi_out, tas_qkvg, tas_bias, tas_out,
               tae_qkvg, tae_bias, tae_out, ptr_in, ptr_out)

    def step(carry, layer_w):
        return evoformer_block(carry[0], carry[1], msa_mask, pair_mask, layer_w), None

    carried, ignored = lax.scan(step, (msa_act, pair_act), stacked)
    return carried[0], carried[1]
```

```python
import functools

import jax
import jax.numpy as jnp
from jax import lax
from jax.experimental import pallas as pl
from jax.experimental.pallas import tpu as pltpu
from jax.sharding import PartitionSpec as P

MESH = pl.DeviceIdType.MESH
F32 = jnp.float32
BF = jnp.bfloat16
LOG2E = 1.4426950408889634
NEG = -1e9 * LOG2E
ND = 8
VMEM_LIMIT = 66_000_000
RB = 128
SQ = 256
TI = 16
HD = 32


def dot(a, b):
    return lax.dot_general(a, b, (((1,), (0,)), ((), ())), preferred_element_type=F32)


def dot_nt(a, b):
    return lax.dot_general(a, b, (((1,), (1,)), ((), ())), preferred_element_type=F32)


def dot_tn(a, b):
    return lax.dot_general(a, b, (((0,), (0,)), ((), ())), preferred_element_type=F32)


def transpose_bf(w):
    return w.astype(F32).T.astype(BF)


def norm_lanes(x):
    mean = jnp.mean(x, axis=-1, keepdims=True)
    centered = x - mean
    var = jnp.mean(centered * centered, axis=-1, keepdims=True)
    return (centered * lax.rsqrt(var + 1e-5)).astype(BF)


def norm_rows(x):
    mean = jnp.mean(x, axis=0, keepdims=True)
    centered = x - mean
    var = jnp.mean(centered * centered, axis=0, keepdims=True)
    return (centered * lax.rsqrt(var + 1e-5)).astype(BF)


def residual(x, update):
    return (x.astype(F32) + update).astype(BF)


def group_barrier(me):
    sem = pltpu.get_barrier_semaphore()
    for p in range(1, ND):
        pl.semaphore_signal(sem, inc=1, device_id={'dap': lax.rem(me + p, ND)}, device_id_type=MESH)
    pl.semaphore_wait(sem, ND - 1)


def remote(src, dst, send_sem, recv_sem, peer):
    return pltpu.make_async_remote_copy(src_ref=src, dst_ref=dst, send_sem=send_sem, recv_sem=recv_sem,
                                        device_id={'dap': peer}, device_id_type=MESH)


class Direct:
    def __init__(self, me, src_of, dst_of, ssem, rsem, base=0):
        self.me, self.src_of, self.dst_of, self.ssem, self.rsem, self.base = me, src_of, dst_of, ssem, rsem, base

    def copy_to(self, p):
        peer = lax.rem(self.me + p, ND)
        return remote(self.src_of(peer), self.dst_of(self.me), self.ssem.at[self.base + p], self.rsem.at[self.base + p], peer)

    def start(self, ps=range(1, ND)):
        for p in ps:
            self.copy_to(p).start()

    def wait_recv(self):
        for p in range(1, ND):
            owner = lax.rem(self.me + ND - p, ND)
            remote(self.src_of(owner), self.dst_of(owner), self.ssem.at[self.base + p], self.rsem.at[self.base + p], owner).wait_recv()

    def wait_send(self):
        for p in range(1, ND):
            self.copy_to(p).wait_send()


class Chain:
    def __init__(self, me, buf, ssem, rsem):
        self.buf, self.ssem, self.rsem = buf, ssem, rsem
        self.z, self.c = lax.div(me, 2), lax.rem(me, 2)
        self.me, self.partner = me, me + 1 - 2 * self.c

    def cp(self, slot, peer, sem):
        return remote(self.buf.at[slot], self.buf.at[slot], self.ssem.at[sem], self.rsem.at[sem], peer)

    def slot(self, off, other=False):
        core = 1 - self.c if other else self.c
        return (self.z + off) * 2 + core

    def start(self):
        @pl.when(self.z < 3)
        def _():
            self.cp(self.me, self.me + 2, 0).start()

        @pl.when(self.z > 0)
        def _():
            self.cp(self.me, self.me - 2, 3).start()

        self.cp(self.me, self.partner, 6).start()

    def finish(self):
        z = self.z
        for t in range(1, 4):
            @pl.when(z >= t)
            def _():
                self.cp(self.slot(-t), self.me, t - 1).wait_recv()
                if t < 3:
                    @pl.when(z < 3)
                    def _():
                        self.cp(self.slot(-t), self.me + 2, t).start()
                self.cp(self.slot(-t), self.partner, 6 + t).start()

            @pl.when(z + t <= 3)
            def _():
                self.cp(self.slot(t), self.me, 3 + t - 1).wait_recv()
                if t < 3:
                    @pl.when(z > 0)
                    def _():
                        self.cp(self.slot(t), self.me - 2, 3 + t).start()
                self.cp(self.slot(t), self.partner, 9 + t).start()
        self.cp(self.partner, self.me, 6).wait_recv()
        for t in range(1, 4):
            @pl.when(z >= t)
            def _():
                self.cp(self.slot(-t, True), self.me, 6 + t).wait_recv()

            @pl.when(z + t <= 3)
            def _():
                self.cp(self.slot(t, True), self.me, 9 + t).wait_recv()

    def wait_send(self):
        z = self.z

        @pl.when(z < 3)
        def _():
            self.cp(self.me, self.me + 2, 0).wait_send()

        @pl.when(z > 0)
        def _():
            self.cp(self.me, self.me - 2, 3).wait_send()

        self.cp(self.me, self.partner, 6).wait_send()
        for t in range(1, 4):
            @pl.when(z >= t)
            def _():
                if t < 3:
                    @pl.when(z < 3)
                    def _():
                        self.cp(self.slot(-t), self.me + 2, t).wait_send()
                self.cp(self.slot(-t), self.partner, 6 + t).wait_send()

            @pl.when(z + t <= 3)
            def _():
                if t < 3:
                    @pl.when(z > 0)
                    def _():
                        self.cp(self.slot(t), self.me - 2, 3 + t).wait_send()
                self.cp(self.slot(t), self.partner, 9 + t).wait_send()


def column_of(row):
    return jnp.broadcast_to(row, (RB, row.shape[1])).T


def attend_tile(xn, wt_ref, wk, w_out, heads, bias_ref, key_mask):
    length = xn.shape[0]
    width = heads * HD
    proj = dot_nt(wt_ref[...], xn)
    q_t = proj[:width].astype(BF)
    v_t = proj[width:2 * width].astype(BF)
    gate = jax.nn.sigmoid(proj[2 * width:].astype(BF).astype(F32))
    keys = dot(xn, wk).astype(BF)
    valid = key_mask > 0
    scale = HD ** -0.5 * LOG2E
    pieces = []
    for qc in range(length // RB):
        outs = []
        for h in range(heads):
            hh = h % 4
            q_h = q_t[HD * h:HD * h + HD, RB * qc:RB * qc + RB]
            rhs = [q_h]
            if hh > 0:
                rhs = [jnp.zeros((HD * hh, RB), BF)] + rhs
            if hh < 3:
                rhs = rhs + [jnp.zeros((96 - HD * hh, RB), BF)]
            logits = dot(keys[:, RB * (h // 4):RB * (h // 4) + RB], jnp.concatenate(rhs, 0)) * scale
            if bias_ref is not None:
                logits = logits + bias_ref[h]
            logits = jnp.where(valid, logits, NEG)
            top = jnp.max(logits, axis=0, keepdims=True)
            e = jnp.exp2(logits - top)
            inv = 1.0 / jnp.sum(e, axis=0, keepdims=True)
            prob = (e * inv).astype(BF)
            outs.append(dot(v_t[HD * h:HD * h + HD], prob))
        gated = (jnp.concatenate(outs, 0) * gate[:, RB * qc:RB * qc + RB]).astype(BF)
        pieces.append(dot_tn(gated, w_out))
    return pieces


def prep_qkvg(w_ref, wt_ref, width):
    wt_ref[0:width, :] = transpose_bf(w_ref[0, :, 0:width])
    wt_ref[width:3 * width, :] = transpose_bf(w_ref[0, :, 2 * width:4 * width])


def mask_kernel(mm_ref, pm_ref, mt_ref, pt_ref, mbuf, pbuf, ssem, rsem):
    me = lax.axis_index('dap')
    group_barrier(me)
    mbuf[me] = mm_ref[...].astype(F32)
    pbuf[me] = pm_ref[...].astype(F32)
    ex_m = Direct(me, lambda peer: mbuf.at[me], lambda owner: mbuf.at[owner], ssem, rsem, 0)
    ex_p = Direct(me, lambda peer: pbuf.at[me], lambda owner: pbuf.at[owner], ssem, rsem, ND)
    ex_m.start()
    ex_p.start()
    ex_m.wait_recv()
    ex_p.wait_recv()
    mt_ref[...] = mbuf[...].reshape(SQ, RB).T
    pt_ref[...] = pbuf[...].reshape(RB, RB).T
    ex_m.wait_send()
    ex_p.wait_send()


def msa_kernel(m_ref, z_ref, rmask_ref, mt_ref, row_w, row_b, row_o, col_w, col_o, mtr_i, mtr_o, opm_p,
               m2_ref, at_ref, bt_ref,
               bloc, ball, bias_t, wt, opt, scr, sendbuf, rbuf, bscr, ssem, rsem):
    me = lax.axis_index('dap')
    group_barrier(me)
    wb = jnp.concatenate([row_b[0], jnp.zeros((RB, 120), BF)], 1)
    wb_t = transpose_bf(wb)[0:8]

    def bias_row(i, carry):
        xn = norm_lanes(z_ref[i].astype(F32))
        bscr[pl.ds(i, 8, stride=TI), :] = dot_nt(wb_t, xn)
        return carry

    lax.fori_loop(0, TI, bias_row, 0)
    ball[me] = bscr[...].astype(BF).reshape(8, TI, RB)
    ex_b = Direct(me, lambda peer: ball.at[me], lambda owner: ball.at[owner], ssem, rsem, 0)
    ex_b.start()
    prep_qkvg(row_w, wt, SQ)
    opt[...] = transpose_bf(jnp.concatenate([opm_p[0], jnp.zeros((SQ, 64), BF)], 1))[0:64]
    ex_b.wait_recv()
    for h in range(8):
        bias_t[h] = ball[:, h].reshape(RB, RB).astype(F32).T * LOG2E
    row_k = row_w[0, :, SQ:512]
    row_ow = row_o[0]
    exchanges = []
    for ck in range(2):
        def row_body(sl, carry):
            s = ck * TI + sl
            x = m_ref[s]
            key_mask = column_of(rmask_ref[pl.ds(s, 1), :])
            upd, = attend_tile(norm_lanes(x.astype(F32)), wt, row_k, row_ow, 8, bias_t, key_mask)
            y = residual(x, upd).astype(F32)
            for half in range(2):
                scr[half, pl.ds(sl, RB, stride=TI), :] = y[:, RB * half:RB * half + RB]
            return carry

        lax.fori_loop(0, TI, row_body, 0)

        def pack(d, carry):
            for half in range(2):
                part = scr[half, pl.ds(pl.multiple_of(d * SQ, SQ), SQ), :].astype(BF).reshape(TI, TI, RB)
                sendbuf[ck, d, :, :, RB * half:RB * half + RB] = part
            return carry

        lax.fori_loop(0, 8, pack, 0)
        ex = Direct(me, lambda peer: sendbuf.at[ck, peer], lambda owner: rbuf.at[owner * 2 + ck], ssem, rsem, 8 * (ck + 1))
        ex.start()
        exchanges.append(ex)
        rbuf[me * 2 + ck] = sendbuf[ck, me]
    ex_b.wait_send()
    prep_qkvg(col_w, wt, SQ)
    for ex in exchanges:
        ex.wait_recv()
    col_k = col_w[0, :, SQ:512]
    col_ow = col_o[0]

    def col_body(r, carry):
        x = rbuf[:, r].reshape(SQ, SQ)
        mrow = mt_ref[pl.ds(me * TI + r, 1), :]
        key_mask = column_of(mrow)
        upd = attend_tile(norm_lanes(x.astype(F32)), wt, col_k, col_ow, 8, None, key_mask)
        y = residual(x, jnp.concatenate(upd, 0))
        hid = jnp.maximum(dot(norm_lanes(y.astype(F32)), mtr_i[0]), 0.0).astype(BF)
        y2 = residual(y, dot(hid, mtr_o[0]))
        m2_ref[r] = y2
        ab = dot_nt(opt[...], norm_lanes(y2.astype(F32))).astype(BF).astype(F32) * mrow
        at_ref[r] = ab[0:HD].astype(BF)
        for half in range(2):
            scr[half, pl.ds(r, HD, stride=TI), :] = ab[HD:64, RB * half:RB * half + RB]
        return carry

    lax.fori_loop(0, TI, col_body, 0)
    for half in range(2):
        bt_ref[:, :, RB * half:RB * half + RB] = scr[half, 0:512, :].astype(BF).reshape(HD, TI, RB)
    for ex in exchanges:
        ex.wait_send()


def pair_kernel(m2_ref, at_ref, bt_ref, z_ref, mt_ref, pm_ref, pt_ref,
                opm_o, tmo_p, tmo_o, tmi_p, tmi_o, tas_w, tas_b, tas_o, tae_w, tae_b, tae_o, ptr_i, ptr_o,
                mout_ref, zout_ref,
                btall, obuf, opw, scr_a, scr_b, scr_x, a_c, ball1, ball2, gbuf, z1, zcol, sbias, ball3, bias_t,
                wt, twt, zsend, z4, mrecv, mscr,
                ch_s, ch_r, ds, dr):
    me = lax.axis_index('dap')
    group_barrier(me)
    btall[me] = bt_ref[...]
    ag0 = Chain(me, btall, ch_s.at[0], ch_r.at[0])
    ag0.start()
    scr_a[0:1024, :] = opm_o[0].astype(F32)

    def perm(e, carry):
        rows = scr_a[pl.ds(e, HD, stride=HD), :]
        scr_b[pl.ds(pl.multiple_of(e * HD, HD), HD), :] = rows
        return carry

    lax.fori_loop(0, HD, perm, 0)
    for q in range(8):
        opw[:, RB * q:RB * q + RB] = scr_b[RB * q:RB * q + RB, :].T.astype(BF)
    mloc = mt_ref[pl.ds(pl.multiple_of(me * TI, TI), TI), :].astype(BF)
    inv_over = 1.0 / (1e-3 + dot_nt(mloc, mt_ref[...].astype(BF)))
    scr_x[0:TI, :] = inv_over
    ag0.finish()

    left = at_ref[...].reshape(512, SQ)

    def opm_e(e, carry):
        rhs = btall[:, e].reshape(RB, SQ)
        o = dot_nt(left, rhs).astype(BF).reshape(TI, HD, RB)
        obuf[:, pl.ds(pl.multiple_of(e * HD, HD), HD), :] = o
        return carry

    lax.fori_loop(0, HD, opm_e, 0)

    ex_m = Direct(me, lambda peer: m2_ref.at[:, pl.ds(pl.multiple_of(peer * HD, HD), HD), :], lambda owner: mrecv.at[owner], ds, dr, 0)
    mrecv[me] = m2_ref[:, pl.ds(pl.multiple_of(me * HD, HD), HD), :]
    ex_m.start([1, 2])

    def opm_i(i, carry):
        y_t = dot(opw[...], obuf[i]) * scr_x[pl.ds(i, 1), :]
        z1[i] = residual(z_ref[i], y_t.T)
        return carry

    lax.fori_loop(0, TI, opm_i, 0)

    def front(w_ref, z_src, ball, left_too):
        wt_l = twt
        wt_l[...] = transpose_bf(w_ref[0, :, 0:512])
        wg = w_ref[0, :, 512:640]

        def body(i, carry):
            xn = norm_lanes(z_src[i].astype(F32))
            mrow = pm_ref[pl.ds(i, 1), :]
            if left_too:
                pr = dot_nt(wt_l[...], xn)
                scr_a[pl.ds(i, RB, stride=TI), :] = mrow * jax.nn.sigmoid(pr[SQ:384]) * pr[0:RB]
                pb, pg = pr[RB:SQ], pr[384:512]
            else:
                pb = dot_nt(wt_l[RB:SQ, :], xn)
                pg = dot_nt(wt_l[384:512, :], xn)
            scr_b[pl.ds(i, RB, stride=TI), :] = mrow * jax.nn.sigmoid(pg) * pb
            gbuf[i] = jax.nn.sigmoid(dot(xn, wg))
            return carry

        lax.fori_loop(0, TI, body, 0)
        ball[me] = scr_b[...].astype(BF).reshape(RB, TI, RB)

    def finish(w_ref, z_src, z_dst):
        w = w_ref[0]

        def body(i, carry):
            xn = norm_rows(scr_x[pl.ds(i, RB, stride=TI), :])
            z_dst[i] = residual(z_src[i], gbuf[i] * dot_tn(xn, w))
            return carry

        lax.fori_loop(0, TI, body, 0)

    front(tmo_p, z1, ball1, True)
    ag1 = Chain(me, ball1, ch_s.at[1], ch_r.at[1])
    ag1.start()
    a_c[...] = scr_a[...].astype(BF).reshape(RB, TI, RB)
    ag1.finish()

    def out_c(cc, carry):
        for u in range(8):
            c = cc * 8 + u
            scr_x[pl.ds(pl.multiple_of(c * TI, TI), TI), :] = dot_nt(a_c[c], ball1[:, c].reshape(RB, RB))
        return carry

    lax.fori_loop(0, TI, out_c, 0)
    ex_m.start([3, 4])
    finish(tmo_o, z1, z1)

    ex_z1 = Direct(me, lambda peer: z1.at[:, pl.ds(pl.multiple_of(peer * TI, TI), TI), :], lambda owner: zcol.at[0, owner], ds, dr, 8)
    ex_z1.start()
    zcol[0, me] = z1[:, pl.ds(pl.multiple_of(me * TI, TI), TI), :]
    front(tmi_p, z1, ball2, False)
    ag2 = Chain(me, ball2, ch_s.at[2], ch_r.at[2])
    ag2.start()
    ex_z1.wait_recv()
    scr_b[...] = zcol[0].astype(F32).reshape(2048, RB)

    def in_left(i, carry):
        xn = norm_lanes(scr_b[pl.ds(i, RB, stride=TI), :])
        mrow = pt_ref[pl.ds(me * TI + i, 1), :]
        pa = dot_nt(twt[0:RB, :], xn)
        pg = dot_nt(twt[SQ:384, :], xn)
        scr_a[pl.ds(i, RB, stride=TI), :] = mrow * jax.nn.sigmoid(pg) * pa
        return carry

    lax.fori_loop(0, TI, in_left, 0)
    a_c[...] = scr_a[...].astype(BF).reshape(RB, TI, RB)
    ag2.finish()

    def in_c(cc, carry):
        for u in range(8):
            c = cc * 8 + u
            scr_x[pl.ds(pl.multiple_of(c * TI, TI), TI), :] = dot(a_c[c], ball2[:, c].reshape(RB, RB))
        return carry

    lax.fori_loop(0, TI, in_c, 0)
    ex_z1.wait_send()
    ex_m.start([5, 6, 7])
    finish(tmi_o, z1, z1)

    def tri_bias(w_ref, tile, slot, base):
        wb_t = transpose_bf(jnp.concatenate([w_ref[0], jnp.zeros((RB, 124), BF)], 1))[0:8]

        def body(i, carry):
            sbias[pl.ds(i, 8, stride=TI), :] = dot_nt(wb_t, norm_lanes(tile(i)))
            return carry

        lax.fori_loop(0, TI, body, 0)
        ball3[slot, me] = sbias[0:64, :].astype(BF).reshape(4, TI, RB)
        ex = Direct(me, lambda peer: ball3.at[slot, me], lambda owner: ball3.at[slot, owner], ds, dr, base)
        ex.start()
        return ex

    def take_bias(slot):
        for h in range(4):
            bias_t[h] = ball3[slot, :, h].reshape(RB, RB).astype(F32).T * LOG2E

    ex_s = tri_bias(tas_b, lambda i: z1[i].astype(F32), 0, TI)
    prep_qkvg(tas_w, wt, RB)
    ex_s.wait_recv()
    take_bias(0)
    tas_k = tas_w[0, :, RB:SQ]

    def tas_body(i, carry):
        x = z1[i]
        upd, = attend_tile(norm_lanes(x.astype(F32)), wt, tas_k, tas_o[0], 4, bias_t, column_of(pm_ref[pl.ds(i, 1), :]))
        z1[i] = residual(x, upd)
        return carry

    lax.fori_loop(0, TI, tas_body, 0)

    ex_z2 = Direct(me, lambda peer: z1.at[:, pl.ds(pl.multiple_of(peer * TI, TI), TI), :], lambda owner: zcol.at[1, owner], ds, dr, 24)
    ex_z2.start()
    zcol[1, me] = z1[:, pl.ds(pl.multiple_of(me * TI, TI), TI), :]
    prep_qkvg(tae_w, wt, RB)
    ex_z2.wait_recv()
    scr_b[...] = zcol[1].astype(F32).reshape(2048, RB)
    ex_e = tri_bias(tae_b, lambda i: scr_b[pl.ds(i, RB, stride=TI), :], 1, HD)
    ex_e.wait_recv()
    take_bias(1)
    tae_k = tae_w[0, :, RB:SQ]

    def tae_body(i, carry):
        x = scr_b[pl.ds(i, RB, stride=TI), :]
        upd, = attend_tile(norm_lanes(x), wt, tae_k, tae_o[0], 4, bias_t, column_of(pt_ref[pl.ds(me * TI + i, 1), :]))
        scr_a[pl.ds(i, RB, stride=TI), :] = x + upd
        return carry

    lax.fori_loop(0, TI, tae_body, 0)
    zsend[...] = scr_a[...].astype(BF).reshape(8, TI, TI, RB)
    ex_z3 = Direct(me, lambda peer: zsend.at[peer], lambda owner: z4.at[:, pl.ds(pl.multiple_of(owner * TI, TI), TI), :], ds, dr, 40)
    ex_z3.start()
    z4[:, pl.ds(pl.multiple_of(me * TI, TI), TI), :] = zsend[me]

    ex_m.wait_recv()

    def widen(d, carry):
        for half in range(2):
            part = mrecv[d, :, :, RB * half:RB * half + RB].astype(F32).reshape(512, RB)
            mscr[half, pl.ds(pl.multiple_of(d * 512, 512), 512), :] = part
        return carry

    lax.fori_loop(0, 8, widen, 0)

    def take_seq(s, carry):
        for half in range(2):
            mout_ref[s, :, RB * half:RB * half + RB] = mscr[half, pl.ds(s, RB, stride=HD), :].astype(BF)
        return carry

    lax.fori_loop(0, HD, take_seq, 0)
    ex_z3.wait_recv()

    def trans(i, carry):
        x = z4[i]
        hid = jnp.maximum(dot(norm_lanes(x.astype(F32)), ptr_i[0]), 0.0).astype(BF)
        zout_ref[i] = residual(x, dot(hid, ptr_o[0]))
        return carry

    lax.fori_loop(0, TI, trans, 0)
    for ex in (ag0, ag1, ag2, ex_m, ex_s, ex_e, ex_z2, ex_z3):
        ex.wait_send()


def full(shape):
    return pl.BlockSpec(shape, lambda g: (0,) * len(shape))


def layer_of(shape, layer):
    return pl.BlockSpec((1,) + shape[1:], lambda g: (layer,) + (0,) * (len(shape) - 1))


def params(cid):
    return pltpu.CompilerParams(collective_id=cid, has_side_effects=True, vmem_limit_bytes=VMEM_LIMIT)


def run_masks(mm, pm):
    outs = [(RB, SQ), (RB, RB)]
    return pl.pallas_call(
        mask_kernel,
        grid=(1,),
        out_shape=[jax.ShapeDtypeStruct(s, F32) for s in outs],
        in_specs=[full(mm.shape), full(pm.shape)],
        out_specs=[full(s) for s in outs],
        scratch_shapes=[pltpu.VMEM((ND, HD, RB), F32), pltpu.VMEM((ND, TI, RB), F32),
                        pltpu.SemaphoreType.DMA((TI,)), pltpu.SemaphoreType.DMA((TI,))],
        compiler_params=params(0),
    )(mm, pm)


def run_msa(layer, m, z, rmask, mt, weights):
    acts = (m, z, rmask, mt)
    outs = [(TI, SQ, SQ), (TI, HD, SQ), (HD, TI, SQ)]
    return pl.pallas_call(
        msa_kernel,
        grid=(1,),
        out_shape=[jax.ShapeDtypeStruct(s, BF) for s in outs],
        in_specs=[full(a.shape) for a in acts] + [layer_of(w.shape, layer) for w in weights],
        out_specs=[full(s) for s in outs],
        scratch_shapes=[
            pltpu.VMEM((8, TI, RB), BF),
            pltpu.VMEM((ND, 8, TI, RB), BF),
            pltpu.VMEM((8, RB, RB), F32),
            pltpu.VMEM((768, SQ), BF),
            pltpu.VMEM((64, SQ), BF),
            pltpu.VMEM((2, 2048, RB), F32),
            pltpu.VMEM((2, ND, TI, TI, SQ), BF),
            pltpu.VMEM((2 * ND, TI, TI, SQ), BF),
            pltpu.VMEM((RB, RB), F32),
            pltpu.SemaphoreType.DMA((24,)), pltpu.SemaphoreType.DMA((24,)),
        ],
        compiler_params=params(1 + 2 * layer),
    )(*acts, *weights)


def run_pair(layer, m2, at, bt, z, mt, pm, pt, weights):
    acts = (m2, at, bt, z, mt, pm, pt)
    outs = [(HD, RB, SQ), (TI, RB, RB)]
    return pl.pallas_call(
        pair_kernel,
        grid=(1,),
        out_shape=[jax.ShapeDtypeStruct(s, BF) for s in outs],
        in_specs=[full(a.shape) for a in acts] + [layer_of(w.shape, layer) for w in weights],
        out_specs=[full(s) for s in outs],
        scratch_shapes=[
            pltpu.VMEM((ND, HD, TI, SQ), BF),
            pltpu.VMEM((TI, 1024, RB), BF),
            pltpu.VMEM((RB, 1024), BF),
            pltpu.VMEM((2048, RB), F32),
            pltpu.VMEM((2048, RB), F32),
            pltpu.VMEM((2048, RB), F32),
            pltpu.VMEM((RB, TI, RB), BF),
            pltpu.VMEM((ND, RB, TI, RB), BF),
            pltpu.VMEM((ND, RB, TI, RB), BF),
            pltpu.VMEM((TI, RB, RB), F32),
            pltpu.VMEM((TI, RB, RB), BF),
            pltpu.VMEM((2, ND, TI, TI, RB), BF),
            pltpu.VMEM((RB, RB), F32),
            pltpu.VMEM((2, ND, 4, TI, RB), BF),
            pltpu.VMEM((4, RB, RB), F32),
            pltpu.VMEM((384, RB), BF),
            pltpu.VMEM((512, RB), BF),
            pltpu.VMEM((ND, TI, TI, RB), BF),
            pltpu.VMEM((TI, RB, RB), BF),
            pltpu.VMEM((ND, TI, HD, SQ), BF),
            pltpu.VMEM((2, 4096, RB), F32),
            pltpu.SemaphoreType.DMA((3, 13)), pltpu.SemaphoreType.DMA((3, 13)),
            pltpu.SemaphoreType.DMA((48,)), pltpu.SemaphoreType.DMA((48,)),
        ],
        compiler_params=params(2 + 2 * layer),
    )(*acts, *weights)


def solution(mesh):
    row_spec = P(('req', 'dap'))

    def local_body(m, z, mm, pm, *weights):
        (row_qkvg, row_bias, row_out, col_qkvg, col_out, mtr_in, mtr_out, opm_proj, opm_out) = weights[:9]
        mt, pt = run_masks(mm, pm)
        rmask = mm.astype(F32)
        pmask = pm.astype(F32)
        for layer in range(weights[0].shape[0]):
            m2, at, bt = run_msa(layer, m, z, rmask, mt, (row_qkvg, row_bias, row_out, col_qkvg, col_out, mtr_in, mtr_out, opm_proj))
            m, z = run_pair(layer, m2, at, bt, z, mt, pmask, pt, (opm_out,) + weights[9:])
        return m, z

    def run_blocks(*arrays):
        n_weights = len(arrays) - 4
        return jax.shard_map(local_body, mesh=mesh, in_specs=(row_spec,) * 4 + (P(),) * n_weights,
                             out_specs=(row_spec, row_spec), check_vma=False)(*arrays)

    return run_blocks
```

```python
import functools

import jax
import jax.numpy as jnp
from jax import lax
from jax.experimental import pallas as pl
from jax.experimental.pallas import tpu as pltpu
from jax.sharding import PartitionSpec as P

MESH = pl.DeviceIdType.MESH
F32 = jnp.float32
BF = jnp.bfloat16
LOG2E = 1.4426950408889634
NEG = -1e9 * LOG2E
ND = 8
VMEM_LIMIT = 66_000_000
RB = 128
SQ = 256
TI = 16
HD = 32


def dot(a, b):
    return lax.dot_general(a, b, (((1,), (0,)), ((), ())), preferred_element_type=F32)


def dot_nt(a, b):
    return lax.dot_general(a, b, (((1,), (1,)), ((), ())), preferred_element_type=F32)


def dot_tn(a, b):
    return lax.dot_general(a, b, (((0,), (0,)), ((), ())), preferred_element_type=F32)


def transpose_bf(w):
    return w.astype(F32).T.astype(BF)


def norm_lanes(x):
    mean = jnp.mean(x, axis=-1, keepdims=True)
    centered = x - mean
    var = jnp.mean(centered * centered, axis=-1, keepdims=True)
    return (centered * lax.rsqrt(var + 1e-5)).astype(BF)


def norm_rows(x):
    mean = jnp.mean(x, axis=0, keepdims=True)
    centered = x - mean
    var = jnp.mean(centered * centered, axis=0, keepdims=True)
    return (centered * lax.rsqrt(var + 1e-5)).astype(BF)


def residual(x, update):
    return (x.astype(F32) + update).astype(BF)


def group_barrier(me):
    sem = pltpu.get_barrier_semaphore()
    for p in range(1, ND):
        pl.semaphore_signal(sem, inc=1, device_id={'dap': lax.rem(me + p, ND)}, device_id_type=MESH)
    pl.semaphore_wait(sem, ND - 1)


def remote(src, dst, send_sem, recv_sem, peer):
    return pltpu.make_async_remote_copy(src_ref=src, dst_ref=dst, send_sem=send_sem, recv_sem=recv_sem,
                                        device_id={'dap': peer}, device_id_type=MESH)


class Direct:
    def __init__(self, me, src_of, dst_of, ssem, rsem, base=0):
        self.me, self.src_of, self.dst_of, self.ssem, self.rsem, self.base = me, src_of, dst_of, ssem, rsem, base

    def copy_to(self, p):
        peer = lax.rem(self.me + p, ND)
        return remote(self.src_of(peer), self.dst_of(self.me), self.ssem.at[self.base + p], self.rsem.at[self.base + p], peer)

    def start(self, ps=range(1, ND)):
        for p in ps:
            self.copy_to(p).start()

    def wait_recv(self):
        for p in range(1, ND):
            owner = lax.rem(self.me + ND - p, ND)
            remote(self.src_of(owner), self.dst_of(owner), self.ssem.at[self.base + p], self.rsem.at[self.base + p], owner).wait_recv()

    def wait_send(self):
        for p in range(1, ND):
            self.copy_to(p).wait_send()


class Chain:
    def __init__(self, me, buf, ssem, rsem):
        self.buf, self.ssem, self.rsem = buf, ssem, rsem
        self.z, self.c = lax.div(me, 2), lax.rem(me, 2)
        self.me, self.partner = me, me + 1 - 2 * self.c

    def cp(self, slot, peer, sem):
        return remote(self.buf.at[slot], self.buf.at[slot], self.ssem.at[sem], self.rsem.at[sem], peer)

    def slot(self, off, other=False):
        core = 1 - self.c if other else self.c
        return (self.z + off) * 2 + core

    def start(self):
        @pl.when(self.z < 3)
        def _():
            self.cp(self.me, self.me + 2, 0).start()

        @pl.when(self.z > 0)
        def _():
            self.cp(self.me, self.me - 2, 3).start()

        self.cp(self.me, self.partner, 6).start()

    def finish(self):
        z = self.z
        for t in range(1, 4):
            @pl.when(z >= t)
            def _():
                self.cp(self.slot(-t), self.me, t - 1).wait_recv()
                if t < 3:
                    @pl.when(z < 3)
                    def _():
                        self.cp(self.slot(-t), self.me + 2, t).start()
                self.cp(self.slot(-t), self.partner, 6 + t).start()

            @pl.when(z + t <= 3)
            def _():
                self.cp(self.slot(t), self.me, 3 + t - 1).wait_recv()
                if t < 3:
                    @pl.when(z > 0)
                    def _():
                        self.cp(self.slot(t), self.me - 2, 3 + t).start()
                self.cp(self.slot(t), self.partner, 9 + t).start()
        self.cp(self.partner, self.me, 6).wait_recv()
        for t in range(1, 4):
            @pl.when(z >= t)
            def _():
                self.cp(self.slot(-t, True), self.me, 6 + t).wait_recv()

            @pl.when(z + t <= 3)
            def _():
                self.cp(self.slot(t, True), self.me, 9 + t).wait_recv()

    def wait_send(self):
        z = self.z

        @pl.when(z < 3)
        def _():
            self.cp(self.me, self.me + 2, 0).wait_send()

        @pl.when(z > 0)
        def _():
            self.cp(self.me, self.me - 2, 3).wait_send()

        self.cp(self.me, self.partner, 6).wait_send()
        for t in range(1, 4):
            @pl.when(z >= t)
            def _():
                if t < 3:
                    @pl.when(z < 3)
                    def _():
                        self.cp(self.slot(-t), self.me + 2, t).wait_send()
                self.cp(self.slot(-t), self.partner, 6 + t).wait_send()

            @pl.when(z + t <= 3)
            def _():
                if t < 3:
                    @pl.when(z > 0)
                    def _():
                        self.cp(self.slot(t), self.me - 2, 3 + t).wait_send()
                self.cp(self.slot(t), self.partner, 9 + t).wait_send()


def column_of(row):
    return jnp.broadcast_to(row, (RB, row.shape[1])).T


def attend_tiles(xns, wt_ref, wk, w_out, heads, bias_ref, key_masks, depth):
    length = xns[0].shape[0]
    width = heads * HD
    projs = [dot_nt(wt_ref[...], xn) for xn in xns]
    keys = [dot(xn, wk).astype(BF) for xn in xns]
    q_t = [proj[:width].astype(BF) for proj in projs]
    v_t = [proj[width:2 * width].astype(BF) for proj in projs]
    gate = [jax.nn.sigmoid(proj[2 * width:].astype(BF).astype(F32)) for proj in projs]
    valid = [key_mask > 0 for key_mask in key_masks]
    scale = HD ** -0.5 * LOG2E

    def logits_of(unit):
        t, qc, h = unit
        hh = h % 4
        rhs = [q_t[t][HD * h:HD * h + HD, RB * qc:RB * qc + RB]]
        if hh > 0:
            rhs = [jnp.zeros((HD * hh, RB), BF)] + rhs
        if hh < 3:
            rhs = rhs + [jnp.zeros((96 - HD * hh, RB), BF)]
        return dot(keys[t][:, RB * (h // 4):RB * (h // 4) + RB], jnp.concatenate(rhs, 0))

    def prob_of(unit, raw):
        t, qc, h = unit
        logits = raw * scale
        if bias_ref is not None:
            logits = logits + bias_ref[h]
        logits = jnp.where(valid[t], logits, NEG)
        e = jnp.exp2(logits - jnp.max(logits, axis=0, keepdims=True))
        return (e * (1.0 / jnp.sum(e, axis=0, keepdims=True))).astype(BF)

    blocks = [(t, qc) for t in range(len(xns)) for qc in range(length // RB)]
    units = [(t, qc, h) for t, qc in blocks for h in range(heads)]
    raws = {i: logits_of(units[i]) for i in range(min(depth, len(units)))}
    outs, probs, upds = {}, {}, {}

    def flush(i):
        t, qc, h = units[i]
        outs[units[i]] = dot(v_t[t][HD * h:HD * h + HD], probs.pop(i))
        if h == heads - 1:
            o = jnp.concatenate([outs.pop((t, qc, hh)) for hh in range(heads)], 0)
            upds[t, qc] = (o * gate[t][:, RB * qc:RB * qc + RB]).astype(BF)

    for i in range(len(units)):
        if i + depth < len(units):
            raws[i + depth] = logits_of(units[i + depth])
        probs[i] = prob_of(units[i], raws.pop(i))
        if i > 0:
            flush(i - 1)
    flush(len(units) - 1)
    pieces = [dot_tn(upds[block], w_out) for block in blocks]
    per = length // RB
    return [jnp.concatenate(pieces[t * per:t * per + per], 0) for t in range(len(xns))]


def tile_loop(count, width, body):
    def step(g, carry):
        body([g * width + u for u in range(width)])
        return carry

    lax.fori_loop(0, count // width, step, 0)


def prep_qkvg(w_ref, wt_ref, width):
    wt_ref[0:width, :] = transpose_bf(w_ref[0, :, 0:width])
    wt_ref[width:3 * width, :] = transpose_bf(w_ref[0, :, 2 * width:4 * width])


def mask_kernel(mm_ref, pm_ref, mt_ref, pt_ref, mbuf, pbuf, ssem, rsem):
    me = lax.axis_index('dap')
    group_barrier(me)
    mbuf[me] = mm_ref[...].astype(F32)
    pbuf[me] = pm_ref[...].astype(F32)
    ex_m = Direct(me, lambda peer: mbuf.at[me], lambda owner: mbuf.at[owner], ssem, rsem, 0)
    ex_p = Direct(me, lambda peer: pbuf.at[me], lambda owner: pbuf.at[owner], ssem, rsem, ND)
    ex_m.start()
    ex_p.start()
    ex_m.wait_recv()
    ex_p.wait_recv()
    mt_ref[...] = mbuf[...].reshape(SQ, RB).T
    pt_ref[...] = pbuf[...].reshape(RB, RB).T
    ex_m.wait_send()
    ex_p.wait_send()


def msa_kernel(m_ref, z_ref, rmask_ref, mt_ref, row_w, row_b, row_o, col_w, col_o, mtr_i, mtr_o, opm_p,
               m2_ref, at_ref, bt_ref,
               bloc, ball, bias_t, wt, opt, scr, sendbuf, rbuf, bscr, ssem, rsem):
    me = lax.axis_index('dap')
    group_barrier(me)
    wb = jnp.concatenate([row_b[0], jnp.zeros((RB, 120), BF)], 1)
    wb_t = transpose_bf(wb)[0:8]

    def bias_row(tiles):
        rows = [dot_nt(wb_t, norm_lanes(z_ref[i].astype(F32))) for i in tiles]
        for i, row in zip(tiles, rows):
            bscr[pl.ds(i, 8, stride=TI), :] = row

    tile_loop(TI, 8, bias_row)
    ball[me] = bscr[...].astype(BF).reshape(8, TI, RB)
    ex_b = Direct(me, lambda peer: ball.at[me], lambda owner: ball.at[owner], ssem, rsem, 0)
    ex_b.start()
    prep_qkvg(row_w, wt, SQ)
    opt[...] = transpose_bf(jnp.concatenate([opm_p[0], jnp.zeros((SQ, 64), BF)], 1))[0:64]
    ex_b.wait_recv()
    for h in range(8):
        bias_t[h] = ball[:, h].reshape(RB, RB).astype(F32).T * LOG2E
    row_k = row_w[0, :, SQ:512]
    row_ow = row_o[0]
    for ck in range(2):
        def row_body(sls):
            xs = [m_ref[ck * TI + sl] for sl in sls]
            masks = [column_of(rmask_ref[pl.ds(ck * TI + sl, 1), :]) for sl in sls]
            xns = [norm_lanes(x.astype(F32)) for x in xs]
            upds = attend_tiles(xns, wt, row_k, row_ow, 8, bias_t, masks, 4)
            for sl, x, upd in zip(sls, xs, upds):
                y = residual(x, upd).astype(F32)
                for half in range(2):
                    scr[half, pl.ds(sl, RB, stride=TI), :] = y[:, RB * half:RB * half + RB]

        tile_loop(TI, 2, row_body)

        def pack(d, carry):
            for half in range(2):
                part = scr[half, pl.ds(pl.multiple_of(d * SQ, SQ), SQ), :].astype(BF).reshape(TI, TI, RB)
                sendbuf[ck, d, :, :, RB * half:RB * half + RB] = part
            return carry

        lax.fori_loop(0, 8, pack, 0)
        rbuf[me * 2 + ck] = sendbuf[ck, me]
        if ck == 0:
            ex0 = Direct(me, lambda peer: sendbuf.at[0, peer], lambda owner: rbuf.at[owner * 2], ssem, rsem, ND)
            ex0.start()

    def quarter(q):
        part = pl.ds(pl.multiple_of(q * 4, 4), 4)
        return Direct(me, lambda peer: sendbuf.at[1, peer, part], lambda owner: rbuf.at[owner * 2 + 1, part], ssem, rsem, ND * 2 + q * ND)

    for q in range(4):
        quarter(q).start()
    ex_b.wait_send()
    prep_qkvg(col_w, wt, SQ)
    ex0.wait_recv()
    col_k = col_w[0, :, SQ:512]
    col_ow = col_o[0]

    def col_body(rs):
        xs = [rbuf[:, r].reshape(SQ, SQ) for r in rs]
        mrows = [mt_ref[pl.ds(me * TI + r, 1), :] for r in rs]
        masks = [column_of(mrow) for mrow in mrows]
        upds = attend_tiles([norm_lanes(x.astype(F32)) for x in xs], wt, col_k, col_ow, 8, None, masks, 2)
        for r, x, upd in zip(rs, xs, upds):
            m2_ref[r] = residual(x, upd)

    def mtr_body(rs):
        ys = [m2_ref[r] for r in rs]
        mrows = [mt_ref[pl.ds(me * TI + r, 1), :] for r in rs]
        xns = [norm_lanes(y.astype(F32)) for y in ys]
        hids = [jnp.maximum(dot(xn, mtr_i[0]), 0.0).astype(BF) for xn in xns]
        y2s = [residual(y, dot(hid, mtr_o[0])) for y, hid in zip(ys, hids)]
        xns = [norm_lanes(y2.astype(F32)) for y2 in y2s]
        abs_ = [dot_nt(opt[...], xn).astype(BF).astype(F32) * mrow for xn, mrow in zip(xns, mrows)]
        for r, y2, ab in zip(rs, y2s, abs_):
            m2_ref[r] = y2
            at_ref[r] = ab[0:HD].astype(BF)
            for half in range(2):
                scr[half, pl.ds(r, HD, stride=TI), :] = ab[HD:2 * HD, RB * half:RB * half + RB]

    def col_quarter(q, carry):
        quarter(q).wait_recv()
        tile_loop(4, 1, lambda rs: col_body([q * 4 + r for r in rs]))
        tile_loop(4, 2, lambda rs: mtr_body([q * 4 + r for r in rs]))
        return carry

    lax.fori_loop(0, 4, col_quarter, 0)
    for half in range(2):
        bt_ref[:, :, RB * half:RB * half + RB] = scr[half, 0:512, :].astype(BF).reshape(HD, TI, RB)
    for ex in [ex0] + [quarter(q) for q in range(4)]:
        ex.wait_send()


def pair_kernel(m2_ref, at_ref, bt_ref, z_ref, mt_ref, pm_ref, pt_ref,
                opm_o, tmo_p, tmo_o, tmi_p, tmi_o, tas_w, tas_b, tas_o, tae_w, tae_b, tae_o, ptr_i, ptr_o,
                mout_ref, zout_ref,
                btall, obuf, opw, scr_a, scr_b, scr_x, a_c, ball1, ball2, gbuf, z1, zcol, sbias, ball3, bias_t,
                wt, twt, zsend, z4, mrecv, mscr,
                ch_s, ch_r, ds, dr):
    me = lax.axis_index('dap')
    group_barrier(me)
    btall[me] = bt_ref[...]
    ag0 = Chain(me, btall, ch_s.at[0], ch_r.at[0])
    ag0.start()
    scr_a[0:1024, :] = opm_o[0].astype(F32)

    def perm(e, carry):
        rows = scr_a[pl.ds(e, HD, stride=HD), :]
        scr_b[pl.ds(pl.multiple_of(e * HD, HD), HD), :] = rows
        return carry

    lax.fori_loop(0, HD, perm, 0)
    for q in range(8):
        opw[:, RB * q:RB * q + RB] = scr_b[RB * q:RB * q + RB, :].T.astype(BF)
    mloc = mt_ref[pl.ds(pl.multiple_of(me * TI, TI), TI), :].astype(BF)
    inv_over = 1.0 / (1e-3 + dot_nt(mloc, mt_ref[...].astype(BF)))
    scr_x[0:TI, :] = inv_over
    ag0.finish()

    left = at_ref[...].reshape(512, SQ)

    def opm_e(es):
        rhs = [btall[:, e].reshape(RB, SQ) for e in es]
        os_ = [dot_nt(left, r).astype(BF).reshape(TI, HD, RB) for r in rhs]
        for e, o in zip(es, os_):
            obuf[:, pl.ds(pl.multiple_of(e * HD, HD), HD), :] = o

    tile_loop(HD, 2, opm_e)

    ex_m = Direct(me, lambda peer: m2_ref.at[:, pl.ds(pl.multiple_of(peer * HD, HD), HD), :], lambda owner: mrecv.at[owner], ds, dr, 0)
    mrecv[me] = m2_ref[:, pl.ds(pl.multiple_of(me * HD, HD), HD), :]
    ex_m.start([1, 2])

    def opm_i(tiles):
        y_ts = [dot(opw[...], obuf[i]) * scr_x[pl.ds(i, 1), :] for i in tiles]
        outs = [residual(z_ref[i], y_t.T) for i, y_t in zip(tiles, y_ts)]
        for i, out in zip(tiles, outs):
            z1[i] = out

    tile_loop(TI, 4, opm_i)

    def front(w_ref, z_src, ball, left_too):
        wt_l = twt
        wt_l[...] = transpose_bf(w_ref[0, :, 0:512])
        wg = w_ref[0, :, 512:640]

        def body(tiles):
            xns = [norm_lanes(z_src[i].astype(F32)) for i in tiles]
            mrows = [pm_ref[pl.ds(i, 1), :] for i in tiles]
            if left_too:
                prs = [dot_nt(wt_l[...], xn) for xn in xns]
                lefts = [mrow * jax.nn.sigmoid(pr[SQ:384]) * pr[0:RB] for mrow, pr in zip(mrows, prs)]
                pbs = [pr[RB:SQ] for pr in prs]
                pgs = [pr[384:512] for pr in prs]
            else:
                lefts = []
                pbs = [dot_nt(wt_l[RB:SQ, :], xn) for xn in xns]
                pgs = [dot_nt(wt_l[384:512, :], xn) for xn in xns]
            gates = [dot(xn, wg) for xn in xns]
            rights = [mrow * jax.nn.sigmoid(pg) * pb for mrow, pg, pb in zip(mrows, pgs, pbs)]
            gates = [jax.nn.sigmoid(g) for g in gates]
            for i, left in zip(tiles, lefts):
                scr_a[pl.ds(i, RB, stride=TI), :] = left
            for i, right, gate in zip(tiles, rights, gates):
                scr_b[pl.ds(i, RB, stride=TI), :] = right
                gbuf[i] = gate

        tile_loop(TI, 4, body)
        ball[me] = scr_b[...].astype(BF).reshape(RB, TI, RB)

    def finish(w_ref, z_src, z_dst):
        w = w_ref[0]

        def body(tiles):
            xns = [norm_rows(scr_x[pl.ds(i, RB, stride=TI), :]) for i in tiles]
            ys = [dot_tn(xn, w) for xn in xns]
            outs = [residual(z_src[i], gbuf[i] * y) for i, y in zip(tiles, ys)]
            for i, out in zip(tiles, outs):
                z_dst[i] = out

        tile_loop(TI, 4, body)

    front(tmo_p, z1, ball1, True)
    ag1 = Chain(me, ball1, ch_s.at[1], ch_r.at[1])
    ag1.start()
    a_c[...] = scr_a[...].astype(BF).reshape(RB, TI, RB)
    ag1.finish()

    def out_c(cc, carry):
        for u in range(8):
            c = cc * 8 + u
            scr_x[pl.ds(pl.multiple_of(c * TI, TI), TI), :] = dot_nt(a_c[c], ball1[:, c].reshape(RB, RB))
        return carry

    lax.fori_loop(0, TI, out_c, 0)
    ex_m.start([3, 4])
    finish(tmo_o, z1, z1)

    ex_z1 = Direct(me, lambda peer: z1.at[:, pl.ds(pl.multiple_of(peer * TI, TI), TI), :], lambda owner: zcol.at[0, owner], ds, dr, 8)
    ex_z1.start()
    zcol[0, me] = z1[:, pl.ds(pl.multiple_of(me * TI, TI), TI), :]
    front(tmi_p, z1, ball2, False)
    ag2 = Chain(me, ball2, ch_s.at[2], ch_r.at[2])
    ag2.start()
    ex_z1.wait_recv()
    scr_b[...] = zcol[0].astype(F32).reshape(2048, RB)

    def in_left(tiles):
        xns = [norm_lanes(scr_b[pl.ds(i, RB, stride=TI), :]) for i in tiles]
        mrows = [pt_ref[pl.ds(me * TI + i, 1), :] for i in tiles]
        pas = [dot_nt(twt[0:RB, :], xn) for xn in xns]
        pgs = [dot_nt(twt[SQ:384, :], xn) for xn in xns]
        lefts = [mrow * jax.nn.sigmoid(pg) * pa for mrow, pg, pa in zip(mrows, pgs, pas)]
        for i, left in zip(tiles, lefts):
            scr_a[pl.ds(i, RB, stride=TI), :] = left

    tile_loop(TI, 4, in_left)
    a_c[...] = scr_a[...].astype(BF).reshape(RB, TI, RB)
    ag2.finish()

    def in_c(cc, carry):
        for u in range(8):
            c = cc * 8 + u
            scr_x[pl.ds(pl.multiple_of(c * TI, TI), TI), :] = dot(a_c[c], ball2[:, c].reshape(RB, RB))
        return carry

    lax.fori_loop(0, TI, in_c, 0)
    ex_z1.wait_send()
    ex_m.start([5, 6, 7])
    finish(tmi_o, z1, z1)

    def tri_bias(w_ref, tile, slot, base):
        wb_t = transpose_bf(jnp.concatenate([w_ref[0], jnp.zeros((RB, 124), BF)], 1))[0:8]

        def body(tiles):
            rows = [dot_nt(wb_t, norm_lanes(tile(i))) for i in tiles]
            for i, row in zip(tiles, rows):
                sbias[pl.ds(i, 8, stride=TI), :] = row

        tile_loop(TI, 8, body)
        ball3[slot, me] = sbias[0:64, :].astype(BF).reshape(4, TI, RB)
        ex = Direct(me, lambda peer: ball3.at[slot, me], lambda owner: ball3.at[slot, owner], ds, dr, base)
        ex.start()
        return ex

    def take_bias(slot):
        for h in range(4):
            bias_t[h] = ball3[slot, :, h].reshape(RB, RB).astype(F32).T * LOG2E

    ex_s = tri_bias(tas_b, lambda i: z1[i].astype(F32), 0, TI)
    prep_qkvg(tas_w, wt, RB)
    ex_s.wait_recv()
    take_bias(0)
    tas_k = tas_w[0, :, RB:SQ]

    def tas_body(tiles):
        xs = [z1[i] for i in tiles]
        masks = [column_of(pm_ref[pl.ds(i, 1), :]) for i in tiles]
        upds = attend_tiles([norm_lanes(x.astype(F32)) for x in xs], wt, tas_k, tas_o[0], 4, bias_t, masks, 4)
        for i, x, upd in zip(tiles, xs, upds):
            z1[i] = residual(x, upd)

    tile_loop(TI, 4, tas_body)

    ex_z2 = Direct(me, lambda peer: z1.at[:, pl.ds(pl.multiple_of(peer * TI, TI), TI), :], lambda owner: zcol.at[1, owner], ds, dr, 24)
    ex_z2.start()
    zcol[1, me] = z1[:, pl.ds(pl.multiple_of(me * TI, TI), TI), :]
    prep_qkvg(tae_w, wt, RB)
    ex_z2.wait_recv()
    scr_b[...] = zcol[1].astype(F32).reshape(2048, RB)
    ex_e = tri_bias(tae_b, lambda i: scr_b[pl.ds(i, RB, stride=TI), :], 1, HD)
    ex_e.wait_recv()
    take_bias(1)
    tae_k = tae_w[0, :, RB:SQ]

    def tae_body(tiles):
        xs = [scr_b[pl.ds(i, RB, stride=TI), :] for i in tiles]
        masks = [column_of(pt_ref[pl.ds(me * TI + i, 1), :]) for i in tiles]
        upds = attend_tiles([norm_lanes(x) for x in xs], wt, tae_k, tae_o[0], 4, bias_t, masks, 4)
        for i, x, upd in zip(tiles, xs, upds):
            scr_a[pl.ds(i, RB, stride=TI), :] = x + upd

    tile_loop(TI, 4, tae_body)
    zsend[...] = scr_a[...].astype(BF).reshape(8, TI, TI, RB)
    ex_z3 = Direct(me, lambda peer: zsend.at[peer], lambda owner: z4.at[:, pl.ds(pl.multiple_of(owner * TI, TI), TI), :], ds, dr, 40)
    ex_z3.start()
    z4[:, pl.ds(pl.multiple_of(me * TI, TI), TI), :] = zsend[me]

    ex_m.wait_recv()

    def widen(d, carry):
        for half in range(2):
            part = mrecv[d, :, :, RB * half:RB * half + RB].astype(F32).reshape(512, RB)
            mscr[half, pl.ds(pl.multiple_of(d * 512, 512), 512), :] = part
        return carry

    lax.fori_loop(0, 8, widen, 0)

    def take_seq(seqs):
        for s in seqs:
            for half in range(2):
                mout_ref[s, :, RB * half:RB * half + RB] = mscr[half, pl.ds(s, RB, stride=HD), :].astype(BF)

    tile_loop(HD, 4, take_seq)
    ex_z3.wait_recv()

    def trans(tiles):
        xs = [z4[i] for i in tiles]
        xns = [norm_lanes(x.astype(F32)) for x in xs]
        hids = [jnp.maximum(dot(xn, ptr_i[0]), 0.0).astype(BF) for xn in xns]
        outs = [residual(x, dot(hid, ptr_o[0])) for x, hid in zip(xs, hids)]
        for i, out in zip(tiles, outs):
            zout_ref[i] = out

    tile_loop(TI, 4, trans)
    for ex in (ag0, ag1, ag2, ex_m, ex_s, ex_e, ex_z2, ex_z3):
        ex.wait_send()


def full(shape):
    return pl.BlockSpec(shape, lambda g: (0,) * len(shape))


def layer_of(shape, layer):
    return pl.BlockSpec((1,) + shape[1:], lambda g: (layer,) + (0,) * (len(shape) - 1))


def params(cid):
    return pltpu.CompilerParams(collective_id=cid, has_side_effects=True, vmem_limit_bytes=VMEM_LIMIT)


def run_masks(mm, pm):
    outs = [(RB, SQ), (RB, RB)]
    return pl.pallas_call(
        mask_kernel,
        grid=(1,),
        out_shape=[jax.ShapeDtypeStruct(s, F32) for s in outs],
        in_specs=[full(mm.shape), full(pm.shape)],
        out_specs=[full(s) for s in outs],
        scratch_shapes=[pltpu.VMEM((ND, HD, RB), F32), pltpu.VMEM((ND, TI, RB), F32),
                        pltpu.SemaphoreType.DMA((TI,)), pltpu.SemaphoreType.DMA((TI,))],
        compiler_params=params(0),
    )(mm, pm)


def run_msa(layer, m, z, rmask, mt, weights):
    acts = (m, z, rmask, mt)
    outs = [(TI, SQ, SQ), (TI, HD, SQ), (HD, TI, SQ)]
    return pl.pallas_call(
        msa_kernel,
        grid=(1,),
        out_shape=[jax.ShapeDtypeStruct(s, BF) for s in outs],
        in_specs=[full(a.shape) for a in acts] + [layer_of(w.shape, layer) for w in weights],
        out_specs=[full(s) for s in outs],
        scratch_shapes=[
            pltpu.VMEM((8, TI, RB), BF),
            pltpu.VMEM((ND, 8, TI, RB), BF),
            pltpu.VMEM((8, RB, RB), F32),
            pltpu.VMEM((768, SQ), BF),
            pltpu.VMEM((64, SQ), BF),
            pltpu.VMEM((2, 2048, RB), F32),
            pltpu.VMEM((2, ND, TI, TI, SQ), BF),
            pltpu.VMEM((2 * ND, TI, TI, SQ), BF),
            pltpu.VMEM((RB, RB), F32),
            pltpu.SemaphoreType.DMA((48,)), pltpu.SemaphoreType.DMA((48,)),
        ],
        compiler_params=params(1 + 2 * layer),
    )(*acts, *weights)


def run_pair(layer, m2, at, bt, z, mt, pm, pt, weights):
    acts = (m2, at, bt, z, mt, pm, pt)
    outs = [(HD, RB, SQ), (TI, RB, RB)]
    return pl.pallas_call(
        pair_kernel,
        grid=(1,),
        out_shape=[jax.ShapeDtypeStruct(s, BF) for s in outs],
        in_specs=[full(a.shape) for a in acts] + [layer_of(w.shape, layer) for w in weights],
        out_specs=[full(s) for s in outs],
        scratch_shapes=[
            pltpu.VMEM((ND, HD, TI, SQ), BF),
            pltpu.VMEM((TI, 1024, RB), BF),
            pltpu.VMEM((RB, 1024), BF),
            pltpu.VMEM((2048, RB), F32),
            pltpu.VMEM((2048, RB), F32),
            pltpu.VMEM((2048, RB), F32),
            pltpu.VMEM((RB, TI, RB), BF),
            pltpu.VMEM((ND, RB, TI, RB), BF),
            pltpu.VMEM((ND, RB, TI, RB), BF),
            pltpu.VMEM((TI, RB, RB), F32),
            pltpu.VMEM((TI, RB, RB), BF),
            pltpu.VMEM((2, ND, TI, TI, RB), BF),
            pltpu.VMEM((RB, RB), F32),
            pltpu.VMEM((2, ND, 4, TI, RB), BF),
            pltpu.VMEM((4, RB, RB), F32),
            pltpu.VMEM((384, RB), BF),
            pltpu.VMEM((512, RB), BF),
            pltpu.VMEM((ND, TI, TI, RB), BF),
            pltpu.VMEM((TI, RB, RB), BF),
            pltpu.VMEM((ND, TI, HD, SQ), BF),
            pltpu.VMEM((2, 4096, RB), F32),
            pltpu.SemaphoreType.DMA((3, 13)), pltpu.SemaphoreType.DMA((3, 13)),
            pltpu.SemaphoreType.DMA((48,)), pltpu.SemaphoreType.DMA((48,)),
        ],
        compiler_params=params(2 + 2 * layer),
    )(*acts, *weights)


def solution(mesh):
    row_spec = P(('req', 'dap'))

    def local_body(m, z, mm, pm, *weights):
        (row_qkvg, row_bias, row_out, col_qkvg, col_out, mtr_in, mtr_out, opm_proj, opm_out) = weights[:9]
        mt, pt = run_masks(mm, pm)
        rmask = mm.astype(F32)
        pmask = pm.astype(F32)
        for layer in range(weights[0].shape[0]):
            m2, at, bt = run_msa(layer, m, z, rmask, mt, (row_qkvg, row_bias, row_out, col_qkvg, col_out, mtr_in, mtr_out, opm_proj))
            m, z = run_pair(layer, m2, at, bt, z, mt, pmask, pt, (opm_out,) + weights[9:])
        return m, z

    def run_blocks(*arrays):
        n_weights = len(arrays) - 4
        return jax.shard_map(local_body, mesh=mesh, in_specs=(row_spec,) * 4 + (P(),) * n_weights,
                             out_specs=(row_spec, row_spec), check_vma=False)(*arrays)

    return run_blocks
```

```python
import jax
import jax.numpy as jnp
from jax import lax
from jax.experimental import pallas as pl
from jax.experimental.pallas import tpu as pltpu
from jax.sharding import PartitionSpec as P

MESH = pl.DeviceIdType.MESH
F32 = jnp.float32
BF = jnp.bfloat16
LOG2E = 1.4426950408889634
NEG = -1e9 * LOG2E
ND = 8
VMEM_LIMIT = 66_000_000
RB = 128
SQ = 256
TI = 16
HD = 32


def dot(a, b):
    return lax.dot_general(a, b, (((1,), (0,)), ((), ())), preferred_element_type=F32)


def dot_nt(a, b):
    return lax.dot_general(a, b, (((1,), (1,)), ((), ())), preferred_element_type=F32)


def dot_tn(a, b):
    return lax.dot_general(a, b, (((0,), (0,)), ((), ())), preferred_element_type=F32)


def transpose_bf(w):
    return w.astype(F32).T.astype(BF)


def norm_lanes(x):
    mean = jnp.mean(x, axis=-1, keepdims=True)
    centered = x - mean
    var = jnp.mean(centered * centered, axis=-1, keepdims=True)
    return (centered * lax.rsqrt(var + 1e-5)).astype(BF)


def norm_rows(x):
    mean = jnp.mean(x, axis=0, keepdims=True)
    centered = x - mean
    var = jnp.mean(centered * centered, axis=0, keepdims=True)
    return (centered * lax.rsqrt(var + 1e-5)).astype(BF)


def residual(x, update):
    return (x.astype(F32) + update).astype(BF)


def group_barrier(me):
    sem = pltpu.get_barrier_semaphore()
    for p in range(1, ND):
        pl.semaphore_signal(sem, inc=1, device_id={'dap': lax.rem(me + p, ND)}, device_id_type=MESH)
    pl.semaphore_wait(sem, ND - 1)


def remote(src, dst, send_sem, recv_sem, peer):
    return pltpu.make_async_remote_copy(src_ref=src, dst_ref=dst, send_sem=send_sem, recv_sem=recv_sem,
                                        device_id={'dap': peer}, device_id_type=MESH)


class Direct:
    def __init__(self, me, src_of, dst_of, ssem, rsem, base=0):
        self.me, self.src_of, self.dst_of, self.ssem, self.rsem, self.base = me, src_of, dst_of, ssem, rsem, base

    def copy_to(self, p):
        peer = lax.rem(self.me + p, ND)
        return remote(self.src_of(peer), self.dst_of(self.me), self.ssem.at[self.base + p], self.rsem.at[self.base + p], peer)

    def start(self, ps=range(1, ND)):
        for p in ps:
            self.copy_to(p).start()

    def wait_recv(self):
        for p in range(1, ND):
            owner = lax.rem(self.me + ND - p, ND)
            remote(self.src_of(owner), self.dst_of(owner), self.ssem.at[self.base + p], self.rsem.at[self.base + p], owner).wait_recv()

    def wait_send(self):
        for p in range(1, ND):
            self.copy_to(p).wait_send()


class Chain:
    def __init__(self, me, buf, ssem, rsem):
        self.buf, self.ssem, self.rsem = buf, ssem, rsem
        self.z, self.c = lax.div(me, 2), lax.rem(me, 2)
        self.me, self.partner = me, me + 1 - 2 * self.c
        self.size = buf.shape[1] // 2

    def cp(self, slot, peer, sem, half):
        ref = self.buf.at[slot, pl.ds(half * self.size, self.size)]
        return remote(ref, ref, self.ssem.at[half, sem], self.rsem.at[half, sem], peer)

    def slot(self, off, other=False):
        core = 1 - self.c if other else self.c
        return (self.z + off) * 2 + core

    def own(self, act):
        for half in range(2):
            @pl.when(self.z < 3)
            def _():
                act(self.cp(self.me, self.me + 2, 0, half))

            @pl.when(self.z > 0)
            def _():
                act(self.cp(self.me, self.me - 2, 3, half))

        for half in range(2):
            act(self.cp(self.me, self.partner, 6, half))

    def forward(self, t, half, before, act):
        z = self.z

        @pl.when(z >= t)
        def _():
            if before:
                before(self.cp(self.slot(-t), self.me, t - 1, half))
            if t < 3:
                @pl.when(z < 3)
                def _():
                    act(self.cp(self.slot(-t), self.me + 2, t, half))
            act(self.cp(self.slot(-t), self.partner, 6 + t, half))

        @pl.when(z + t <= 3)
        def _():
            if before:
                before(self.cp(self.slot(t), self.me, 2 + t, half))
            if t < 3:
                @pl.when(z > 0)
                def _():
                    act(self.cp(self.slot(t), self.me - 2, 3 + t, half))
            act(self.cp(self.slot(t), self.partner, 9 + t, half))

    def start(self):
        self.own(lambda c: c.start())

    def finish(self, hook=None):
        z = self.z
        for t in range(1, 4):
            for half in range(2):
                self.forward(t, half, lambda c: c.wait_recv(), lambda c: c.start())
            if hook is not None:
                hook(t)
        for half in range(2):
            self.cp(self.partner, self.me, 6, half).wait_recv()
            for t in range(1, 4):
                @pl.when(z >= t)
                def _():
                    self.cp(self.slot(-t, True), self.me, 6 + t, half).wait_recv()

                @pl.when(z + t <= 3)
                def _():
                    self.cp(self.slot(t, True), self.me, 9 + t, half).wait_recv()

    def wait_send(self):
        self.own(lambda c: c.wait_send())
        for t in range(1, 4):
            for half in range(2):
                self.forward(t, half, None, lambda c: c.wait_send())


class Return:
    def __init__(self, me, src, dst, ssem, rsem):
        self.me, self.src, self.dst, self.ssem, self.rsem = me, src, dst, ssem, rsem
        self.z, self.c = lax.div(me, 2), lax.rem(me, 2)

    def copy_to(self, off, core):
        peer = (self.z + off) * 2 + core
        return remote(self.src(peer), self.dst(self.me), self.ssem.at[(off + 3) * 2 + core], self.rsem.at[(off + 3) * 2 + self.c], peer)

    def start(self, off, cond, cores=(0, 1)):
        @pl.when(cond)
        def _():
            for core in cores:
                self.copy_to(off, core).start()

    def start_partner(self):
        self.copy_to(0, 1 - self.c).start()

    def each(self, fn):
        fn(0, 1 - self.c)
        for off in (-3, -2, -1, 1, 2, 3):
            @pl.when(jnp.logical_and(self.z + off >= 0, self.z + off <= 3))
            def _():
                for core in range(2):
                    fn(off, core)

    def wait_recv(self):
        def one(off, core):
            owner = (self.z + off) * 2 + core
            sem = (3 - off) * 2 + core
            remote(self.src(self.me), self.dst(owner), self.ssem.at[sem], self.rsem.at[sem], self.me).wait_recv()

        self.each(one)

    def wait_send(self):
        self.each(lambda off, core: self.copy_to(off, core).wait_send())


def column_of(row):
    return jnp.broadcast_to(row, (RB, row.shape[1])).T


def attend_tiles(xns, wt_ref, wk, w_out, heads, bias_ref, key_masks, depth):
    length = xns[0].shape[0]
    width = heads * HD
    projs = [dot_nt(wt_ref[...], xn) for xn in xns]
    keys = [dot(xn, wk).astype(BF) for xn in xns]
    q_t = [proj[:width].astype(BF) for proj in projs]
    v_t = [proj[width:2 * width].astype(BF) for proj in projs]
    gate = [jax.nn.sigmoid(proj[2 * width:].astype(BF).astype(F32)) for proj in projs]
    valid = [key_mask > 0 for key_mask in key_masks]
    scale = HD ** -0.5 * LOG2E

    def logits_of(unit):
        t, qc, h = unit
        hh = h % 4
        rhs = [q_t[t][HD * h:HD * h + HD, RB * qc:RB * qc + RB]]
        if hh > 0:
            rhs = [jnp.zeros((HD * hh, RB), BF)] + rhs
        if hh < 3:
            rhs = rhs + [jnp.zeros((96 - HD * hh, RB), BF)]
        return dot(keys[t][:, RB * (h // 4):RB * (h // 4) + RB], jnp.concatenate(rhs, 0))

    def prob_of(unit, raw):
        t, qc, h = unit
        logits = raw * scale
        if bias_ref is not None:
            logits = logits + bias_ref[h]
        logits = jnp.where(valid[t], logits, NEG)
        e = jnp.exp2(logits - jnp.max(logits, axis=0, keepdims=True))
        return (e * (1.0 / jnp.sum(e, axis=0, keepdims=True))).astype(BF)

    blocks = [(t, qc) for t in range(len(xns)) for qc in range(length // RB)]
    units = [(t, qc, h) for t, qc in blocks for h in range(heads)]
    raws = {i: logits_of(units[i]) for i in range(min(depth, len(units)))}
    outs, probs, upds = {}, {}, {}

    def flush(i):
        t, qc, h = units[i]
        outs[units[i]] = dot(v_t[t][HD * h:HD * h + HD], probs.pop(i))
        if h == heads - 1:
            o = jnp.concatenate([outs.pop((t, qc, hh)) for hh in range(heads)], 0)
            upds[t, qc] = (o * gate[t][:, RB * qc:RB * qc + RB]).astype(BF)

    for i in range(len(units)):
        if i + depth < len(units):
            raws[i + depth] = logits_of(units[i + depth])
        probs[i] = prob_of(units[i], raws.pop(i))
        if i > 0:
            flush(i - 1)
    flush(len(units) - 1)
    pieces = [dot_tn(upds[block], w_out) for block in blocks]
    per = length // RB
    return [jnp.concatenate(pieces[t * per:t * per + per], 0) for t in range(len(xns))]


def tile_loop(count, width, body):
    def step(g, carry):
        body([g * width + u for u in range(width)])
        return carry

    lax.fori_loop(0, count // width, step, 0)


def prep_qkvg(w_ref, wt_ref, width):
    wt_ref[0:width, :] = transpose_bf(w_ref[0, :, 0:width])
    wt_ref[width:3 * width, :] = transpose_bf(w_ref[0, :, 2 * width:4 * width])


def blocks_kernel(m_in, z_in, mm_ref, pm_in,
                  row_w, row_bt, row_o, col_w, col_o, mtr_i, mtr_o, opt, opm_o,
                  tmo_p, tmo_o, tmi_p, tmi_o, tas_w, tas_bt, tas_o, tae_w, tae_bt, tae_o, ptr_i, ptr_o,
                  mout_ref, zout_ref,
                  mbuf, pbuf, mt_ref, pt_ref, rmask_ref, pm_ref,
                  ball, bias_t, wt, scr, sendbuf, rbuf, bscr, m2_ref, at_ref,
                  btall, obuf, opw, scr_a, scr_b, scr_x, a_c, ball1, ball2, gbuf, z1, zcol, sbias, ball3,
                  wt2, twt, zsend, z4, mrecv, mscr,
                  ssem, rsem, ch_s, ch_r, ms, mr):
    me = lax.axis_index('dap')
    chip = lax.div(me, 2)
    first = pl.program_id(0) == 0
    group_barrier(me)
    ex_k = [Direct(me, lambda peer, buf=buf: buf.at[me], lambda owner, buf=buf: buf.at[owner], ssem, rsem, base)
            for buf, base in ((mbuf, 104), (pbuf, 112))]

    @pl.when(first)
    def _():
        rmask_ref[...] = mm_ref[...].astype(F32)
        pm_ref[...] = pm_in[...].astype(F32)
        mbuf[me] = rmask_ref[...]
        pbuf[me] = pm_ref[...]
        for ex in ex_k:
            ex.start()

        def take(s, carry):
            mout_ref[s] = m_in[s]
            return carry

        lax.fori_loop(0, HD, take, 0)
        zout_ref[...] = z_in[...]

    m_ref, z_ref = mout_ref, zout_ref
    wb_t = row_bt[0]

    def bias_row(tiles):
        rows = [dot_nt(wb_t, norm_lanes(z_ref[i].astype(F32))) for i in tiles]
        for i, row in zip(tiles, rows):
            bscr[pl.ds(i, 8, stride=TI), :] = row

    tile_loop(TI, 8, bias_row)
    ball[me] = bscr[...].astype(BF).reshape(8, TI, RB)
    ex_b = Direct(me, lambda peer: ball.at[me], lambda owner: ball.at[owner], ssem, rsem, TI)
    ex_b.start()
    prep_qkvg(row_w, wt, SQ)

    @pl.when(first)
    def _():
        for ex in ex_k:
            ex.wait_recv()
        mt_ref[...] = mbuf[...].reshape(SQ, RB).T
        pt_ref[...] = pbuf[...].reshape(RB, RB).T
        for ex in ex_k:
            ex.wait_send()

    ex_b.wait_recv()
    for h in range(8):
        bias_t[h] = ball[:, h].reshape(RB, RB).astype(F32).T * LOG2E
    row_k = row_w[0, :, SQ:512]
    row_ow = row_o[0]
    for ck in range(2):
        def row_body(sls):
            xs = [m_ref[ck * TI + sl] for sl in sls]
            masks = [column_of(rmask_ref[pl.ds(ck * TI + sl, 1), :]) for sl in sls]
            xns = [norm_lanes(x.astype(F32)) for x in xs]
            upds = attend_tiles(xns, wt, row_k, row_ow, 8, bias_t, masks, 4)
            for sl, x, upd in zip(sls, xs, upds):
                y = residual(x, upd).astype(F32)
                for half in range(2):
                    scr[half, pl.ds(sl, RB, stride=TI), :] = y[:, RB * half:RB * half + RB]

        tile_loop(TI, 2, row_body)

        def pack(d, carry):
            for half in range(2):
                part = scr[half, pl.ds(pl.multiple_of(d * SQ, SQ), SQ), :].astype(BF).reshape(TI, TI, RB)
                sendbuf[ck, d, :, :, RB * half:RB * half + RB] = part
            return carry

        lax.fori_loop(0, 8, pack, 0)
        rbuf[me * 2 + ck] = sendbuf[ck, me]
        if ck == 0:
            ex0 = Direct(me, lambda peer: sendbuf.at[0, peer], lambda owner: rbuf.at[owner * 2], ssem, rsem, 24)
            ex0.start()

    def quarter(q):
        part = pl.ds(pl.multiple_of(q * 4, 4), 4)
        return Direct(me, lambda peer: sendbuf.at[1, peer, part], lambda owner: rbuf.at[owner * 2 + 1, part], ssem, rsem, HD + q * ND)

    for q in range(4):
        quarter(q).start()
    ex_b.wait_send()
    prep_qkvg(col_w, wt, SQ)
    ex0.wait_recv()
    col_k = col_w[0, :, SQ:512]
    col_ow = col_o[0]

    def col_body(rs):
        xs = [rbuf[:, r].reshape(SQ, SQ) for r in rs]
        mrows = [mt_ref[pl.ds(me * TI + r, 1), :] for r in rs]
        masks = [column_of(mrow) for mrow in mrows]
        upds = attend_tiles([norm_lanes(x.astype(F32)) for x in xs], wt, col_k, col_ow, 8, None, masks, 2)
        for r, x, upd in zip(rs, xs, upds):
            m2_ref[r] = residual(x, upd)

    def mtr_body(rs):
        ys = [m2_ref[r] for r in rs]
        mrows = [mt_ref[pl.ds(me * TI + r, 1), :] for r in rs]
        xns = [norm_lanes(y.astype(F32)) for y in ys]
        hids = [jnp.maximum(dot(xn, mtr_i[0]), 0.0).astype(BF) for xn in xns]
        y2s = [residual(y, dot(hid, mtr_o[0])) for y, hid in zip(ys, hids)]
        xns = [norm_lanes(y2.astype(F32)) for y2 in y2s]
        abs_ = [dot_nt(opt[0], xn).astype(BF).astype(F32) * mrow for xn, mrow in zip(xns, mrows)]
        for r, y2, ab in zip(rs, y2s, abs_):
            m2_ref[r] = y2
            at_ref[r] = ab[0:HD].astype(BF)
            for half in range(2):
                scr[half, pl.ds(r, HD, stride=TI), :] = ab[HD:2 * HD, RB * half:RB * half + RB]

    def col_quarter(q, carry):
        quarter(q).wait_recv()
        tile_loop(4, 1, lambda rs: col_body([q * 4 + r for r in rs]))
        tile_loop(4, 2, lambda rs: mtr_body([q * 4 + r for r in rs]))
        return carry

    lax.fori_loop(0, 4, col_quarter, 0)
    for half in range(2):
        btall[me, :, :, RB * half:RB * half + RB] = scr[half, 0:512, :].astype(BF).reshape(HD, TI, RB)
    ag0 = Chain(me, btall, ch_s.at[0], ch_r.at[0])
    ag0.start()
    scr_a[0:1024, :] = opm_o[0].astype(F32)

    def perm(e, carry):
        rows = scr_a[pl.ds(e, HD, stride=HD), :]
        scr_b[pl.ds(pl.multiple_of(e * HD, HD), HD), :] = rows
        return carry

    lax.fori_loop(0, HD, perm, 0)
    for q in range(8):
        opw[:, RB * q:RB * q + RB] = scr_b[RB * q:RB * q + RB, :].T.astype(BF)
    mloc = mt_ref[pl.ds(pl.multiple_of(me * TI, TI), TI), :].astype(BF)
    inv_over = 1.0 / (1e-3 + dot_nt(mloc, mt_ref[...].astype(BF)))
    scr_x[0:TI, :] = inv_over
    ag0.finish()
    ret = Return(me, lambda peer: m2_ref.at[:, pl.ds(pl.multiple_of(peer * HD, HD), HD), :], lambda owner: mrecv.at[owner], ms, mr)
    ret.start(3, chip == 0)
    ret.start(-3, chip == 3)
    mrecv[me] = m2_ref[:, pl.ds(pl.multiple_of(me * HD, HD), HD), :]

    left = at_ref[...].reshape(512, SQ)

    def opm_e(es):
        rhs = [btall[:, e].reshape(RB, SQ) for e in es]
        os_ = [dot_nt(left, r).astype(BF).reshape(TI, HD, RB) for r in rhs]
        for e, o in zip(es, os_):
            obuf[:, pl.ds(pl.multiple_of(e * HD, HD), HD), :] = o

    tile_loop(HD, 2, opm_e)

    def opm_i(tiles):
        y_ts = [dot(opw[...], obuf[i]) * scr_x[pl.ds(i, 1), :] for i in tiles]
        outs = [residual(z_ref[i], y_t.T) for i, y_t in zip(tiles, y_ts)]
        for i, out in zip(tiles, outs):
            z1[i] = out

    tile_loop(TI, 4, opm_i)

    def front(w_ref, z_src, ball, left_too):
        wt_l = twt
        wt_l[...] = transpose_bf(w_ref[0, :, 0:512])
        wg = w_ref[0, :, 512:640]

        def body(tiles):
            xns = [norm_lanes(z_src[i].astype(F32)) for i in tiles]
            mrows = [pm_ref[pl.ds(i, 1), :] for i in tiles]
            if left_too:
                prs = [dot_nt(wt_l[...], xn) for xn in xns]
                lefts = [mrow * jax.nn.sigmoid(pr[SQ:384]) * pr[0:RB] for mrow, pr in zip(mrows, prs)]
                pbs = [pr[RB:SQ] for pr in prs]
                pgs = [pr[384:512] for pr in prs]
            else:
                lefts = []
                pbs = [dot_nt(wt_l[RB:SQ, :], xn) for xn in xns]
                pgs = [dot_nt(wt_l[384:512, :], xn) for xn in xns]
            gates = [dot(xn, wg) for xn in xns]
            rights = [mrow * jax.nn.sigmoid(pg) * pb for mrow, pg, pb in zip(mrows, pgs, pbs)]
            gates = [jax.nn.sigmoid(g) for g in gates]
            for i, left in zip(tiles, lefts):
                scr_a[pl.ds(i, RB, stride=TI), :] = left
            for i, right, gate in zip(tiles, rights, gates):
                scr_b[pl.ds(i, RB, stride=TI), :] = right
                gbuf[i] = gate

        tile_loop(TI, 4, body)
        ball[me] = scr_b[...].astype(BF).reshape(RB, TI, RB)

    def finish(w_ref, z_src, z_dst):
        w = w_ref[0]

        def body(tiles):
            xns = [norm_rows(scr_x[pl.ds(i, RB, stride=TI), :]) for i in tiles]
            ys = [dot_tn(xn, w) for xn in xns]
            outs = [residual(z_src[i], gbuf[i] * y) for i, y in zip(tiles, ys)]
            for i, out in zip(tiles, outs):
                z_dst[i] = out

        tile_loop(TI, 4, body)

    front(tmo_p, z1, ball1, True)
    ag1 = Chain(me, ball1, ch_s.at[1], ch_r.at[1])
    ag1.start()
    ret.start(1, chip == 0)
    ret.start(-1, chip == 3)
    ret.start_partner()
    a_c[...] = scr_a[...].astype(BF).reshape(RB, TI, RB)

    def inner(t):
        if t == 1:
            ret.start(1, chip == 1)
            ret.start(-1, chip == 2)

    ag1.finish(inner)

    def out_c(cc, carry):
        for u in range(8):
            c = cc * 8 + u
            scr_x[pl.ds(pl.multiple_of(c * TI, TI), TI), :] = dot_nt(a_c[c], ball1[:, c].reshape(RB, RB))
        return carry

    lax.fori_loop(0, TI, out_c, 0)
    ret.start(1, chip == 2, (0,))
    ret.start(-1, chip == 1, (0,))
    finish(tmo_o, z1, z1)

    ex_z1 = Direct(me, lambda peer: z1.at[:, pl.ds(pl.multiple_of(peer * TI, TI), TI), :], lambda owner: zcol.at[0, owner], ssem, rsem, 64)
    ex_z1.start()
    zcol[0, me] = z1[:, pl.ds(pl.multiple_of(me * TI, TI), TI), :]
    front(tmi_p, z1, ball2, False)
    ag2 = Chain(me, ball2, ch_s.at[2], ch_r.at[2])
    ag2.start()
    ex_z1.wait_recv()
    scr_b[...] = zcol[0].astype(F32).reshape(2048, RB)

    def in_left(tiles):
        xns = [norm_lanes(scr_b[pl.ds(i, RB, stride=TI), :]) for i in tiles]
        mrows = [pt_ref[pl.ds(me * TI + i, 1), :] for i in tiles]
        pas = [dot_nt(twt[0:RB, :], xn) for xn in xns]
        pgs = [dot_nt(twt[SQ:384, :], xn) for xn in xns]
        lefts = [mrow * jax.nn.sigmoid(pg) * pa for mrow, pg, pa in zip(mrows, pgs, pas)]
        for i, left in zip(tiles, lefts):
            scr_a[pl.ds(i, RB, stride=TI), :] = left

    tile_loop(TI, 4, in_left)
    a_c[...] = scr_a[...].astype(BF).reshape(RB, TI, RB)

    def two(t):
        if t == 2:
            ret.start(2, chip == 0)
            ret.start(-2, chip == 3)

    ag2.finish(two)

    def in_c(cc, carry):
        for u in range(8):
            c = cc * 8 + u
            scr_x[pl.ds(pl.multiple_of(c * TI, TI), TI), :] = dot(a_c[c], ball2[:, c].reshape(RB, RB))
        return carry

    lax.fori_loop(0, TI, in_c, 0)
    ex_z1.wait_send()
    ret.start(1, chip == 2, (1,))
    ret.start(-1, chip == 1, (1,))
    finish(tmi_o, z1, z1)

    def send_bias(slot, base):
        ball3[slot, me] = sbias[0:64, :].astype(BF).reshape(4, TI, RB)
        ex = Direct(me, lambda peer: ball3.at[slot, me], lambda owner: ball3.at[slot, owner], ssem, rsem, base)
        ex.start()
        return ex

    def tas_bias(tiles):
        rows = [dot_nt(tas_bt[0], norm_lanes(z1[i].astype(F32))) for i in tiles]
        for i, row in zip(tiles, rows):
            sbias[pl.ds(i, 4, stride=TI), :] = row

    tile_loop(TI, 8, tas_bias)
    ex_s = send_bias(0, 72)
    prep_qkvg(tas_w, wt2, RB)
    ex_s.wait_recv()
    for h in range(4):
        bias_t[h] = ball3[0, :, h].reshape(RB, RB).astype(F32).T * LOG2E
    ret.start(2, chip == 1, (0,))
    ret.start(-2, chip == 2, (0,))
    tas_k = tas_w[0, :, RB:SQ]

    def tas_body(tiles):
        xs = [z1[i] for i in tiles]
        masks = [column_of(pm_ref[pl.ds(i, 1), :]) for i in tiles]
        upds = attend_tiles([norm_lanes(x.astype(F32)) for x in xs], wt2, tas_k, tas_o[0], 4, bias_t, masks, 4)
        outs = [residual(x, upd) for x, upd in zip(xs, upds)]
        rows = [dot_nt(tae_bt[0], norm_lanes(out.astype(F32))) for out in outs]
        for i, out, row in zip(tiles, outs, rows):
            z1[i] = out
            sbias[pl.ds(i, 4, stride=TI), :] = row

    tile_loop(TI, 4, tas_body)

    ex_z2 = Direct(me, lambda peer: z1.at[:, pl.ds(pl.multiple_of(peer * TI, TI), TI), :], lambda owner: zcol.at[1, owner], ssem, rsem, 80)
    ex_z2.start()
    ex_e = send_bias(1, 88)
    zcol[1, me] = z1[:, pl.ds(pl.multiple_of(me * TI, TI), TI), :]
    prep_qkvg(tae_w, wt2, RB)
    ex_z2.wait_recv()
    scr_b[...] = zcol[1].astype(F32).reshape(2048, RB)
    ex_e.wait_recv()
    for h in range(4):
        bias_t[h] = ball3[1, :, h].reshape(RB, RB).astype(F32) * LOG2E
    ret.start(2, chip == 1, (1,))
    ret.start(-2, chip == 2, (1,))
    tae_k = tae_w[0, :, RB:SQ]

    def tae_body(tiles):
        xs = [scr_b[pl.ds(i, RB, stride=TI), :] for i in tiles]
        masks = [column_of(pt_ref[pl.ds(me * TI + i, 1), :]) for i in tiles]
        upds = attend_tiles([norm_lanes(x) for x in xs], wt2, tae_k, tae_o[0], 4, bias_t, masks, 4)
        for i, x, upd in zip(tiles, xs, upds):
            scr_a[pl.ds(i, RB, stride=TI), :] = x + upd

    tile_loop(TI, 4, tae_body)
    zsend[...] = scr_a[...].astype(BF).reshape(8, TI, TI, RB)
    ex_z3 = Direct(me, lambda peer: zsend.at[peer], lambda owner: z4.at[:, pl.ds(pl.multiple_of(owner * TI, TI), TI), :], ssem, rsem, 96)
    ex_z3.start()
    z4[:, pl.ds(pl.multiple_of(me * TI, TI), TI), :] = zsend[me]

    ret.wait_recv()

    def widen(d, carry):
        for half in range(2):
            part = mrecv[d, :, :, RB * half:RB * half + RB].astype(F32).reshape(512, RB)
            mscr[half, pl.ds(pl.multiple_of(d * 512, 512), 512), :] = part
        return carry

    lax.fori_loop(0, 8, widen, 0)

    def take_seq(seqs):
        for s in seqs:
            for half in range(2):
                mout_ref[s, :, RB * half:RB * half + RB] = mscr[half, pl.ds(s, RB, stride=HD), :].astype(BF)

    tile_loop(HD, 4, take_seq)
    ex_z3.wait_recv()

    def trans(tiles):
        xs = [z4[i] for i in tiles]
        xns = [norm_lanes(x.astype(F32)) for x in xs]
        hids = [jnp.maximum(dot(xn, ptr_i[0]), 0.0).astype(BF) for xn in xns]
        outs = [residual(x, dot(hid, ptr_o[0])) for x, hid in zip(xs, hids)]
        for i, out in zip(tiles, outs):
            zout_ref[i] = out

    tile_loop(TI, 4, trans)
    for ex in [ex0] + [quarter(q) for q in range(4)] + [ag0, ag1, ag2, ret, ex_s, ex_e, ex_z2, ex_z3]:
        ex.wait_send()


def full(shape):
    return pl.BlockSpec(shape, lambda g: (0,) * len(shape))


def layer_of(shape):
    return pl.BlockSpec((1,) + shape[1:], lambda g: (g,) + (0,) * (len(shape) - 1))


def run(m, z, mm, pm, weights):
    acts = (m, z, mm, pm)
    outs = [(HD, RB, SQ), (TI, RB, RB)]
    vm = pltpu.VMEM
    return pl.pallas_call(
        blocks_kernel,
        grid=(weights[0].shape[0],),
        out_shape=[jax.ShapeDtypeStruct(s, BF) for s in outs],
        in_specs=[full(a.shape) for a in acts] + [layer_of(w.shape) for w in weights],
        out_specs=[full(s) for s in outs],
        scratch_shapes=[
            vm((ND, HD, RB), F32), vm((ND, TI, RB), F32), vm((RB, SQ), F32), vm((RB, RB), F32), vm((HD, RB), F32), vm((TI, RB), F32),
            vm((ND, 8, TI, RB), BF), vm((8, RB, RB), F32), vm((768, SQ), BF), vm((2, 2048, RB), F32),
            vm((2, ND, TI, TI, SQ), BF), vm((2 * ND, TI, TI, SQ), BF), vm((RB, RB), F32), vm((TI, SQ, SQ), BF), vm((TI, HD, SQ), BF),
            vm((ND, HD, TI, SQ), BF), vm((TI, 1024, RB), BF), vm((RB, 1024), BF),
            vm((2048, RB), F32), vm((2048, RB), F32), vm((2048, RB), F32),
            vm((RB, TI, RB), BF), vm((ND, RB, TI, RB), BF), vm((ND, RB, TI, RB), BF), vm((TI, RB, RB), F32), vm((TI, RB, RB), BF),
            vm((2, ND, TI, TI, RB), BF), vm((RB, RB), F32), vm((2, ND, 4, TI, RB), BF),
            vm((384, RB), BF), vm((512, RB), BF), vm((ND, TI, TI, RB), BF), vm((TI, RB, RB), BF),
            vm((ND, TI, HD, SQ), BF), vm((2, 4096, RB), F32),
            pltpu.SemaphoreType.DMA((120,)), pltpu.SemaphoreType.DMA((120,)),
            pltpu.SemaphoreType.DMA((3, 2, 13)), pltpu.SemaphoreType.DMA((3, 2, 13)),
            pltpu.SemaphoreType.DMA((14,)), pltpu.SemaphoreType.DMA((14,)),
        ],
        compiler_params=pltpu.CompilerParams(collective_id=0, has_side_effects=True, vmem_limit_bytes=VMEM_LIMIT),
    )(*acts, *weights)


def solution(mesh):
    row_spec = P(('req', 'dap'))

    def local_body(m, z, mm, pm, *weights):
        weights = [jnp.swapaxes(w, 1, 2) if k in (1, 7, 14, 17) else w for k, w in enumerate(weights)]
        return tuple(run(m, z, mm, pm, weights))

    def run_blocks(*arrays):
        n_weights = len(arrays) - 4
        return jax.shard_map(local_body, mesh=mesh, in_specs=(row_spec,) * 4 + (P(),) * n_weights,
                             out_specs=(row_spec, row_spec), check_vma=False)(*arrays)

    return run_blocks
```

```python
import jax
import jax.numpy as jnp
from jax import lax
from jax.experimental import pallas as pl
from jax.experimental.pallas import tpu as pltpu
from jax.sharding import PartitionSpec as P

MESH = pl.DeviceIdType.MESH
F32 = jnp.float32
BF = jnp.bfloat16
LOG2E = 1.4426950408889634
NEG = -1e9 * LOG2E
ND = 8
VMEM_LIMIT = 66_000_000
RB = 128
SQ = 256
TI = 16
HD = 32


def dot(a, b):
    return lax.dot_general(a, b, (((1,), (0,)), ((), ())), preferred_element_type=F32)


def dot_nt(a, b):
    return lax.dot_general(a, b, (((1,), (1,)), ((), ())), preferred_element_type=F32)


def dot_tn(a, b):
    return lax.dot_general(a, b, (((0,), (0,)), ((), ())), preferred_element_type=F32)


def transpose_bf(w):
    return w.astype(F32).T.astype(BF)


def norm_lanes(x):
    mean = jnp.mean(x, axis=-1, keepdims=True)
    centered = x - mean
    var = jnp.mean(centered * centered, axis=-1, keepdims=True)
    return (centered * lax.rsqrt(var + 1e-5)).astype(BF)


def norm_rows(x):
    mean = jnp.mean(x, axis=0, keepdims=True)
    centered = x - mean
    var = jnp.mean(centered * centered, axis=0, keepdims=True)
    return (centered * lax.rsqrt(var + 1e-5)).astype(BF)


def residual(x, update):
    return (x.astype(F32) + update).astype(BF)


def group_barrier(me):
    sem = pltpu.get_barrier_semaphore()
    for p in range(1, ND):
        pl.semaphore_signal(sem, inc=1, device_id={'dap': lax.rem(me + p, ND)}, device_id_type=MESH)
    pl.semaphore_wait(sem, ND - 1)


def remote(src, dst, send_sem, recv_sem, peer):
    return pltpu.make_async_remote_copy(src_ref=src, dst_ref=dst, send_sem=send_sem, recv_sem=recv_sem,
                                        device_id={'dap': peer}, device_id_type=MESH)


class Direct:
    def __init__(self, me, src_of, dst_of, ssem, rsem, base=0):
        self.me, self.src_of, self.dst_of, self.ssem, self.rsem, self.base = me, src_of, dst_of, ssem, rsem, base

    def copy_to(self, p):
        peer = lax.rem(self.me + p, ND)
        return remote(self.src_of(peer), self.dst_of(self.me), self.ssem.at[self.base + p], self.rsem.at[self.base + p], peer)

    def start(self, ps=range(1, ND)):
        for p in ps:
            self.copy_to(p).start()

    def wait_recv(self):
        for p in range(1, ND):
            owner = lax.rem(self.me + ND - p, ND)
            remote(self.src_of(owner), self.dst_of(owner), self.ssem.at[self.base + p], self.rsem.at[self.base + p], owner).wait_recv()

    def wait_send(self):
        for p in range(1, ND):
            self.copy_to(p).wait_send()


class Chain:
    def __init__(self, me, buf, ssem, rsem):
        self.buf, self.ssem, self.rsem = buf, ssem, rsem
        self.z, self.c = lax.div(me, 2), lax.rem(me, 2)
        self.me, self.partner = me, me + 1 - 2 * self.c
        self.size = buf.shape[1] // 2

    def cp(self, slot, peer, sem, half):
        ref = self.buf.at[slot, pl.ds(half * self.size, self.size)]
        return remote(ref, ref, self.ssem.at[half, sem], self.rsem.at[half, sem], peer)

    def slot(self, off, other=False):
        core = 1 - self.c if other else self.c
        return (self.z + off) * 2 + core

    def own(self, act):
        for half in range(2):
            @pl.when(self.z < 3)
            def _():
                act(self.cp(self.me, self.me + 2, 0, half))

            @pl.when(self.z > 0)
            def _():
                act(self.cp(self.me, self.me - 2, 3, half))

        for half in range(2):
            act(self.cp(self.me, self.partner, 6, half))

    def forward(self, t, half, before, act):
        z = self.z

        @pl.when(z >= t)
        def _():
            if before:
                before(self.cp(self.slot(-t), self.me, t - 1, half))
            if t < 3:
                @pl.when(z < 3)
                def _():
                    act(self.cp(self.slot(-t), self.me + 2, t, half))
            act(self.cp(self.slot(-t), self.partner, 6 + t, half))

        @pl.when(z + t <= 3)
        def _():
            if before:
                before(self.cp(self.slot(t), self.me, 2 + t, half))
            if t < 3:
                @pl.when(z > 0)
                def _():
                    act(self.cp(self.slot(t), self.me - 2, 3 + t, half))
            act(self.cp(self.slot(t), self.partner, 9 + t, half))

    def start(self):
        self.own(lambda c: c.start())

    def finish(self, hook=None):
        z = self.z
        for t in range(1, 4):
            for half in range(2):
                self.forward(t, half, lambda c: c.wait_recv(), lambda c: c.start())
            if hook is not None:
                hook(t)
        for half in range(2):
            self.cp(self.partner, self.me, 6, half).wait_recv()
            for t in range(1, 4):
                @pl.when(z >= t)
                def _():
                    self.cp(self.slot(-t, True), self.me, 6 + t, half).wait_recv()

                @pl.when(z + t <= 3)
                def _():
                    self.cp(self.slot(t, True), self.me, 9 + t, half).wait_recv()

    def stream(self, process, hook):
        z = self.z

        def take(t, other):
            for sign, cond in ((-1, z >= t), (1, z + t <= 3)):
                @pl.when(cond)
                def _():
                    if other:
                        for half in range(2):
                            self.cp(self.slot(sign * t, True), self.me, (6 if sign < 0 else 9) + t, half).wait_recv()
                    process(self.slot(sign * t, other))

        for t in range(1, 4):
            for half in range(2):
                self.forward(t, half, lambda c: c.wait_recv(), lambda c: c.start())
            hook(t)
            if t == 1:
                for half in range(2):
                    self.cp(self.partner, self.me, 6, half).wait_recv()
                process(self.partner)
            else:
                take(t - 1, True)
            take(t, False)
        take(3, True)

    def wait_send(self):
        self.own(lambda c: c.wait_send())
        for t in range(1, 4):
            for half in range(2):
                self.forward(t, half, None, lambda c: c.wait_send())


class Return:
    def __init__(self, me, src, dst, ssem, rsem):
        self.me, self.src, self.dst, self.ssem, self.rsem = me, src, dst, ssem, rsem
        self.z, self.c = lax.div(me, 2), lax.rem(me, 2)

    def copy_to(self, off, core):
        peer = (self.z + off) * 2 + core
        return remote(self.src(peer), self.dst(self.me), self.ssem.at[(off + 3) * 2 + core], self.rsem.at[(off + 3) * 2 + self.c], peer)

    def start(self, off, cond, cores=(0, 1)):
        @pl.when(cond)
        def _():
            for core in cores:
                self.copy_to(off, core).start()

    def start_partner(self):
        self.copy_to(0, 1 - self.c).start()

    def each(self, fn):
        fn(0, 1 - self.c)
        for off in (-3, -2, -1, 1, 2, 3):
            @pl.when(jnp.logical_and(self.z + off >= 0, self.z + off <= 3))
            def _():
                for core in range(2):
                    fn(off, core)

    def wait_recv(self):
        def one(off, core):
            owner = (self.z + off) * 2 + core
            sem = (3 - off) * 2 + core
            remote(self.src(self.me), self.dst(owner), self.ssem.at[sem], self.rsem.at[sem], self.me).wait_recv()

        self.each(one)

    def wait_send(self):
        self.each(lambda off, core: self.copy_to(off, core).wait_send())


def column_of(row):
    return jnp.broadcast_to(row, (RB, row.shape[1])).T


def attend_tiles(xns, wt_ref, wk, w_out, heads, bias_ref, key_masks, depth):
    length = xns[0].shape[0]
    width = heads * HD
    projs = [dot_nt(wt_ref[...], xn) for xn in xns]
    keys = [dot(xn, wk).astype(BF) for xn in xns]
    q_t = [proj[:width].astype(BF) for proj in projs]
    v_t = [proj[width:2 * width].astype(BF) for proj in projs]
    gate = [jax.nn.sigmoid(proj[2 * width:].astype(BF).astype(F32)) for proj in projs]
    valid = [key_mask > 0 for key_mask in key_masks]
    scale = HD ** -0.5 * LOG2E

    def logits_of(unit):
        t, qc, h = unit
        hh = h % 4
        rhs = [q_t[t][HD * h:HD * h + HD, RB * qc:RB * qc + RB]]
        if hh > 0:
            rhs = [jnp.zeros((HD * hh, RB), BF)] + rhs
        if hh < 3:
            rhs = rhs + [jnp.zeros((96 - HD * hh, RB), BF)]
        return dot(keys[t][:, RB * (h // 4):RB * (h // 4) + RB], jnp.concatenate(rhs, 0))

    def prob_of(unit, raw):
        t, qc, h = unit
        logits = raw * scale
        if bias_ref is not None:
            logits = logits + bias_ref[h]
        logits = jnp.where(valid[t], logits, NEG)
        e = jnp.exp2(logits - jnp.max(logits, axis=0, keepdims=True))
        return (e * (1.0 / jnp.sum(e, axis=0, keepdims=True))).astype(BF)

    blocks = [(t, qc) for t in range(len(xns)) for qc in range(length // RB)]
    units = [(t, qc, h) for t, qc in blocks for h in range(heads)]
    raws = {i: logits_of(units[i]) for i in range(min(depth, len(units)))}
    outs, probs, upds = {}, {}, {}

    def flush(i):
        t, qc, h = units[i]
        outs[units[i]] = dot(v_t[t][HD * h:HD * h + HD], probs.pop(i))
        if h == heads - 1:
            o = jnp.concatenate([outs.pop((t, qc, hh)) for hh in range(heads)], 0)
            upds[t, qc] = (o * gate[t][:, RB * qc:RB * qc + RB]).astype(BF)

    for i in range(len(units)):
        if i + depth < len(units):
            raws[i + depth] = logits_of(units[i + depth])
        probs[i] = prob_of(units[i], raws.pop(i))
        if i > 0:
            flush(i - 1)
    flush(len(units) - 1)
    pieces = [dot_tn(upds[block], w_out) for block in blocks]
    per = length // RB
    return [jnp.concatenate(pieces[t * per:t * per + per], 0) for t in range(len(xns))]


def tile_loop(count, width, body):
    def step(g, carry):
        body([g * width + u for u in range(width)])
        return carry

    lax.fori_loop(0, count // width, step, 0)


def prep_qkvg(w_ref, wt_ref, width):
    wt_ref[0:width, :] = transpose_bf(w_ref[0, :, 0:width])
    wt_ref[width:3 * width, :] = transpose_bf(w_ref[0, :, 2 * width:4 * width])


def blocks_kernel(m_in, z_in, mm_ref, pm_in,
                  row_w, row_bt, row_o, col_w, col_o, mtr_i, mtr_o, opt, opm_o,
                  tmo_p, tmo_o, tmi_p, tmi_o, tas_w, tas_bt, tas_o, tae_w, tae_bt, tae_o, ptr_i, ptr_o,
                  mout_ref, zout_ref,
                  mbuf, pbuf, mt_ref, pt_ref, rmask_ref, pm_ref,
                  ball, bias_t, wt, scr, sendbuf, rbuf, bscr, m2_ref, at_ref,
                  btall, obuf, opw, scr_a, scr_b, scr_x, a_c, ball1, ball2, gbuf, z1, zcol, sbias, ball3,
                  wt2, twt, twt2, zall, zsend, z4, mrecv, mscr,
                  ssem, rsem, ch_s, ch_r, ms, mr):
    me = lax.axis_index('dap')
    chip = lax.div(me, 2)
    first = pl.program_id(0) == 0
    group_barrier(me)
    ex_k = [Direct(me, lambda peer, buf=buf: buf.at[me], lambda owner, buf=buf: buf.at[owner], ssem, rsem, base)
            for buf, base in ((mbuf, 0), (pbuf, 8))]

    @pl.when(first)
    def _():
        rmask_ref[...] = mm_ref[...].astype(F32)
        pm_ref[...] = pm_in[...].astype(F32)
        mbuf[me] = rmask_ref[...]
        pbuf[me] = pm_ref[...]
        for ex in ex_k:
            ex.start()

        def take(s, carry):
            mout_ref[s] = m_in[s]
            return carry

        lax.fori_loop(0, HD, take, 0)
        zout_ref[...] = z_in[...]

    m_ref, z_ref = mout_ref, zout_ref
    wb_t = row_bt[0]

    def bias_row(tiles):
        rows = [dot_nt(wb_t, norm_lanes(z_ref[i].astype(F32))) for i in tiles]
        for i, row in zip(tiles, rows):
            bscr[pl.ds(i, 8, stride=TI), :] = row

    tile_loop(TI, 8, bias_row)
    ball[me] = bscr[...].astype(BF).reshape(8, TI, RB)
    ex_b = Direct(me, lambda peer: ball.at[me], lambda owner: ball.at[owner], ssem, rsem, TI)
    ex_b.start()
    prep_qkvg(row_w, wt, SQ)

    @pl.when(first)
    def _():
        for ex in ex_k:
            ex.wait_recv()
        mt_ref[...] = mbuf[...].reshape(SQ, RB).T
        pt_ref[...] = pbuf[...].reshape(RB, RB).T
        for ex in ex_k:
            ex.wait_send()

    ex_b.wait_recv()
    for h in range(8):
        bias_t[h] = ball[:, h].reshape(RB, RB).astype(F32).T * LOG2E
    row_k = row_w[0, :, SQ:512]
    row_ow = row_o[0]
    for ck in range(2):
        def row_body(sls):
            xs = [m_ref[ck * TI + sl] for sl in sls]
            masks = [column_of(rmask_ref[pl.ds(ck * TI + sl, 1), :]) for sl in sls]
            xns = [norm_lanes(x.astype(F32)) for x in xs]
            upds = attend_tiles(xns, wt, row_k, row_ow, 8, bias_t, masks, 4)
            for sl, x, upd in zip(sls, xs, upds):
                y = residual(x, upd).astype(F32)
                for half in range(2):
                    scr[half, pl.ds(sl, RB, stride=TI), :] = y[:, RB * half:RB * half + RB]

        tile_loop(TI, 2, row_body)

        def pack(d, carry):
            for half in range(2):
                part = scr[half, pl.ds(pl.multiple_of(d * SQ, SQ), SQ), :].astype(BF).reshape(TI, TI, RB)
                sendbuf[ck, d, :, :, RB * half:RB * half + RB] = part
            return carry

        lax.fori_loop(0, 8, pack, 0)
        rbuf[me * 2 + ck] = sendbuf[ck, me]
        if ck == 0:
            ex0 = Direct(me, lambda peer: sendbuf.at[0, peer], lambda owner: rbuf.at[owner * 2], ssem, rsem, 24)
            ex0.start()

    def quarter(q):
        part = pl.ds(q * 2, 2)
        return Direct(me, lambda peer: sendbuf.at[1, peer, part], lambda owner: rbuf.at[owner * 2 + 1, part], ssem, rsem, HD + q * ND)

    for q in range(8):
        quarter(q).start()
    ex_b.wait_send()
    prep_qkvg(col_w, wt, SQ)
    ex0.wait_recv()
    col_k = col_w[0, :, SQ:512]
    col_ow = col_o[0]

    def col_body(rs):
        xs = [rbuf[:, r].reshape(SQ, SQ) for r in rs]
        mrows = [mt_ref[pl.ds(me * TI + r, 1), :] for r in rs]
        masks = [column_of(mrow) for mrow in mrows]
        upds = attend_tiles([norm_lanes(x.astype(F32)) for x in xs], wt, col_k, col_ow, 8, None, masks, 2)
        for r, x, upd in zip(rs, xs, upds):
            m2_ref[r] = residual(x, upd)

    def mtr_body(rs):
        ys = [m2_ref[r] for r in rs]
        mrows = [mt_ref[pl.ds(me * TI + r, 1), :] for r in rs]
        xns = [norm_lanes(y.astype(F32)) for y in ys]
        hids = [jnp.maximum(dot(xn, mtr_i[0]), 0.0).astype(BF) for xn in xns]
        y2s = [residual(y, dot(hid, mtr_o[0])) for y, hid in zip(ys, hids)]
        xns = [norm_lanes(y2.astype(F32)) for y2 in y2s]
        abs_ = [dot_nt(opt[0], xn).astype(BF).astype(F32) * mrow for xn, mrow in zip(xns, mrows)]
        for r, y2, ab in zip(rs, y2s, abs_):
            m2_ref[r] = y2
            at_ref[r] = ab[0:HD].astype(BF)
            for half in range(2):
                scr[half, pl.ds(r, HD, stride=TI), :] = ab[HD:2 * HD, RB * half:RB * half + RB]

    def col_quarter(q, carry):
        quarter(q).wait_recv()
        tile_loop(2, 1, lambda rs: col_body([q * 2 + r for r in rs]))
        mtr_body([q * 2, q * 2 + 1])
        return carry

    lax.fori_loop(0, 8, col_quarter, 0)
    for half in range(2):
        btall[me, :, :, RB * half:RB * half + RB] = scr[half, 0:512, :].astype(BF).reshape(HD, TI, RB)
    ag0 = Chain(me, btall, ch_s.at[0], ch_r.at[0])
    ag0.start()
    scr_a[0:1024, :] = opm_o[0].astype(F32)

    def perm(e, carry):
        rows = scr_a[pl.ds(e, HD, stride=HD), :]
        scr_b[pl.ds(pl.multiple_of(e * HD, HD), HD), :] = rows
        return carry

    lax.fori_loop(0, HD, perm, 0)
    for q in range(8):
        opw[:, RB * q:RB * q + RB] = scr_b[RB * q:RB * q + RB, :].T.astype(BF)
    mloc = mt_ref[pl.ds(pl.multiple_of(me * TI, TI), TI), :].astype(BF)
    inv_over = 1.0 / (1e-3 + dot_nt(mloc, mt_ref[...].astype(BF)))
    scr_x[0:TI, :] = inv_over
    twt[...] = transpose_bf(tmo_p[0, :, 0:512])
    ag0.finish()
    ret = Return(me, lambda peer: m2_ref.at[:, pl.ds(pl.multiple_of(peer * HD, HD), HD), :], lambda owner: mrecv.at[owner], ms, mr)
    ret.start(3, chip == 0)
    ret.start(-3, chip == 3)
    mrecv[me] = m2_ref[:, pl.ds(pl.multiple_of(me * HD, HD), HD), :]

    left = at_ref[...].reshape(512, SQ)

    def opm_e(es):
        rhs = [btall[:, e].reshape(RB, SQ) for e in es]
        os_ = [dot_nt(left, r).astype(BF).reshape(TI, HD, RB) for r in rhs]
        for e, o in zip(es, os_):
            obuf[:, pl.ds(pl.multiple_of(e * HD, HD), HD), :] = o

    tile_loop(HD, 2, opm_e)

    def opm_i(tiles):
        y_ts = [dot(opw[...], obuf[i]) * scr_x[pl.ds(i, 1), :] for i in tiles]
        outs = [residual(z_ref[i], y_t.T) for i, y_t in zip(tiles, y_ts)]
        for i, out in zip(tiles, outs):
            z1[i] = out

    tile_loop(TI, 4, opm_i)

    def front(w_ref, wt_l, z_src, ball, left_too):
        wg = w_ref[0, :, 512:640]

        def body(tiles):
            xns = [norm_lanes(z_src[i].astype(F32)) for i in tiles]
            mrows = [pm_ref[pl.ds(i, 1), :] for i in tiles]
            if left_too:
                prs = [dot_nt(wt_l[...], xn) for xn in xns]
                lefts = [mrow * jax.nn.sigmoid(pr[SQ:384]) * pr[0:RB] for mrow, pr in zip(mrows, prs)]
                pbs = [pr[RB:SQ] for pr in prs]
                pgs = [pr[384:512] for pr in prs]
            else:
                lefts = []
                pbs = [dot_nt(wt_l[RB:SQ, :], xn) for xn in xns]
                pgs = [dot_nt(wt_l[384:512, :], xn) for xn in xns]
            gates = [dot(xn, wg) for xn in xns]
            rights = [mrow * jax.nn.sigmoid(pg) * pb for mrow, pg, pb in zip(mrows, pgs, pbs)]
            gates = [jax.nn.sigmoid(g) for g in gates]
            for i, left in zip(tiles, lefts):
                scr_a[pl.ds(i, RB, stride=TI), :] = left
            for i, right, gate in zip(tiles, rights, gates):
                scr_b[pl.ds(i, RB, stride=TI), :] = right
                gbuf[i] = gate

        tile_loop(TI, 4, body)
        ball[me] = scr_b[...].astype(BF).reshape(RB, TI, RB)

    def finish(w_ref, z_src, z_dst):
        w = w_ref[0]

        def body(tiles):
            xns = [norm_rows(scr_x[pl.ds(i, RB, stride=TI), :]) for i in tiles]
            ys = [dot_tn(xn, w) for xn in xns]
            outs = [residual(z_src[i], gbuf[i] * y) for i, y in zip(tiles, ys)]
            for i, out in zip(tiles, outs):
                z_dst[i] = out

        tile_loop(TI, 4, body)

    front(tmo_p, twt, z1, ball1, True)
    ag1 = Chain(me, ball1, ch_s.at[1], ch_r.at[1])
    ag1.start()
    ret.start(1, chip == 0)
    ret.start(-1, chip == 3)
    ret.start_partner()
    a_c[...] = scr_a[...].astype(BF).reshape(RB, TI, RB)

    twt2[...] = transpose_bf(tmi_p[0, :, 0:512])

    def inner(t):
        if t == 1:
            ret.start(1, chip == 1)
            ret.start(-1, chip == 2)

    ag1.finish(inner)

    def out_c(cc, carry):
        for u in range(8):
            c = cc * 8 + u
            scr_x[pl.ds(pl.multiple_of(c * TI, TI), TI), :] = dot_nt(a_c[c], ball1[:, c].reshape(RB, RB))
        return carry

    lax.fori_loop(0, TI, out_c, 0)
    ret.start(1, chip == 2, (0,))
    ret.start(-1, chip == 1, (0,))
    finish(tmo_o, z1, z1)

    zall[me] = z1[...]
    ag2 = Chain(me, zall, ch_s.at[2], ch_r.at[2])
    ag2.start()
    front(tmi_p, twt2, z1, ball2, False)
    prep_qkvg(tas_w, wt2, RB)

    def in_right(slot):
        def body(tiles):
            xns = [norm_lanes(zall[slot, i].astype(F32)) for i in tiles]
            mrows = [pbuf[slot, pl.ds(i, 1), :] for i in tiles]
            pbs = [dot_nt(twt2[RB:SQ, :], xn) for xn in xns]
            pgs = [dot_nt(twt2[384:512, :], xn) for xn in xns]
            rights = [mrow * jax.nn.sigmoid(pg) * pb for mrow, pg, pb in zip(mrows, pgs, pbs)]
            for i, right in zip(tiles, rights):
                scr_b[pl.ds(i, RB, stride=TI), :] = right

        tile_loop(TI, 4, body)
        ball2[slot] = scr_b[...].astype(BF).reshape(RB, TI, RB)

    def two(t):
        if t == 2:
            ret.start(2, chip == 0)
            ret.start(-2, chip == 3)

    ag2.stream(in_right, two)
    scr_b[...] = zall[:, :, pl.ds(pl.multiple_of(me * TI, TI), TI), :].astype(F32).reshape(2048, RB)

    def in_left(tiles):
        xns = [norm_lanes(scr_b[pl.ds(i, RB, stride=TI), :]) for i in tiles]
        mrows = [pt_ref[pl.ds(me * TI + i, 1), :] for i in tiles]
        pas = [dot_nt(twt2[0:RB, :], xn) for xn in xns]
        pgs = [dot_nt(twt2[SQ:384, :], xn) for xn in xns]
        lefts = [mrow * jax.nn.sigmoid(pg) * pa for mrow, pg, pa in zip(mrows, pgs, pas)]
        for i, left in zip(tiles, lefts):
            scr_a[pl.ds(i, RB, stride=TI), :] = left

    tile_loop(TI, 4, in_left)
    a_c[...] = scr_a[...].astype(BF).reshape(RB, TI, RB)

    def in_c(cc, carry):
        for u in range(8):
            c = cc * 8 + u
            scr_x[pl.ds(pl.multiple_of(c * TI, TI), TI), :] = dot(a_c[c], ball2[:, c].reshape(RB, RB))
        return carry

    lax.fori_loop(0, TI, in_c, 0)
    ret.start(1, chip == 2, (1,))
    ret.start(-1, chip == 1, (1,))
    finish(tmi_o, z1, z1)

    def send_bias(slot, base):
        ball3[slot, me] = sbias[0:64, :].astype(BF).reshape(4, TI, RB)
        ex = Direct(me, lambda peer: ball3.at[slot, me], lambda owner: ball3.at[slot, owner], ssem, rsem, base)
        ex.start()
        return ex

    def tas_bias(tiles):
        rows = [dot_nt(tas_bt[0], norm_lanes(z1[i].astype(F32))) for i in tiles]
        for i, row in zip(tiles, rows):
            sbias[pl.ds(i, 4, stride=TI), :] = row

    tile_loop(TI, 8, tas_bias)
    ex_s = send_bias(0, 96)
    ex_s.wait_recv()
    for h in range(4):
        bias_t[h] = ball3[0, :, h].reshape(RB, RB).astype(F32).T * LOG2E
    ret.start(2, chip == 1, (0,))
    ret.start(-2, chip == 2, (0,))
    tas_k = tas_w[0, :, RB:SQ]

    def tas_body(tiles):
        xs = [z1[i] for i in tiles]
        masks = [column_of(pm_ref[pl.ds(i, 1), :]) for i in tiles]
        upds = attend_tiles([norm_lanes(x.astype(F32)) for x in xs], wt2, tas_k, tas_o[0], 4, bias_t, masks, 4)
        outs = [residual(x, upd) for x, upd in zip(xs, upds)]
        rows = [dot_nt(tae_bt[0], norm_lanes(out.astype(F32))) for out in outs]
        for i, out, row in zip(tiles, outs, rows):
            z1[i] = out
            sbias[pl.ds(i, 4, stride=TI), :] = row

    tile_loop(TI, 4, tas_body)

    ex_z2 = Direct(me, lambda peer: z1.at[:, pl.ds(pl.multiple_of(peer * TI, TI), TI), :], lambda owner: zcol.at[owner], ssem, rsem, 104)
    ex_z2.start()
    ex_e = send_bias(1, 112)
    zcol[me] = z1[:, pl.ds(pl.multiple_of(me * TI, TI), TI), :]
    prep_qkvg(tae_w, wt2, RB)
    ex_z2.wait_recv()
    scr_b[...] = zcol[...].astype(F32).reshape(2048, RB)
    ex_e.wait_recv()
    for h in range(4):
        bias_t[h] = ball3[1, :, h].reshape(RB, RB).astype(F32) * LOG2E
    ret.start(2, chip == 1, (1,))
    ret.start(-2, chip == 2, (1,))
    tae_k = tae_w[0, :, RB:SQ]

    def tae_body(tiles):
        xs = [scr_b[pl.ds(i, RB, stride=TI), :] for i in tiles]
        masks = [column_of(pt_ref[pl.ds(me * TI + i, 1), :]) for i in tiles]
        upds = attend_tiles([norm_lanes(x) for x in xs], wt2, tae_k, tae_o[0], 4, bias_t, masks, 4)
        for i, x, upd in zip(tiles, xs, upds):
            scr_a[pl.ds(i, RB, stride=TI), :] = x + upd

    tile_loop(TI, 4, tae_body)
    zsend[...] = scr_a[...].astype(BF).reshape(8, TI, TI, RB)
    ex_z3 = Direct(me, lambda peer: zsend.at[peer], lambda owner: z4.at[:, pl.ds(pl.multiple_of(owner * TI, TI), TI), :], ssem, rsem, 120)
    ex_z3.start()
    z4[:, pl.ds(pl.multiple_of(me * TI, TI), TI), :] = zsend[me]

    ret.wait_recv()

    def widen(d, carry):
        for half in range(2):
            part = mrecv[d, :, :, RB * half:RB * half + RB].astype(F32).reshape(512, RB)
            mscr[half, pl.ds(pl.multiple_of(d * 512, 512), 512), :] = part
        return carry

    lax.fori_loop(0, 8, widen, 0)

    def take_seq(seqs):
        for s in seqs:
            for half in range(2):
                mout_ref[s, :, RB * half:RB * half + RB] = mscr[half, pl.ds(s, RB, stride=HD), :].astype(BF)

    tile_loop(HD, 4, take_seq)
    ex_z3.wait_recv()

    def trans(tiles):
        xs = [z4[i] for i in tiles]
        xns = [norm_lanes(x.astype(F32)) for x in xs]
        hids = [jnp.maximum(dot(xn, ptr_i[0]), 0.0).astype(BF) for xn in xns]
        outs = [residual(x, dot(hid, ptr_o[0])) for x, hid in zip(xs, hids)]
        for i, out in zip(tiles, outs):
            zout_ref[i] = out

    tile_loop(TI, 4, trans)
    for ex in [ex0] + [quarter(q) for q in range(8)] + [ag0, ag1, ag2, ret, ex_s, ex_e, ex_z2, ex_z3]:
        ex.wait_send()


def full(shape):
    return pl.BlockSpec(shape, lambda g: (0,) * len(shape))


def layer_of(shape):
    return pl.BlockSpec((1,) + shape[1:], lambda g: (g,) + (0,) * (len(shape) - 1))


def run(m, z, mm, pm, weights):
    acts = (m, z, mm, pm)
    outs = [(HD, RB, SQ), (TI, RB, RB)]
    vm = pltpu.VMEM
    return pl.pallas_call(
        blocks_kernel,
        grid=(weights[0].shape[0],),
        out_shape=[jax.ShapeDtypeStruct(s, BF) for s in outs],
        in_specs=[full(a.shape) for a in acts] + [layer_of(w.shape) for w in weights],
        out_specs=[full(s) for s in outs],
        scratch_shapes=[
            vm((ND, HD, RB), F32), vm((ND, TI, RB), F32), vm((RB, SQ), F32), vm((RB, RB), F32), vm((HD, RB), F32), vm((TI, RB), F32),
            vm((ND, 8, TI, RB), BF), vm((8, RB, RB), F32), vm((768, SQ), BF), vm((2, 2048, RB), F32),
            vm((2, ND, TI, TI, SQ), BF), vm((2 * ND, TI, TI, SQ), BF), vm((RB, RB), F32), vm((TI, SQ, SQ), BF), vm((TI, HD, SQ), BF),
            vm((ND, HD, TI, SQ), BF), vm((TI, 1024, RB), BF), vm((RB, 1024), BF),
            vm((2048, RB), F32), vm((2048, RB), F32), vm((2048, RB), F32),
            vm((RB, TI, RB), BF), vm((ND, RB, TI, RB), BF), vm((ND, RB, TI, RB), BF), vm((TI, RB, RB), F32), vm((TI, RB, RB), BF),
            vm((ND, TI, TI, RB), BF), vm((RB, RB), F32), vm((2, ND, 4, TI, RB), BF),
            vm((384, RB), BF), vm((512, RB), BF), vm((512, RB), BF), vm((ND, TI, RB, RB), BF), vm((ND, TI, TI, RB), BF), vm((TI, RB, RB), BF),
            vm((ND, TI, HD, SQ), BF), vm((2, 4096, RB), F32),
            pltpu.SemaphoreType.DMA((RB,)), pltpu.SemaphoreType.DMA((RB,)),
            pltpu.SemaphoreType.DMA((3, 2, 13)), pltpu.SemaphoreType.DMA((3, 2, 13)),
            pltpu.SemaphoreType.DMA((14,)), pltpu.SemaphoreType.DMA((14,)),
        ],
        compiler_params=pltpu.CompilerParams(collective_id=0, has_side_effects=True, vmem_limit_bytes=VMEM_LIMIT),
    )(*acts, *weights)


def solution(mesh):
    row_spec = P(('req', 'dap'))

    def local_body(m, z, mm, pm, *weights):
        weights = [jnp.swapaxes(w, 1, 2) if k in (1, 7, 14, 17) else w for k, w in enumerate(weights)]
        return tuple(run(m, z, mm, pm, weights))

    def run_blocks(*arrays):
        n_weights = len(arrays) - 4
        return jax.shard_map(local_body, mesh=mesh, in_specs=(row_spec,) * 4 + (P(),) * n_weights,
                             out_specs=(row_spec, row_spec), check_vma=False)(*arrays)

    return run_blocks
```

```python
import jax
import jax.numpy as jnp
from jax import lax
from jax.experimental import pallas as pl
from jax.experimental.pallas import tpu as pltpu
from jax.sharding import PartitionSpec as P

MESH = pl.DeviceIdType.MESH
F32 = jnp.float32
BF = jnp.bfloat16
LOG2E = 1.4426950408889634
NEG = -1e9 * LOG2E
ND = 8
VMEM_LIMIT = 66_000_000
RB = 128
SQ = 256
TI = 16
HD = 32
EARLY = 3


def dot(a, b):
    return lax.dot_general(a, b, (((1,), (0,)), ((), ())), preferred_element_type=F32)


def dot_nt(a, b):
    return lax.dot_general(a, b, (((1,), (1,)), ((), ())), preferred_element_type=F32)


def dot_tn(a, b):
    return lax.dot_general(a, b, (((0,), (0,)), ((), ())), preferred_element_type=F32)


def transpose_bf(w):
    return w.astype(F32).T.astype(BF)


def norm_lanes(x):
    mean = jnp.mean(x, axis=-1, keepdims=True)
    centered = x - mean
    var = jnp.mean(centered * centered, axis=-1, keepdims=True)
    return (centered * lax.rsqrt(var + 1e-5)).astype(BF)


def norm_rows(x):
    mean = jnp.mean(x, axis=0, keepdims=True)
    centered = x - mean
    var = jnp.mean(centered * centered, axis=0, keepdims=True)
    return (centered * lax.rsqrt(var + 1e-5)).astype(BF)


def residual(x, update):
    return (x.astype(F32) + update).astype(BF)


def group_barrier(me):
    sem = pltpu.get_barrier_semaphore()
    for p in range(1, ND):
        pl.semaphore_signal(sem, inc=1, device_id={'dap': lax.rem(me + p, ND)}, device_id_type=MESH)
    pl.semaphore_wait(sem, ND - 1)


def remote(src, dst, send_sem, recv_sem, peer):
    return pltpu.make_async_remote_copy(src_ref=src, dst_ref=dst, send_sem=send_sem, recv_sem=recv_sem,
                                        device_id={'dap': peer}, device_id_type=MESH)


class Direct:
    def __init__(self, me, src_of, dst_of, ssem, rsem, base=0):
        self.me, self.src_of, self.dst_of, self.ssem, self.rsem, self.base = me, src_of, dst_of, ssem, rsem, base

    def copy_to(self, p):
        peer = lax.rem(self.me + p, ND)
        return remote(self.src_of(peer), self.dst_of(self.me), self.ssem.at[self.base + p], self.rsem.at[self.base + p], peer)

    def start(self, ps=range(1, ND)):
        for p in ps:
            self.copy_to(p).start()

    def wait_recv(self):
        for p in range(1, ND):
            owner = lax.rem(self.me + ND - p, ND)
            remote(self.src_of(owner), self.dst_of(owner), self.ssem.at[self.base + p], self.rsem.at[self.base + p], owner).wait_recv()

    def wait_send(self):
        for p in range(1, ND):
            self.copy_to(p).wait_send()


class Chain:
    def __init__(self, me, buf, ssem, rsem):
        self.buf, self.ssem, self.rsem = buf, ssem, rsem
        self.z, self.c = lax.div(me, 2), lax.rem(me, 2)
        self.me, self.partner = me, me + 1 - 2 * self.c
        self.size = buf.shape[1] // 2

    def cp(self, slot, peer, sem, half):
        ref = self.buf.at[slot, pl.ds(half * self.size, self.size)]
        return remote(ref, ref, self.ssem.at[half, sem], self.rsem.at[half, sem], peer)

    def slot(self, off, other=False):
        core = 1 - self.c if other else self.c
        return (self.z + off) * 2 + core

    def own(self, act):
        for half in range(2):
            @pl.when(self.z < 3)
            def _():
                act(self.cp(self.me, self.me + 2, 0, half))

            @pl.when(self.z > 0)
            def _():
                act(self.cp(self.me, self.me - 2, 3, half))

        for half in range(2):
            act(self.cp(self.me, self.partner, 6, half))

    def forward(self, t, half, before, act):
        z = self.z

        @pl.when(z >= t)
        def _():
            if before:
                before(self.cp(self.slot(-t), self.me, t - 1, half))
            if t < 3:
                @pl.when(z < 3)
                def _():
                    act(self.cp(self.slot(-t), self.me + 2, t, half))
            act(self.cp(self.slot(-t), self.partner, 6 + t, half))

        @pl.when(z + t <= 3)
        def _():
            if before:
                before(self.cp(self.slot(t), self.me, 2 + t, half))
            if t < 3:
                @pl.when(z > 0)
                def _():
                    act(self.cp(self.slot(t), self.me - 2, 3 + t, half))
            act(self.cp(self.slot(t), self.partner, 9 + t, half))

    def start(self):
        self.own(lambda c: c.start())

    def finish(self, hook=None):
        z = self.z
        for t in range(1, 4):
            for half in range(2):
                self.forward(t, half, lambda c: c.wait_recv(), lambda c: c.start())
            if hook is not None:
                hook(t)
        for half in range(2):
            self.cp(self.partner, self.me, 6, half).wait_recv()
            for t in range(1, 4):
                @pl.when(z >= t)
                def _():
                    self.cp(self.slot(-t, True), self.me, 6 + t, half).wait_recv()

                @pl.when(z + t <= 3)
                def _():
                    self.cp(self.slot(t, True), self.me, 9 + t, half).wait_recv()

    def stream(self, process, hook):
        z = self.z

        def take(t, other):
            def one(k, carry):
                off = (2 * k - 1) * t

                @pl.when(jnp.logical_and(z + off >= 0, z + off <= 3))
                def _():
                    if other:
                        for half in range(2):
                            self.cp(self.slot(off, True), self.me, 6 + 3 * k + t, half).wait_recv()
                    process(self.slot(off, other))

                return carry

            lax.fori_loop(0, 2, one, 0)

        for t in range(1, 4):
            for half in range(2):
                self.forward(t, half, lambda c: c.wait_recv(), lambda c: c.start())
            hook(t)
            if t == 1:
                for half in range(2):
                    self.cp(self.partner, self.me, 6, half).wait_recv()
                process(self.partner)
            else:
                take(t - 1, True)
            take(t, False)
        take(3, True)

    def wait_send(self):
        self.own(lambda c: c.wait_send())
        for t in range(1, 4):
            for half in range(2):
                self.forward(t, half, None, lambda c: c.wait_send())


class Return:
    def __init__(self, me, src, dst, ssem, rsem):
        self.me, self.src, self.dst, self.ssem, self.rsem = me, src, dst, ssem, rsem
        self.z, self.c = lax.div(me, 2), lax.rem(me, 2)

    def copy_to(self, off, core):
        peer = (self.z + off) * 2 + core
        return remote(self.src(peer), self.dst(self.me), self.ssem.at[(off + 3) * 2 + core], self.rsem.at[(off + 3) * 2 + self.c], peer)

    def start(self, off, cond, cores=(0, 1)):
        @pl.when(cond)
        def _():
            for core in cores:
                self.copy_to(off, core).start()

    def start_partner(self):
        self.copy_to(0, 1 - self.c).start()

    def each(self, fn):
        fn(0, 1 - self.c)
        for off in (-3, -2, -1, 1, 2, 3):
            @pl.when(jnp.logical_and(self.z + off >= 0, self.z + off <= 3))
            def _():
                for core in range(2):
                    fn(off, core)

    def wait_recv(self):
        def one(off, core):
            owner = (self.z + off) * 2 + core
            sem = (3 - off) * 2 + core
            remote(self.src(self.me), self.dst(owner), self.ssem.at[sem], self.rsem.at[sem], self.me).wait_recv()

        self.each(one)

    def wait_send(self):
        self.each(lambda off, core: self.copy_to(off, core).wait_send())


def column_of(row):
    return jnp.broadcast_to(row, (RB, row.shape[1])).T


def attend_tiles(xns, wt_ref, wk, w_out, heads, bias_ref, key_masks, depth):
    length = xns[0].shape[0]
    width = heads * HD
    projs = [dot_nt(wt_ref[...], xn) for xn in xns]
    keys = [dot(xn, wk).astype(BF) for xn in xns]
    q_t = [proj[:width].astype(BF) for proj in projs]
    v_t = [proj[width:2 * width].astype(BF) for proj in projs]
    gate = [jax.nn.sigmoid(proj[2 * width:].astype(BF).astype(F32)) for proj in projs]
    valid = [key_mask > 0 for key_mask in key_masks]
    scale = HD ** -0.5 * LOG2E

    def logits_of(unit):
        t, qc, h = unit
        hh = h % 4
        rhs = [q_t[t][HD * h:HD * h + HD, RB * qc:RB * qc + RB]]
        if hh > 0:
            rhs = [jnp.zeros((HD * hh, RB), BF)] + rhs
        if hh < 3:
            rhs = rhs + [jnp.zeros((96 - HD * hh, RB), BF)]
        return dot(keys[t][:, RB * (h // 4):RB * (h // 4) + RB], jnp.concatenate(rhs, 0))

    def prob_of(unit, raw):
        t, qc, h = unit
        logits = raw * scale
        if bias_ref is not None:
            logits = logits + bias_ref[h]
        logits = jnp.where(valid[t], logits, NEG)
        e = jnp.exp2(logits - jnp.max(logits, axis=0, keepdims=True))
        return (e * (1.0 / jnp.sum(e, axis=0, keepdims=True))).astype(BF)

    blocks = [(t, qc) for t in range(len(xns)) for qc in range(length // RB)]
    units = [(t, qc, h) for t, qc in blocks for h in range(heads)]
    raws = {i: logits_of(units[i]) for i in range(min(depth, len(units)))}
    outs, probs, upds = {}, {}, {}

    def flush(i):
        t, qc, h = units[i]
        outs[units[i]] = dot(v_t[t][HD * h:HD * h + HD], probs.pop(i))
        if h == heads - 1:
            o = jnp.concatenate([outs.pop((t, qc, hh)) for hh in range(heads)], 0)
            upds[t, qc] = (o * gate[t][:, RB * qc:RB * qc + RB]).astype(BF)

    for i in range(len(units)):
        if i + depth < len(units):
            raws[i + depth] = logits_of(units[i + depth])
        probs[i] = prob_of(units[i], raws.pop(i))
        if i > 0:
            flush(i - 1)
    flush(len(units) - 1)
    pieces = [dot_tn(upds[block], w_out) for block in blocks]
    per = length // RB
    return [jnp.concatenate(pieces[t * per:t * per + per], 0) for t in range(len(xns))]


def tile_loop(count, width, body):
    def step(g, carry):
        body([g * width + u for u in range(width)])
        return carry

    lax.fori_loop(0, count // width, step, 0)


def prep_qkvg(w_ref, wt_ref, width):
    wt_ref[0:width, :] = transpose_bf(w_ref[0, :, 0:width])
    wt_ref[width:3 * width, :] = transpose_bf(w_ref[0, :, 2 * width:4 * width])


def blocks_kernel(m_in, z_in, mm_ref, pm_in,
                  row_w, row_bt, row_o, col_w, col_o, mtr_i, mtr_o, opt, opm_o,
                  tmo_p, tmo_o, tmi_p, tmi_o, tas_w, tas_bt, tas_o, tae_w, tae_bt, tae_o, ptr_i, ptr_o,
                  mout_ref, zout_ref,
                  mbuf, pbuf, mt_ref, pt_ref, rmask_ref, pm_ref,
                  ball, bias_t, wt, scr, sendbuf, rbuf, bscr, m2_ref, at_ref,
                  btall, obuf, opw, scr_a, scr_b, scr_x, a_c, ball1, ball2, gbuf, z1, zcol, sbias, ball3,
                  wt2, twt, twt2, zall, zsend, z4, mrecv, mscr,
                  ssem, rsem, ch_s, ch_r, ms, mr):
    me = lax.axis_index('dap')
    chip = lax.div(me, 2)
    first = pl.program_id(0) == 0
    group_barrier(me)
    ex_k = [Direct(me, lambda peer, buf=buf: buf.at[me], lambda owner, buf=buf: buf.at[owner], ssem, rsem, base)
            for buf, base in ((mbuf, 0), (pbuf, 8))]

    @pl.when(first)
    def _():
        rmask_ref[...] = mm_ref[...].astype(F32)
        pm_ref[...] = pm_in[...].astype(F32)
        mbuf[me] = rmask_ref[...]
        pbuf[me] = pm_ref[...]
        for ex in ex_k:
            ex.start()

        def take(s, carry):
            mout_ref[s] = m_in[s]
            return carry

        lax.fori_loop(0, HD, take, 0)
        zout_ref[...] = z_in[...]

    m_ref, z_ref = mout_ref, zout_ref
    wb_t = row_bt[0]

    def bias_row(tiles):
        rows = [dot_nt(wb_t, norm_lanes(z_ref[i].astype(F32))) for i in tiles]
        for i, row in zip(tiles, rows):
            bscr[pl.ds(i, 8, stride=TI), :] = row

    tile_loop(TI, 8, bias_row)
    ball[me] = bscr[...].astype(BF).reshape(8, TI, RB)
    ex_b = Direct(me, lambda peer: ball.at[me], lambda owner: ball.at[owner], ssem, rsem, TI)
    ex_b.start()
    prep_qkvg(row_w, wt, SQ)

    @pl.when(first)
    def _():
        for ex in ex_k:
            ex.wait_recv()
        mt_ref[...] = mbuf[...].reshape(SQ, RB).T
        pt_ref[...] = pbuf[...].reshape(RB, RB).T
        for ex in ex_k:
            ex.wait_send()

    ex_b.wait_recv()
    for h in range(8):
        bias_t[h] = ball[:, h].reshape(RB, RB).astype(F32).T * LOG2E
    row_k = row_w[0, :, SQ:512]
    row_ow = row_o[0]
    def piece(ck, q):
        part = pl.ds(q * 2, 2)
        return Direct(me, lambda peer: sendbuf.at[ck, peer, part], lambda owner: rbuf.at[owner * 2 + ck, part], ssem, rsem, 24 + ck * 64 + q * ND)

    def half_rows(ck, carry):
        def row_body(sls):
            xs = [m_ref[ck * TI + sl] for sl in sls]
            masks = [column_of(rmask_ref[pl.ds(ck * TI + sl, 1), :]) for sl in sls]
            xns = [norm_lanes(x.astype(F32)) for x in xs]
            upds = attend_tiles(xns, wt, row_k, row_ow, 8, bias_t, masks, 4)
            for sl, x, upd in zip(sls, xs, upds):
                y = residual(x, upd).astype(F32)
                for half in range(2):
                    scr[half, pl.ds(sl, RB, stride=TI), :] = y[:, RB * half:RB * half + RB]

        tile_loop(TI, 8, row_body)

        def pack(d, carry):
            for half in range(2):
                part = scr[half, pl.ds(pl.multiple_of(d * SQ, SQ), SQ), :].astype(BF).reshape(TI, TI, RB)
                sendbuf[ck, d, :, :, RB * half:RB * half + RB] = part
            return carry

        lax.fori_loop(0, 8, pack, 0)
        rbuf[me * 2 + ck] = sendbuf[ck, me]
        for q in range(EARLY):
            piece(ck, q).start()
        return carry

    lax.fori_loop(0, 2, half_rows, 0)

    def send_rest(q, carry):
        piece(0, q).start()
        piece(1, q).start()
        return carry

    lax.fori_loop(EARLY, 8, send_rest, 0)
    ex_b.wait_send()
    prep_qkvg(col_w, wt, SQ)
    col_k = col_w[0, :, SQ:512]
    col_ow = col_o[0]

    def col_body(rs):
        xs = [rbuf[:, r].reshape(SQ, SQ) for r in rs]
        mrows = [mt_ref[pl.ds(me * TI + r, 1), :] for r in rs]
        masks = [column_of(mrow) for mrow in mrows]
        upds = attend_tiles([norm_lanes(x.astype(F32)) for x in xs], wt, col_k, col_ow, 8, None, masks, 4)
        for r, x, upd in zip(rs, xs, upds):
            m2_ref[r] = residual(x, upd)

    def mtr_body(rs):
        ys = [m2_ref[r] for r in rs]
        mrows = [mt_ref[pl.ds(me * TI + r, 1), :] for r in rs]
        xns = [norm_lanes(y.astype(F32)) for y in ys]
        hids = [jnp.maximum(dot(xn, mtr_i[0]), 0.0).astype(BF) for xn in xns]
        y2s = [residual(y, dot(hid, mtr_o[0])) for y, hid in zip(ys, hids)]
        xns = [norm_lanes(y2.astype(F32)) for y2 in y2s]
        abs_ = [dot_nt(opt[0], xn).astype(BF).astype(F32) * mrow for xn, mrow in zip(xns, mrows)]
        for r, y2, ab in zip(rs, y2s, abs_):
            m2_ref[r] = y2
            at_ref[r] = ab[0:HD].astype(BF)
            for half in range(2):
                scr[half, pl.ds(r, HD, stride=TI), :] = ab[HD:2 * HD, RB * half:RB * half + RB]

    def col_quarter(q, carry):
        piece(0, q).wait_recv()
        piece(1, q).wait_recv()
        col_body([q * 2, q * 2 + 1])
        mtr_body([q * 2, q * 2 + 1])
        return carry

    lax.fori_loop(0, 8, col_quarter, 0)
    for half in range(2):
        btall[me, :, :, RB * half:RB * half + RB] = scr[half, 0:512, :].astype(BF).reshape(HD, TI, RB)
    ag0 = Chain(me, btall, ch_s.at[0], ch_r.at[0])
    ag0.start()
    scr_a[0:1024, :] = opm_o[0].astype(F32)

    def perm(e, carry):
        rows = scr_a[pl.ds(e, HD, stride=HD), :]
        scr_b[pl.ds(pl.multiple_of(e * HD, HD), HD), :] = rows
        return carry

    lax.fori_loop(0, HD, perm, 0)
    for q in range(8):
        opw[:, RB * q:RB * q + RB] = scr_b[RB * q:RB * q + RB, :].T.astype(BF)
    mloc = mt_ref[pl.ds(pl.multiple_of(me * TI, TI), TI), :].astype(BF)
    inv_over = 1.0 / (1e-3 + dot_nt(mloc, mt_ref[...].astype(BF)))
    scr_x[0:TI, :] = inv_over
    twt[...] = transpose_bf(tmo_p[0, :, 0:512])
    ag0.finish()
    ret = Return(me, lambda peer: m2_ref.at[:, pl.ds(pl.multiple_of(peer * HD, HD), HD), :], lambda owner: mrecv.at[owner], ms, mr)
    ret.start(3, chip == 0)
    ret.start(-3, chip == 3)
    mrecv[me] = m2_ref[:, pl.ds(pl.multiple_of(me * HD, HD), HD), :]

    left = at_ref[...].reshape(512, SQ)

    def opm_e(es):
        rhs = [btall[:, e].reshape(RB, SQ) for e in es]
        os_ = [dot_nt(left, r).astype(BF).reshape(TI, HD, RB) for r in rhs]
        for e, o in zip(es, os_):
            obuf[:, pl.ds(pl.multiple_of(e * HD, HD), HD), :] = o

    tile_loop(HD, 4, opm_e)

    def opm_i(tiles):
        y_ts = [dot(opw[...], obuf[i]) * scr_x[pl.ds(i, 1), :] for i in tiles]
        outs = [residual(z_ref[i], y_t.T) for i, y_t in zip(tiles, y_ts)]
        for i, out in zip(tiles, outs):
            z1[i] = out

    tile_loop(TI, 8, opm_i)

    def front(w_ref, wt_l, z_src, ball, left_too):
        wg = w_ref[0, :, 512:640]

        def body(tiles):
            xns = [norm_lanes(z_src[i].astype(F32)) for i in tiles]
            mrows = [pm_ref[pl.ds(i, 1), :] for i in tiles]
            if left_too:
                prs = [dot_nt(wt_l[...], xn) for xn in xns]
                lefts = [mrow * jax.nn.sigmoid(pr[SQ:384]) * pr[0:RB] for mrow, pr in zip(mrows, prs)]
                pbs = [pr[RB:SQ] for pr in prs]
                pgs = [pr[384:512] for pr in prs]
            else:
                lefts = []
                pbs = [dot_nt(wt_l[RB:SQ, :], xn) for xn in xns]
                pgs = [dot_nt(wt_l[384:512, :], xn) for xn in xns]
            gates = [dot(xn, wg) for xn in xns]
            rights = [mrow * jax.nn.sigmoid(pg) * pb for mrow, pg, pb in zip(mrows, pgs, pbs)]
            gates = [jax.nn.sigmoid(g) for g in gates]
            for i, left in zip(tiles, lefts):
                scr_a[pl.ds(i, RB, stride=TI), :] = left
            for i, right, gate in zip(tiles, rights, gates):
                scr_b[pl.ds(i, RB, stride=TI), :] = right
                gbuf[i] = gate

        tile_loop(TI, 8, body)
        ball[me] = scr_b[...].astype(BF).reshape(RB, TI, RB)

    def finish(w_ref, z_src, z_dst):
        w = w_ref[0]

        def body(tiles):
            xns = [norm_rows(scr_x[pl.ds(i, RB, stride=TI), :]) for i in tiles]
            ys = [dot_tn(xn, w) for xn in xns]
            outs = [residual(z_src[i], gbuf[i] * y) for i, y in zip(tiles, ys)]
            for i, out in zip(tiles, outs):
                z_dst[i] = out

        tile_loop(TI, 8, body)

    front(tmo_p, twt, z1, ball1, True)
    ag1 = Chain(me, ball1, ch_s.at[1], ch_r.at[1])
    ag1.start()
    ret.start(1, chip == 0)
    ret.start(-1, chip == 3)
    ret.start_partner()
    a_c[...] = scr_a[...].astype(BF).reshape(RB, TI, RB)

    twt2[...] = transpose_bf(tmi_p[0, :, 0:512])

    def inner(t):
        if t == 1:
            ret.start(1, chip == 1)
            ret.start(-1, chip == 2)

    ag1.finish(inner)

    def out_c(cc, carry):
        for u in range(8):
            c = cc * 8 + u
            scr_x[pl.ds(pl.multiple_of(c * TI, TI), TI), :] = dot_nt(a_c[c], ball1[:, c].reshape(RB, RB))
        return carry

    lax.fori_loop(0, TI, out_c, 0)
    ret.start(1, chip == 2, (0,))
    ret.start(-1, chip == 1, (0,))
    finish(tmo_o, z1, z1)

    zall[me] = z1[...]
    ag2 = Chain(me, zall, ch_s.at[2], ch_r.at[2])
    ag2.start()
    front(tmi_p, twt2, z1, ball2, False)
    prep_qkvg(tas_w, wt2, RB)

    def in_right(slot):
        def body(tiles):
            xns = [norm_lanes(zall[slot, i].astype(F32)) for i in tiles]
            mrows = [pbuf[slot, pl.ds(i, 1), :] for i in tiles]
            pbs = [dot_nt(twt2[RB:SQ, :], xn) for xn in xns]
            pgs = [dot_nt(twt2[384:512, :], xn) for xn in xns]
            rights = [mrow * jax.nn.sigmoid(pg) * pb for mrow, pg, pb in zip(mrows, pgs, pbs)]
            for i, right in zip(tiles, rights):
                scr_b[pl.ds(i, RB, stride=TI), :] = right

        tile_loop(TI, 8, body)
        ball2[slot] = scr_b[...].astype(BF).reshape(RB, TI, RB)

    def two(t):
        if t == 2:
            ret.start(2, chip == 0)
            ret.start(-2, chip == 3)

    ag2.stream(in_right, two)
    scr_b[...] = zall[:, :, pl.ds(pl.multiple_of(me * TI, TI), TI), :].astype(F32).reshape(2048, RB)

    def in_left(tiles):
        xns = [norm_lanes(scr_b[pl.ds(i, RB, stride=TI), :]) for i in tiles]
        mrows = [pt_ref[pl.ds(me * TI + i, 1), :] for i in tiles]
        pas = [dot_nt(twt2[0:RB, :], xn) for xn in xns]
        pgs = [dot_nt(twt2[SQ:384, :], xn) for xn in xns]
        lefts = [mrow * jax.nn.sigmoid(pg) * pa for mrow, pg, pa in zip(mrows, pgs, pas)]
        for i, left in zip(tiles, lefts):
            scr_a[pl.ds(i, RB, stride=TI), :] = left

    tile_loop(TI, 8, in_left)
    a_c[...] = scr_a[...].astype(BF).reshape(RB, TI, RB)

    def in_c(cc, carry):
        for u in range(8):
            c = cc * 8 + u
            scr_x[pl.ds(pl.multiple_of(c * TI, TI), TI), :] = dot(a_c[c], ball2[:, c].reshape(RB, RB))
        return carry

    lax.fori_loop(0, TI, in_c, 0)
    ret.start(1, chip == 2, (1,))
    ret.start(-1, chip == 1, (1,))
    finish(tmi_o, z1, z1)

    def send_bias(slot, base):
        ball3[slot, me] = sbias[0:64, :].astype(BF).reshape(4, TI, RB)
        ex = Direct(me, lambda peer: ball3.at[slot, me], lambda owner: ball3.at[slot, owner], ssem, rsem, base)
        ex.start()
        return ex

    def tas_bias(tiles):
        rows = [dot_nt(tas_bt[0], norm_lanes(z1[i].astype(F32))) for i in tiles]
        for i, row in zip(tiles, rows):
            sbias[pl.ds(i, 4, stride=TI), :] = row

    tile_loop(TI, 8, tas_bias)
    ex_s = send_bias(0, 152)
    ex_s.wait_recv()
    for h in range(4):
        bias_t[h] = ball3[0, :, h].reshape(RB, RB).astype(F32).T * LOG2E
    ret.start(2, chip == 1, (0,))
    ret.start(-2, chip == 2, (0,))
    tas_k = tas_w[0, :, RB:SQ]

    def tas_body(tiles):
        xs = [z1[i] for i in tiles]
        masks = [column_of(pm_ref[pl.ds(i, 1), :]) for i in tiles]
        upds = attend_tiles([norm_lanes(x.astype(F32)) for x in xs], wt2, tas_k, tas_o[0], 4, bias_t, masks, 4)
        outs = [residual(x, upd) for x, upd in zip(xs, upds)]
        rows = [dot_nt(tae_bt[0], norm_lanes(out.astype(F32))) for out in outs]
        for i, out, row in zip(tiles, outs, rows):
            z1[i] = out
            sbias[pl.ds(i, 4, stride=TI), :] = row

    tile_loop(TI, 8, tas_body)

    ex_z2 = Direct(me, lambda peer: z1.at[:, pl.ds(pl.multiple_of(peer * TI, TI), TI), :], lambda owner: zcol.at[owner], ssem, rsem, 160)
    ex_z2.start()
    ex_e = send_bias(1, 168)
    zcol[me] = z1[:, pl.ds(pl.multiple_of(me * TI, TI), TI), :]
    prep_qkvg(tae_w, wt2, RB)
    ex_z2.wait_recv()
    scr_b[...] = zcol[...].astype(F32).reshape(2048, RB)
    ex_e.wait_recv()
    for h in range(4):
        bias_t[h] = ball3[1, :, h].reshape(RB, RB).astype(F32) * LOG2E
    ret.start(2, chip == 1, (1,))
    ret.start(-2, chip == 2, (1,))
    tae_k = tae_w[0, :, RB:SQ]

    def tae_body(tiles):
        xs = [scr_b[pl.ds(i, RB, stride=TI), :] for i in tiles]
        masks = [column_of(pt_ref[pl.ds(me * TI + i, 1), :]) for i in tiles]
        upds = attend_tiles([norm_lanes(x) for x in xs], wt2, tae_k, tae_o[0], 4, bias_t, masks, 4)
        for i, x, upd in zip(tiles, xs, upds):
            scr_a[pl.ds(i, RB, stride=TI), :] = x + upd

    tile_loop(TI, 8, tae_body)
    zsend[...] = scr_a[...].astype(BF).reshape(8, TI, TI, RB)
    ex_z3 = Direct(me, lambda peer: zsend.at[peer], lambda owner: z4.at[:, pl.ds(pl.multiple_of(owner * TI, TI), TI), :], ssem, rsem, 176)
    ex_z3.start()
    z4[:, pl.ds(pl.multiple_of(me * TI, TI), TI), :] = zsend[me]

    ret.wait_recv()

    def widen(d, carry):
        for half in range(2):
            part = mrecv[d, :, :, RB * half:RB * half + RB].astype(F32).reshape(512, RB)
            mscr[half, pl.ds(pl.multiple_of(d * 512, 512), 512), :] = part
        return carry

    lax.fori_loop(0, 8, widen, 0)

    def take_seq(seqs):
        for s in seqs:
            for half in range(2):
                mout_ref[s, :, RB * half:RB * half + RB] = mscr[half, pl.ds(s, RB, stride=HD), :].astype(BF)

    tile_loop(HD, 4, take_seq)
    ex_z3.wait_recv()

    def trans(tiles):
        xs = [z4[i] for i in tiles]
        xns = [norm_lanes(x.astype(F32)) for x in xs]
        hids = [jnp.maximum(dot(xn, ptr_i[0]), 0.0).astype(BF) for xn in xns]
        outs = [residual(x, dot(hid, ptr_o[0])) for x, hid in zip(xs, hids)]
        for i, out in zip(tiles, outs):
            zout_ref[i] = out

    tile_loop(TI, 8, trans)
    def sent(q, carry):
        piece(0, q).wait_send()
        piece(1, q).wait_send()
        return carry

    lax.fori_loop(0, 8, sent, 0)
    for ex in (ag0, ag1, ag2, ret, ex_s, ex_e, ex_z2, ex_z3):
        ex.wait_send()


def full(shape):
    return pl.BlockSpec(shape, lambda g: (0,) * len(shape))


def layer_of(shape):
    return pl.BlockSpec((1,) + shape[1:], lambda g: (g,) + (0,) * (len(shape) - 1))


def run(m, z, mm, pm, weights):
    acts = (m, z, mm, pm)
    outs = [(HD, RB, SQ), (TI, RB, RB)]
    vm = pltpu.VMEM
    return pl.pallas_call(
        blocks_kernel,
        grid=(weights[0].shape[0],),
        out_shape=[jax.ShapeDtypeStruct(s, BF) for s in outs],
        in_specs=[full(a.shape) for a in acts] + [layer_of(w.shape) for w in weights],
        out_specs=[full(s) for s in outs],
        scratch_shapes=[
            vm((ND, HD, RB), F32), vm((ND, TI, RB), F32), vm((RB, SQ), F32), vm((RB, RB), F32), vm((HD, RB), F32), vm((TI, RB), F32),
            vm((ND, 8, TI, RB), BF), vm((8, RB, RB), F32), vm((768, SQ), BF), vm((2, 2048, RB), F32),
            vm((2, ND, TI, TI, SQ), BF), vm((2 * ND, TI, TI, SQ), BF), vm((RB, RB), F32), vm((TI, SQ, SQ), BF), vm((TI, HD, SQ), BF),
            vm((ND, HD, TI, SQ), BF), vm((TI, 1024, RB), BF), vm((RB, 1024), BF),
            vm((2048, RB), F32), vm((2048, RB), F32), vm((2048, RB), F32),
            vm((RB, TI, RB), BF), vm((ND, RB, TI, RB), BF), vm((ND, RB, TI, RB), BF), vm((TI, RB, RB), F32), vm((TI, RB, RB), BF),
            vm((ND, TI, TI, RB), BF), vm((RB, RB), F32), vm((2, ND, 4, TI, RB), BF),
            vm((384, RB), BF), vm((512, RB), BF), vm((512, RB), BF), vm((ND, TI, RB, RB), BF), vm((ND, TI, TI, RB), BF), vm((TI, RB, RB), BF),
            vm((ND, TI, HD, SQ), BF), vm((2, 4096, RB), F32),
            pltpu.SemaphoreType.DMA((184,)), pltpu.SemaphoreType.DMA((184,)),
            pltpu.SemaphoreType.DMA((3, 2, 13)), pltpu.SemaphoreType.DMA((3, 2, 13)),
            pltpu.SemaphoreType.DMA((14,)), pltpu.SemaphoreType.DMA((14,)),
        ],
        compiler_params=pltpu.CompilerParams(collective_id=0, has_side_effects=True, vmem_limit_bytes=VMEM_LIMIT),
    )(*acts, *weights)


def solution(mesh):
    row_spec = P(('req', 'dap'))

    def local_body(m, z, mm, pm, *weights):
        weights = [jnp.swapaxes(w, 1, 2) if k in (1, 7, 14, 17) else w for k, w in enumerate(weights)]
        return tuple(run(m, z, mm, pm, weights))

    def run_blocks(*arrays):
        n_weights = len(arrays) - 4
        return jax.shard_map(local_body, mesh=mesh, in_specs=(row_spec,) * 4 + (P(),) * n_weights,
                             out_specs=(row_spec, row_spec), check_vma=False)(*arrays)

    return run_blocks
```

```python
import jax
import jax.numpy as jnp
from jax import lax
from jax.experimental import pallas as pl
from jax.experimental.pallas import tpu as pltpu
from jax.sharding import PartitionSpec as P

MESH = pl.DeviceIdType.MESH
F32 = jnp.float32
BF = jnp.bfloat16
LOG2E = 1.4426950408889634
NEG = -1e9 * LOG2E
ND = 8
VMEM_LIMIT = 66_000_000
RB = 128
SQ = 256
TI = 16
HD = 32
EARLY = 3


def dot(a, b):
    return lax.dot_general(a, b, (((1,), (0,)), ((), ())), preferred_element_type=F32)


def dot_nt(a, b):
    return lax.dot_general(a, b, (((1,), (1,)), ((), ())), preferred_element_type=F32)


def dot_tn(a, b):
    return lax.dot_general(a, b, (((0,), (0,)), ((), ())), preferred_element_type=F32)


def transpose_bf(w):
    return w.astype(F32).T.astype(BF)


def norm_lanes(x):
    mean = jnp.mean(x, axis=-1, keepdims=True)
    centered = x - mean
    var = jnp.mean(centered * centered, axis=-1, keepdims=True)
    return (centered * lax.rsqrt(var + 1e-5)).astype(BF)


def norm_rows(x):
    mean = jnp.mean(x, axis=0, keepdims=True)
    centered = x - mean
    var = jnp.mean(centered * centered, axis=0, keepdims=True)
    return (centered * lax.rsqrt(var + 1e-5)).astype(BF)


def residual(x, update):
    return (x.astype(F32) + update).astype(BF)


def group_barrier(me):
    sem = pltpu.get_barrier_semaphore()
    for p in range(1, ND):
        pl.semaphore_signal(sem, inc=1, device_id={'dap': lax.rem(me + p, ND)}, device_id_type=MESH)
    pl.semaphore_wait(sem, ND - 1)


def remote(src, dst, send_sem, recv_sem, peer):
    return pltpu.make_async_remote_copy(src_ref=src, dst_ref=dst, send_sem=send_sem, recv_sem=recv_sem,
                                        device_id={'dap': peer}, device_id_type=MESH)


class Direct:
    def __init__(self, me, src_of, dst_of, ssem, rsem, base=0):
        self.me, self.src_of, self.dst_of, self.ssem, self.rsem, self.base = me, src_of, dst_of, ssem, rsem, base

    def copy_to(self, p):
        peer = lax.rem(self.me + p, ND)
        return remote(self.src_of(peer), self.dst_of(self.me), self.ssem.at[self.base + p], self.rsem.at[self.base + p], peer)

    def start(self, ps=range(1, ND)):
        for p in ps:
            self.copy_to(p).start()

    def wait_recv(self):
        for p in range(1, ND):
            owner = lax.rem(self.me + ND - p, ND)
            remote(self.src_of(owner), self.dst_of(owner), self.ssem.at[self.base + p], self.rsem.at[self.base + p], owner).wait_recv()

    def wait_send(self):
        for p in range(1, ND):
            self.copy_to(p).wait_send()


class Chain:
    def __init__(self, me, buf, ssem, rsem):
        self.buf, self.ssem, self.rsem = buf, ssem, rsem
        self.z, self.c = lax.div(me, 2), lax.rem(me, 2)
        self.me, self.partner = me, me + 1 - 2 * self.c
        self.size = buf.shape[1] // 2

    def cp(self, slot, peer, sem, half):
        ref = self.buf.at[slot, pl.ds(half * self.size, self.size)]
        return remote(ref, ref, self.ssem.at[half, sem], self.rsem.at[half, sem], peer)

    def slot(self, off, other=False):
        core = 1 - self.c if other else self.c
        return (self.z + off) * 2 + core

    def own(self, act):
        for half in range(2):
            @pl.when(self.z < 3)
            def _():
                act(self.cp(self.me, self.me + 2, 0, half))

            @pl.when(self.z > 0)
            def _():
                act(self.cp(self.me, self.me - 2, 3, half))

        for half in range(2):
            act(self.cp(self.me, self.partner, 6, half))

    def forward(self, t, half, before, act):
        z = self.z

        @pl.when(z >= t)
        def _():
            if before:
                before(self.cp(self.slot(-t), self.me, t - 1, half))
            if t < 3:
                @pl.when(z < 3)
                def _():
                    act(self.cp(self.slot(-t), self.me + 2, t, half))
            act(self.cp(self.slot(-t), self.partner, 6 + t, half))

        @pl.when(z + t <= 3)
        def _():
            if before:
                before(self.cp(self.slot(t), self.me, 2 + t, half))
            if t < 3:
                @pl.when(z > 0)
                def _():
                    act(self.cp(self.slot(t), self.me - 2, 3 + t, half))
            act(self.cp(self.slot(t), self.partner, 9 + t, half))

    def start(self):
        self.own(lambda c: c.start())

    def finish(self, hook=None):
        z = self.z
        for t in range(1, 4):
            for half in range(2):
                self.forward(t, half, lambda c: c.wait_recv(), lambda c: c.start())
            if hook is not None:
                hook(t)
        for half in range(2):
            self.cp(self.partner, self.me, 6, half).wait_recv()
            for t in range(1, 4):
                @pl.when(z >= t)
                def _():
                    self.cp(self.slot(-t, True), self.me, 6 + t, half).wait_recv()

                @pl.when(z + t <= 3)
                def _():
                    self.cp(self.slot(t, True), self.me, 9 + t, half).wait_recv()

    def stream(self, process, hook):
        z = self.z

        def take(t, other):
            def one(k, carry):
                off = (2 * k - 1) * t

                @pl.when(jnp.logical_and(z + off >= 0, z + off <= 3))
                def _():
                    if other:
                        for half in range(2):
                            self.cp(self.slot(off, True), self.me, 6 + 3 * k + t, half).wait_recv()
                    process(self.slot(off, other))

                return carry

            lax.fori_loop(0, 2, one, 0)

        for t in range(1, 4):
            for half in range(2):
                self.forward(t, half, lambda c: c.wait_recv(), lambda c: c.start())
            hook(t)
            if t == 1:
                for half in range(2):
                    self.cp(self.partner, self.me, 6, half).wait_recv()
                process(self.partner)
            else:
                take(t - 1, True)
            take(t, False)
        take(3, True)

    def wait_send(self):
        self.own(lambda c: c.wait_send())
        for t in range(1, 4):
            for half in range(2):
                self.forward(t, half, None, lambda c: c.wait_send())


class Return:
    def __init__(self, me, src, dst, ssem, rsem):
        self.me, self.src, self.dst, self.ssem, self.rsem = me, src, dst, ssem, rsem
        self.z, self.c = lax.div(me, 2), lax.rem(me, 2)

    def copy_to(self, off, core):
        peer = (self.z + off) * 2 + core
        return remote(self.src(peer), self.dst(self.me), self.ssem.at[(off + 3) * 2 + core], self.rsem.at[(off + 3) * 2 + self.c], peer)

    def start(self, off, cond, cores=(0, 1)):
        @pl.when(cond)
        def _():
            for core in cores:
                self.copy_to(off, core).start()

    def start_partner(self):
        self.copy_to(0, 1 - self.c).start()

    def each(self, fn):
        fn(0, 1 - self.c)
        for off in (-3, -2, -1, 1, 2, 3):
            @pl.when(jnp.logical_and(self.z + off >= 0, self.z + off <= 3))
            def _():
                for core in range(2):
                    fn(off, core)

    def wait_recv(self):
        def one(off, core):
            owner = (self.z + off) * 2 + core
            sem = (3 - off) * 2 + core
            remote(self.src(self.me), self.dst(owner), self.ssem.at[sem], self.rsem.at[sem], self.me).wait_recv()

        self.each(one)

    def wait_send(self):
        self.each(lambda off, core: self.copy_to(off, core).wait_send())


def column_of(row):
    return jnp.broadcast_to(row, (RB, row.shape[1])).T


def attend_tiles(xns, wt_ref, wk, w_out, heads, bias_ref, key_masks, depth):
    length = xns[0].shape[0]
    width = heads * HD
    projs = [dot_nt(wt_ref[...], xn) for xn in xns]
    keys = [dot(xn, wk).astype(BF) for xn in xns]
    q_t = [proj[:width].astype(BF) for proj in projs]
    v_t = [proj[width:2 * width].astype(BF) for proj in projs]
    gate = [jax.nn.sigmoid(proj[2 * width:].astype(BF).astype(F32)) for proj in projs]
    valid = [key_mask > 0 for key_mask in key_masks]
    scale = HD ** -0.5 * LOG2E

    def logits_of(unit):
        t, qc, h = unit
        hh = h % 4
        rhs = [q_t[t][HD * h:HD * h + HD, RB * qc:RB * qc + RB]]
        if hh > 0:
            rhs = [jnp.zeros((HD * hh, RB), BF)] + rhs
        if hh < 3:
            rhs = rhs + [jnp.zeros((96 - HD * hh, RB), BF)]
        return dot(keys[t][:, RB * (h // 4):RB * (h // 4) + RB], jnp.concatenate(rhs, 0))

    def prob_of(unit, raw):
        t, qc, h = unit
        logits = raw * scale
        if bias_ref is not None:
            logits = logits + bias_ref[h]
        logits = jnp.where(valid[t], logits, NEG)
        e = jnp.exp2(logits - jnp.max(logits, axis=0, keepdims=True))
        return (e * (1.0 / jnp.sum(e, axis=0, keepdims=True))).astype(BF)

    blocks = [(t, qc) for t in range(len(xns)) for qc in range(length // RB)]
    units = [(t, qc, h) for t, qc in blocks for h in range(heads)]
    raws = {i: logits_of(units[i]) for i in range(min(depth, len(units)))}
    outs, probs, upds = {}, {}, {}

    def flush(i):
        t, qc, h = units[i]
        outs[units[i]] = dot(v_t[t][HD * h:HD * h + HD], probs.pop(i))
        if h == heads - 1:
            o = jnp.concatenate([outs.pop((t, qc, hh)) for hh in range(heads)], 0)
            upds[t, qc] = (o * gate[t][:, RB * qc:RB * qc + RB]).astype(BF)

    for i in range(len(units)):
        if i + depth < len(units):
            raws[i + depth] = logits_of(units[i + depth])
        probs[i] = prob_of(units[i], raws.pop(i))
        if i > 0:
            flush(i - 1)
    flush(len(units) - 1)
    pieces = [dot_tn(upds[block], w_out) for block in blocks]
    per = length // RB
    return [jnp.concatenate(pieces[t * per:t * per + per], 0) for t in range(len(xns))]


def tile_loop(count, width, body):
    def step(g, carry):
        body([g * width + u for u in range(width)])
        return carry

    lax.fori_loop(0, count // width, step, 0)


def prep_qkvg(w_ref, wt_ref, width):
    wt_ref[0:width, :] = transpose_bf(w_ref[0, :, 0:width])
    wt_ref[width:3 * width, :] = transpose_bf(w_ref[0, :, 2 * width:4 * width])


def blocks_kernel(m_in, z_in, mm_ref, pm_in,
                  row_w, row_bt, row_o, col_w, col_o, mtr_i, mtr_o, opt, opm_o,
                  tmo_p, tmo_o, tmi_p, tmi_o, tas_w, tas_bt, tas_o, tae_w, tae_bt, tae_o, ptr_i, ptr_o,
                  mout_ref, zout_ref,
                  mbuf, pbuf, mt_ref, pt_ref, rmask_ref, pm_ref,
                  ball, bias_t, wt, scr, sendbuf, rbuf, bscr, m2_ref, at_ref,
                  btall, obuf, opw, scr_a, scr_b, scr_x, a_c, ball1, ball2, gbuf, z1, zcol, sbias, ball3,
                  wt2, twt, twt2, zall, zsend, z4, mrecv, mscr,
                  ssem, rsem, ch_s, ch_r, ms, mr):
    me = lax.axis_index('dap')
    chip = lax.div(me, 2)
    first = pl.program_id(0) == 0
    group_barrier(me)
    ex_k = [Direct(me, lambda peer, buf=buf: buf.at[me], lambda owner, buf=buf: buf.at[owner], ssem, rsem, base)
            for buf, base in ((mbuf, 0), (pbuf, 8))]

    @pl.when(first)
    def _():
        rmask_ref[...] = mm_ref[...].astype(F32)
        pm_ref[...] = pm_in[...].astype(F32)
        mbuf[me] = rmask_ref[...]
        pbuf[me] = pm_ref[...]
        for ex in ex_k:
            ex.start()

        zout_ref[...] = z_in[...]

    m_ref, z_ref = mout_ref, zout_ref
    wb_t = row_bt[0]

    def bias_row(tiles):
        rows = [dot_nt(wb_t, norm_lanes(z_ref[i].astype(F32))) for i in tiles]
        for i, row in zip(tiles, rows):
            bscr[pl.ds(i, 8, stride=TI), :] = row

    tile_loop(TI, 8, bias_row)
    ball[me] = bscr[...].astype(BF).reshape(8, TI, RB)
    ex_b = Direct(me, lambda peer: ball.at[me], lambda owner: ball.at[owner], ssem, rsem, TI)
    ex_b.start()

    @pl.when(first)
    def _():
        def take(s, carry):
            mout_ref[s] = m_in[s]
            return carry

        lax.fori_loop(0, HD, take, 0)

    prep_qkvg(row_w, wt, SQ)

    @pl.when(first)
    def _():
        for ex in ex_k:
            ex.wait_recv()
        mt_ref[...] = mbuf[...].reshape(SQ, RB).T
        pt_ref[...] = pbuf[...].reshape(RB, RB).T
        for ex in ex_k:
            ex.wait_send()

    ex_b.wait_recv()
    for h in range(8):
        bias_t[h] = ball[:, h].reshape(RB, RB).astype(F32).T * LOG2E
    row_k = row_w[0, :, SQ:512]
    row_ow = row_o[0]
    def piece(ck, q):
        part = pl.ds(q * 2, 2)
        return Direct(me, lambda peer: sendbuf.at[ck, peer, part], lambda owner: rbuf.at[owner * 2 + ck, part], ssem, rsem, 24 + ck * 64 + q * ND)

    def half_rows(ck, carry):
        def row_body(sls):
            xs = [m_ref[ck * TI + sl] for sl in sls]
            masks = [column_of(rmask_ref[pl.ds(ck * TI + sl, 1), :]) for sl in sls]
            xns = [norm_lanes(x.astype(F32)) for x in xs]
            upds = attend_tiles(xns, wt, row_k, row_ow, 8, bias_t, masks, 6)
            for sl, x, upd in zip(sls, xs, upds):
                y = residual(x, upd).astype(F32)
                for half in range(2):
                    scr[half, pl.ds(sl, RB, stride=TI), :] = y[:, RB * half:RB * half + RB]

        tile_loop(TI, 8, row_body)

        def pack(d, carry):
            for half in range(2):
                part = scr[half, pl.ds(pl.multiple_of(d * SQ, SQ), SQ), :].astype(BF).reshape(TI, TI, RB)
                sendbuf[ck, d, :, :, RB * half:RB * half + RB] = part
            return carry

        lax.fori_loop(0, 8, pack, 0)
        rbuf[me * 2 + ck] = sendbuf[ck, me]
        for q in range(EARLY):
            piece(ck, q).start()
        return carry

    lax.fori_loop(0, 2, half_rows, 0)

    def send_rest(q, carry):
        piece(0, q).start()
        piece(1, q).start()
        return carry

    lax.fori_loop(EARLY, 8, send_rest, 0)
    ex_b.wait_send()
    prep_qkvg(col_w, wt, SQ)
    col_k = col_w[0, :, SQ:512]
    col_ow = col_o[0]

    def col_body(rs):
        xs = [rbuf[:, r].reshape(SQ, SQ) for r in rs]
        mrows = [mt_ref[pl.ds(me * TI + r, 1), :] for r in rs]
        masks = [column_of(mrow) for mrow in mrows]
        upds = attend_tiles([norm_lanes(x.astype(F32)) for x in xs], wt, col_k, col_ow, 8, None, masks, 6)
        for r, x, upd in zip(rs, xs, upds):
            m2_ref[r] = residual(x, upd)

    def mtr_body(rs):
        ys = [m2_ref[r] for r in rs]
        mrows = [mt_ref[pl.ds(me * TI + r, 1), :] for r in rs]
        xns = [norm_lanes(y.astype(F32)) for y in ys]
        hids = [jnp.maximum(dot(xn, mtr_i[0]), 0.0).astype(BF) for xn in xns]
        y2s = [residual(y, dot(hid, mtr_o[0])) for y, hid in zip(ys, hids)]
        xns = [norm_lanes(y2.astype(F32)) for y2 in y2s]
        abs_ = [dot_nt(opt[0], xn).astype(BF).astype(F32) * mrow for xn, mrow in zip(xns, mrows)]
        for r, y2, ab in zip(rs, y2s, abs_):
            m2_ref[r] = y2
            at_ref[r] = ab[0:HD].astype(BF)
            for half in range(2):
                scr[half, pl.ds(r, HD, stride=TI), :] = ab[HD:2 * HD, RB * half:RB * half + RB]

    def col_quarter(q, carry):
        piece(0, q).wait_recv()
        piece(1, q).wait_recv()
        col_body([q * 2, q * 2 + 1])
        mtr_body([q * 2, q * 2 + 1])
        return carry

    lax.fori_loop(0, 8, col_quarter, 0)
    for half in range(2):
        btall[me, :, :, RB * half:RB * half + RB] = scr[half, 0:512, :].astype(BF).reshape(HD, TI, RB)
    ag0 = Chain(me, btall, ch_s.at[0], ch_r.at[0])
    ag0.start()
    scr_a[0:1024, :] = opm_o[0].astype(F32)

    def perm(e, carry):
        rows = scr_a[pl.ds(e, HD, stride=HD), :]
        scr_b[pl.ds(pl.multiple_of(e * HD, HD), HD), :] = rows
        return carry

    lax.fori_loop(0, HD, perm, 0)
    for q in range(8):
        opw[:, RB * q:RB * q + RB] = scr_b[RB * q:RB * q + RB, :].T.astype(BF)
    mloc = mt_ref[pl.ds(pl.multiple_of(me * TI, TI), TI), :].astype(BF)
    inv_over = 1.0 / (1e-3 + dot_nt(mloc, mt_ref[...].astype(BF)))
    scr_x[0:TI, :] = inv_over
    twt[...] = transpose_bf(tmo_p[0, :, 0:512])
    ag0.finish()
    ret = Return(me, lambda peer: m2_ref.at[:, pl.ds(pl.multiple_of(peer * HD, HD), HD), :], lambda owner: mrecv.at[owner], ms, mr)
    ret.start(3, chip == 0)
    ret.start(-3, chip == 3)
    mrecv[me] = m2_ref[:, pl.ds(pl.multiple_of(me * HD, HD), HD), :]

    left = at_ref[...].reshape(512, SQ)

    def opm_e(es):
        rhs = [btall[:, e].reshape(RB, SQ) for e in es]
        os_ = [dot_nt(left, r).astype(BF).reshape(TI, HD, RB) for r in rhs]
        for e, o in zip(es, os_):
            obuf[:, pl.ds(pl.multiple_of(e * HD, HD), HD), :] = o

    tile_loop(HD, 8, opm_e)

    def opm_i(tiles):
        y_ts = [dot(opw[...], obuf[i]) * scr_x[pl.ds(i, 1), :] for i in tiles]
        outs = [residual(z_ref[i], y_t.T) for i, y_t in zip(tiles, y_ts)]
        for i, out in zip(tiles, outs):
            z1[i] = out

    tile_loop(TI, 8, opm_i)

    def front(w_ref, wt_l, z_src, ball, left_too):
        wg = w_ref[0, :, 512:640]

        def body(tiles):
            xns = [norm_lanes(z_src[i].astype(F32)) for i in tiles]
            mrows = [pm_ref[pl.ds(i, 1), :] for i in tiles]
            if left_too:
                prs = [dot_nt(wt_l[...], xn) for xn in xns]
                lefts = [mrow * jax.nn.sigmoid(pr[SQ:384]) * pr[0:RB] for mrow, pr in zip(mrows, prs)]
                pbs = [pr[RB:SQ] for pr in prs]
                pgs = [pr[384:512] for pr in prs]
            else:
                lefts = []
                pbs = [dot_nt(wt_l[RB:SQ, :], xn) for xn in xns]
                pgs = [dot_nt(wt_l[384:512, :], xn) for xn in xns]
            gates = [dot(xn, wg) for xn in xns]
            rights = [mrow * jax.nn.sigmoid(pg) * pb for mrow, pg, pb in zip(mrows, pgs, pbs)]
            gates = [jax.nn.sigmoid(g) for g in gates]
            for i, left in zip(tiles, lefts):
                scr_a[pl.ds(i, RB, stride=TI), :] = left
            for i, right, gate in zip(tiles, rights, gates):
                scr_b[pl.ds(i, RB, stride=TI), :] = right
                gbuf[i] = gate

        tile_loop(TI, 8, body)
        ball[me] = scr_b[...].astype(BF).reshape(RB, TI, RB)

    def finish(w_ref, z_src, z_dst):
        w = w_ref[0]

        def body(tiles):
            xns = [norm_rows(scr_x[pl.ds(i, RB, stride=TI), :]) for i in tiles]
            ys = [dot_tn(xn, w) for xn in xns]
            outs = [residual(z_src[i], gbuf[i] * y) for i, y in zip(tiles, ys)]
            for i, out in zip(tiles, outs):
                z_dst[i] = out

        tile_loop(TI, 8, body)

    front(tmo_p, twt, z1, ball1, True)
    ag1 = Chain(me, ball1, ch_s.at[1], ch_r.at[1])
    ag1.start()
    ret.start(1, chip == 0)
    ret.start(-1, chip == 3)
    ret.start_partner()
    a_c[...] = scr_a[...].astype(BF).reshape(RB, TI, RB)

    twt2[...] = transpose_bf(tmi_p[0, :, 0:512])

    def inner(t):
        if t == 1:
            ret.start(1, chip == 1)
            ret.start(-1, chip == 2)

    ag1.finish(inner)

    def out_c(cc, carry):
        for u in range(TI):
            c = cc * TI + u
            scr_x[pl.ds(pl.multiple_of(c * TI, TI), TI), :] = dot_nt(a_c[c], ball1[:, c].reshape(RB, RB))
        return carry

    lax.fori_loop(0, 8, out_c, 0)
    ret.start(1, chip == 2, (0,))
    ret.start(-1, chip == 1, (0,))
    finish(tmo_o, z1, z1)

    zall[me] = z1[...]
    ag2 = Chain(me, zall, ch_s.at[2], ch_r.at[2])
    ag2.start()
    front(tmi_p, twt2, z1, ball2, False)
    prep_qkvg(tas_w, wt2, RB)

    def in_right(slot):
        def body(tiles):
            xns = [norm_lanes(zall[slot, i].astype(F32)) for i in tiles]
            mrows = [pbuf[slot, pl.ds(i, 1), :] for i in tiles]
            pbs = [dot_nt(twt2[RB:SQ, :], xn) for xn in xns]
            pgs = [dot_nt(twt2[384:512, :], xn) for xn in xns]
            rights = [mrow * jax.nn.sigmoid(pg) * pb for mrow, pg, pb in zip(mrows, pgs, pbs)]
            for i, right in zip(tiles, rights):
                scr_b[pl.ds(i, RB, stride=TI), :] = right

        tile_loop(TI, 8, body)
        ball2[slot] = scr_b[...].astype(BF).reshape(RB, TI, RB)

    def two(t):
        if t == 2:
            ret.start(2, chip == 0)
            ret.start(-2, chip == 3)

    ag2.stream(in_right, two)
    scr_b[...] = zall[:, :, pl.ds(pl.multiple_of(me * TI, TI), TI), :].astype(F32).reshape(2048, RB)

    def in_left(tiles):
        xns = [norm_lanes(scr_b[pl.ds(i, RB, stride=TI), :]) for i in tiles]
        mrows = [pt_ref[pl.ds(me * TI + i, 1), :] for i in tiles]
        pas = [dot_nt(twt2[0:RB, :], xn) for xn in xns]
        pgs = [dot_nt(twt2[SQ:384, :], xn) for xn in xns]
        lefts = [mrow * jax.nn.sigmoid(pg) * pa for mrow, pg, pa in zip(mrows, pgs, pas)]
        for i, left in zip(tiles, lefts):
            scr_a[pl.ds(i, RB, stride=TI), :] = left

    tile_loop(TI, 8, in_left)
    a_c[...] = scr_a[...].astype(BF).reshape(RB, TI, RB)

    def in_c(cc, carry):
        for u in range(TI):
            c = cc * TI + u
            scr_x[pl.ds(pl.multiple_of(c * TI, TI), TI), :] = dot(a_c[c], ball2[:, c].reshape(RB, RB))
        return carry

    lax.fori_loop(0, 8, in_c, 0)
    ret.start(1, chip == 2, (1,))
    ret.start(-1, chip == 1, (1,))
    finish(tmi_o, z1, z1)

    def send_bias(slot, base):
        ball3[slot, me] = sbias[0:64, :].astype(BF).reshape(4, TI, RB)
        ex = Direct(me, lambda peer: ball3.at[slot, me], lambda owner: ball3.at[slot, owner], ssem, rsem, base)
        ex.start()
        return ex

    def tas_bias(tiles):
        rows = [dot_nt(tas_bt[0], norm_lanes(z1[i].astype(F32))) for i in tiles]
        for i, row in zip(tiles, rows):
            sbias[pl.ds(i, 4, stride=TI), :] = row

    tile_loop(TI, 8, tas_bias)
    ex_s = send_bias(0, 168)
    ex_s.wait_recv()
    for h in range(4):
        bias_t[h] = ball3[0, :, h].reshape(RB, RB).astype(F32).T * LOG2E
    ret.start(2, chip == 1, (0,))
    ret.start(-2, chip == 2, (0,))
    tas_k = tas_w[0, :, RB:SQ]

    def tas_body(tiles):
        xs = [z1[i] for i in tiles]
        masks = [column_of(pm_ref[pl.ds(i, 1), :]) for i in tiles]
        upds = attend_tiles([norm_lanes(x.astype(F32)) for x in xs], wt2, tas_k, tas_o[0], 4, bias_t, masks, 4)
        outs = [residual(x, upd) for x, upd in zip(xs, upds)]
        rows = [dot_nt(tae_bt[0], norm_lanes(out.astype(F32))) for out in outs]
        for i, out, row in zip(tiles, outs, rows):
            z1[i] = out
            sbias[pl.ds(i, 4, stride=TI), :] = row
        half_z(tiles[0]).start()

    def half_z(row):
        rows = pl.ds(pl.multiple_of(row, 8), 8)
        return Direct(me, lambda peer: z1.at[rows, pl.ds(pl.multiple_of(peer * TI, TI), TI), :], lambda owner: zcol.at[owner, rows],
                      ssem, rsem, 152 + row)

    tile_loop(TI, 8, tas_body)

    ex_e = send_bias(1, 184)
    zcol[me] = z1[:, pl.ds(pl.multiple_of(me * TI, TI), TI), :]
    prep_qkvg(tae_w, wt2, RB)
    for row in (0, 8):
        half_z(row).wait_recv()
    scr_b[...] = zcol[...].astype(F32).reshape(2048, RB)
    ex_e.wait_recv()
    for h in range(4):
        bias_t[h] = ball3[1, :, h].reshape(RB, RB).astype(F32) * LOG2E
    ret.start(2, chip == 1, (1,))
    ret.start(-2, chip == 2, (1,))
    tae_k = tae_w[0, :, RB:SQ]

    def tae_body(tiles):
        xs = [scr_b[pl.ds(i, RB, stride=TI), :] for i in tiles]
        masks = [column_of(pt_ref[pl.ds(me * TI + i, 1), :]) for i in tiles]
        upds = attend_tiles([norm_lanes(x) for x in xs], wt2, tae_k, tae_o[0], 4, bias_t, masks, 4)
        for i, x, upd in zip(tiles, xs, upds):
            scr_a[pl.ds(i, RB, stride=TI), :] = x + upd

    tile_loop(TI, 8, tae_body)
    zsend[...] = scr_a[...].astype(BF).reshape(8, TI, TI, RB)
    ex_z3 = Direct(me, lambda peer: zsend.at[peer], lambda owner: z4.at[:, pl.ds(pl.multiple_of(owner * TI, TI), TI), :], ssem, rsem, 176)
    ex_z3.start()
    z4[:, pl.ds(pl.multiple_of(me * TI, TI), TI), :] = zsend[me]

    ret.wait_recv()

    def widen(d, carry):
        for half in range(2):
            part = mrecv[d, :, :, RB * half:RB * half + RB].astype(F32).reshape(512, RB)
            mscr[half, pl.ds(pl.multiple_of(d * 512, 512), 512), :] = part
        return carry

    lax.fori_loop(0, 8, widen, 0)

    def take_seq(seqs):
        for s in seqs:
            for half in range(2):
                mout_ref[s, :, RB * half:RB * half + RB] = mscr[half, pl.ds(s, RB, stride=HD), :].astype(BF)

    tile_loop(HD, 4, take_seq)
    ex_z3.wait_recv()

    def trans(tiles):
        xs = [z4[i] for i in tiles]
        xns = [norm_lanes(x.astype(F32)) for x in xs]
        hids = [jnp.maximum(dot(xn, ptr_i[0]), 0.0).astype(BF) for xn in xns]
        outs = [residual(x, dot(hid, ptr_o[0])) for x, hid in zip(xs, hids)]
        for i, out in zip(tiles, outs):
            zout_ref[i] = out

    tile_loop(TI, 8, trans)
    def sent(q, carry):
        piece(0, q).wait_send()
        piece(1, q).wait_send()
        return carry

    lax.fori_loop(0, 8, sent, 0)
    for ex in (ag0, ag1, ag2, ret, ex_s, ex_e, half_z(0), half_z(8), ex_z3):
        ex.wait_send()


def full(shape):
    return pl.BlockSpec(shape, lambda g: (0,) * len(shape))


def layer_of(shape):
    return pl.BlockSpec((1,) + shape[1:], lambda g: (g,) + (0,) * (len(shape) - 1))


def run(m, z, mm, pm, weights):
    acts = (m, z, mm, pm)
    outs = [(HD, RB, SQ), (TI, RB, RB)]
    vm = pltpu.VMEM
    return pl.pallas_call(
        blocks_kernel,
        grid=(weights[0].shape[0],),
        out_shape=[jax.ShapeDtypeStruct(s, BF) for s in outs],
        in_specs=[full(a.shape) for a in acts] + [layer_of(w.shape) for w in weights],
        out_specs=[full(s) for s in outs],
        scratch_shapes=[
            vm((ND, HD, RB), F32), vm((ND, TI, RB), F32), vm((RB, SQ), F32), vm((RB, RB), F32), vm((HD, RB), F32), vm((TI, RB), F32),
            vm((ND, 8, TI, RB), BF), vm((8, RB, RB), F32), vm((768, SQ), BF), vm((2, 2048, RB), F32),
            vm((2, ND, TI, TI, SQ), BF), vm((2 * ND, TI, TI, SQ), BF), vm((RB, RB), F32), vm((TI, SQ, SQ), BF), vm((TI, HD, SQ), BF),
            vm((ND, HD, TI, SQ), BF), vm((TI, 1024, RB), BF), vm((RB, 1024), BF),
            vm((2048, RB), F32), vm((2048, RB), F32), vm((2048, RB), F32),
            vm((RB, TI, RB), BF), vm((ND, RB, TI, RB), BF), vm((ND, RB, TI, RB), BF), vm((TI, RB, RB), F32), vm((TI, RB, RB), BF),
            vm((ND, TI, TI, RB), BF), vm((RB, RB), F32), vm((2, ND, 4, TI, RB), BF),
            vm((384, RB), BF), vm((512, RB), BF), vm((512, RB), BF), vm((ND, TI, RB, RB), BF), vm((ND, TI, TI, RB), BF), vm((TI, RB, RB), BF),
            vm((ND, TI, HD, SQ), BF), vm((2, 4096, RB), F32),
            pltpu.SemaphoreType.DMA((192,)), pltpu.SemaphoreType.DMA((192,)),
            pltpu.SemaphoreType.DMA((3, 2, 13)), pltpu.SemaphoreType.DMA((3, 2, 13)),
            pltpu.SemaphoreType.DMA((14,)), pltpu.SemaphoreType.DMA((14,)),
        ],
        compiler_params=pltpu.CompilerParams(collective_id=0, has_side_effects=True, vmem_limit_bytes=VMEM_LIMIT),
    )(*acts, *weights)


def solution(mesh):
    row_spec = P(('req', 'dap'))

    def local_body(m, z, mm, pm, *weights):
        weights = [jnp.swapaxes(w, 1, 2) if k in (1, 7, 14, 17) else w for k, w in enumerate(weights)]
        return tuple(run(m, z, mm, pm, weights))

    def run_blocks(*arrays):
        n_weights = len(arrays) - 4
        return jax.shard_map(local_body, mesh=mesh, in_specs=(row_spec,) * 4 + (P(),) * n_weights,
                             out_specs=(row_spec, row_spec), check_vma=False)(*arrays)

    return run_blocks
```
